32 devices in a mesh: nest: 2 (over core), row: 4 (over y, x), col: 4 (over z).
Axes of the slice: x: 2, y: 2, z: 4, core: 2. Of those that a mesh axis runs over, the one named last changes fastest.
Arguments:
- strips: float32 [2, 3, 4, 16, 24, 1536], P('nest', None, None, ('row', 'col')), may hold values from -1.5 to 2, as said below
- anchor: int32 [2, 2], replicated, may hold values from 1 to 127
- wet_mask: int32 [2, 512, 512], P('nest', 'row', 'col'), may hold values 0 or 1
- bathy_index: int32 [2, 512, 512], P('nest', 'row', 'col'), may hold values from 0 to 15
- bed_levels: float32 [16], replicated, may hold values from 0 to 1.5
- coarse: float32 [3, 1024, 512], P(None, ('nest', 'row'), 'col'), may hold values from -6 to 6
Outputs:
- fine_fields: float32 [2, 3, 1536, 1536], P('nest', None, 'row', 'col')
- coarse_next: float32 [3, 1024, 512], P(None, ('nest', 'row'), 'col')
The draws below stay inside these ranges and needn't reach their ends.
Inputs may be any that keep to these rules, and one draw needn't show every extreme that they name: `strips`: plane 0 of the second dimension is the water depth, within 0.5 to 2; planes 1 and 2 are momenta within -1.5 to 1.5. anchor[n] holds the row and then the column offset of nest n's first coarse cell within its block of coarse rows.
All inputs are finite; a program needn't handle non-finite values. No bound on the sum of `wet_mask` on one device may be relied on, other than what follows from the above.
Results may differ from the reference program's by a relative error of at most 0.0003.
Values sent between devices are 32-bit elements; how exact they have to be, the bound alone decides.
A program may use at most 128 MiB of HBM per device.

```python
import jax
import jax.numpy as jnp
from jax import lax

TR = 384
TC = 384
NLEV = 16
STRIPS = 16
BAND = 24
NFR = 1536
NFC = 1536
CR = 128
CC = 128
NCR = 1024
NCC = 512
N_NEST = 2
N_ROW = 4
N_COL = 4


def draw_strips(key, part):
    shape_depth = (N_NEST, 1, N_ROW, STRIPS, BAND, NFC)
    shape_flow = (N_NEST, 2, N_ROW, STRIPS, BAND, NFC)
    key_depth = jax.random.fold_in(key, 11)
    key_flow = jax.random.fold_in(key, 12)
    depth_part = jnp.clip(1.25 + 0.3 * jax.random.normal(key_depth, shape_depth, jnp.float32), 0.5, 2.0)
    flow_part = jnp.clip(0.4 * jax.random.normal(key_flow, shape_flow, jnp.float32), -1.5, 1.5)
    return jnp.concatenate([depth_part, flow_part], axis=1)


def plant(array, own_key, smallest, largest):
    longest = array.shape.index(max(array.shape))
    spots = []
    for shift in (0, 1):
        where = [jax.random.randint(jax.random.fold_in(own_key, axis), (), 0, length) for axis, length in enumerate(array.shape)]
        where[longest] = (where[longest] + shift) % array.shape[longest]
        spots.append(tuple(where))
    return array.at[spots[0]].set(smallest).at[spots[1]].set(largest)


def level_of(own_key, shape, shards, least, top_value):
    gain = 1.0
    for axis_at, parts in shards:
        draws = jax.random.uniform(jax.random.fold_in(jax.random.fold_in(own_key, 6), axis_at), (parts,), jnp.float32, least / len(shards), top_value / len(shards))
        gain = gain * jnp.repeat(jnp.exp(draws), shape[axis_at] // parts).reshape((-1,) + (1,) * (len(shape) - 1 - axis_at))
    return gain


def gaussian(own_key, extent, deviation, bound, cuts=(), held_as=jnp.bfloat16):
    entries = jax.random.normal(own_key, extent, jnp.float32) * deviation
    if len(cuts) > 0:
        entries = level_of(own_key, extent, cuts, -0.22, 0.18) * entries
    return jnp.clip(entries, min=-bound, max=bound).astype(held_as)


def setup_inputs(seed: int = 0) -> dict:
    splits = jax.random.split(jax.random.key(seed), 7)
    strips = draw_strips(jax.random.fold_in(splits[6], 71), 0)
    anchor = plant(jax.random.randint(splits[1], (N_NEST, 2), 1, min(TR, TC) // 3), jax.random.fold_in(splits[1], 1), 1, (min(TR, TC) // 3) - 1).astype(jnp.int32)
    wet_mask = plant((jax.random.randint(splits[2], (N_NEST, NFR // 3, NFC // 3), 0, 5) < 4).astype(jnp.int32), jax.random.fold_in(splits[2], 1), 0, 1)
    bathy_index = plant(jax.random.randint(splits[3], (N_NEST, NFR // 3, NFC // 3), 0, NLEV), jax.random.fold_in(splits[3], 1), 0, NLEV - 1).astype(jnp.int32)
    bed_levels = jnp.clip(jax.random.uniform(splits[4], (NLEV,), jnp.float32, 0.0, 1.5), 0.0, 1.5)
    coarse = gaussian(splits[5], (3, NCR, NCC), 1.0, 6.0, ((1, 8), (2, 4)), jnp.float32)
    return {"strips": strips, "anchor": anchor, "wet_mask": wet_mask, "bathy_index": bathy_index, "bed_levels": bed_levels, "coarse": coarse}


gravity = 1.0
courant = 0.2

def advance(padded, bed_pad, wet_pad):
    depth_now = padded[0]
    flow_u = padded[1]
    flow_v = padded[2]
    depth_safe = jnp.where(wet_pad > 0.5, depth_now, 1.0)
    speed_u = flow_u / depth_safe
    speed_v = flow_v / depth_safe
    celerity = jnp.sqrt(gravity * depth_safe)
    pressure = 0.5 * gravity * depth_safe * depth_safe
    fluxes_x = (flow_u, flow_u * speed_u + pressure, flow_v * speed_u)
    fluxes_y = (flow_v, flow_u * speed_v, flow_v * speed_v + pressure)
    reach_x = jnp.abs(speed_u) + celerity
    reach_y = jnp.abs(speed_v) + celerity
    open_x = wet_pad[1:-1, :-1] * wet_pad[1:-1, 1:]
    open_y = wet_pad[:-1, 1:-1] * wet_pad[1:, 1:-1]
    bound_x = jnp.maximum(reach_x[1:-1, :-1], reach_x[1:-1, 1:])
    bound_y = jnp.maximum(reach_y[:-1, 1:-1], reach_y[1:, 1:-1])
    slope_x = (bed_pad[1:-1, 1:] - bed_pad[1:-1, :-1]) * open_x
    slope_y = (bed_pad[1:, 1:-1] - bed_pad[:-1, 1:-1]) * open_y
    centre = depth_now[1:-1, 1:-1]
    sources = (None, -0.5 * gravity * centre * (slope_x[:, 1:] + slope_x[:, :-1]), -0.5 * gravity * centre * (slope_y[1:] + slope_y[:-1]))
    results = []
    for plane in range(3):
        state = padded[plane]
        flux_col = fluxes_x[plane]
        flux_row = fluxes_y[plane]
        face_x = (0.5 * (flux_col[1:-1, :-1] + flux_col[1:-1, 1:]) - 0.5 * bound_x * (state[1:-1, 1:] - state[1:-1, :-1])) * open_x
        face_y = (0.5 * (flux_row[:-1, 1:-1] + flux_row[1:, 1:-1]) - 0.5 * bound_y * (state[1:, 1:-1] - state[:-1, 1:-1])) * open_y
        value = state[1:-1, 1:-1] - courant * (face_x[:, 1:] - face_x[:, :-1]) - courant * (face_y[1:] - face_y[:-1])
        if plane > 0:
            value = value + courant * sources[plane]
        results.append(value)
    return jnp.stack(results)

def expand(cells):
    return jnp.repeat(jnp.repeat(cells, 3, axis=-2), 3, axis=-1)

def lookup(classes, levels):
    ladder = jnp.arange(levels.shape[0], dtype=jnp.int32)
    matches = classes[None] == ladder[:, None, None]
    return lax.optimization_barrier(jnp.sum(jnp.where(matches, levels[:, None, None], 0.0), axis=0))

def restrict(updated):
    planes, row_count, col_count = updated.shape
    return updated.reshape(planes, row_count // 3, 3, col_count // 3, 3).sum(axis=(2, 4)) / 9.0

def reference(strips, anchor, wet_mask, bathy_index, bed_levels, coarse):
    fine_rows = TR * N_ROW
    fine_cols = TC * N_COL
    fields_all = strips.reshape(N_NEST, 3, fine_rows, fine_cols)
    coarse_rows = NCR
    coarse_cols = NCC
    canvas = jnp.zeros((4, coarse_rows + CR, coarse_cols + CC), jnp.float32)
    outputs = []
    for nest_id in range(N_NEST):
        wetness = expand(wet_mask[nest_id].astype(jnp.float32))
        bed_fine = expand(lookup(bathy_index[nest_id], bed_levels))
        padded = jnp.pad(fields_all[nest_id], ((0, 0), (1, 1), (1, 1)))
        wet_pad = jnp.pad(wetness, 1)
        bed_pad = jnp.pad(bed_fine, 1)
        updated = advance(padded, bed_pad, wet_pad)
        outputs.append(updated)
        restricted = restrict(updated)
        contribution = jnp.concatenate([restricted, jnp.ones((1,) + restricted.shape[1:], jnp.float32)], axis=0)
        start_row = (nest_id * N_ROW * CR + anchor[nest_id, 0]).astype(jnp.int32)
        start_col = anchor[nest_id, 1].astype(jnp.int32)
        placed = lax.dynamic_update_slice(jnp.zeros_like(canvas), contribution, (jnp.int32(0), start_row, start_col))
        canvas = canvas + placed
    received_sum = canvas[:, :coarse_rows, :coarse_cols]
    coarse_next = (coarse + received_sum[:3]) / (1.0 + received_sum[3])
    return (jnp.stack(outputs), coarse_next)
```

```python
import functools

import jax
import jax.numpy as jnp
from jax import lax
from jax.experimental import pallas as pl
from jax.experimental.pallas import tpu as pltpu
from jax.sharding import PartitionSpec as P

gravity = 1.0
courant = 0.2
MESH = pl.DeviceIdType.MESH
LANES = 128
SUB = 8
HEAD = 7
VMEM_BYTES = 67043328


def onehot(cond):
    return jnp.where(cond, 1.0, 0.0).astype(jnp.bfloat16)


def iota(shape, dim):
    return lax.broadcasted_iota(jnp.int32, shape, dim)


def dot(a, b):
    return jnp.dot(a, b, preferred_element_type=jnp.float32)


def dot_t(a, b):
    return lax.dot_general(
        a, b, (((1,), (1,)), ((), ())), preferred_element_type=jnp.float32
    )


def split(x, terms):
    parts = []
    for _ in range(terms):
        part = x.astype(jnp.bfloat16)
        parts.append(part)
        x = x - part.astype(jnp.float32)
    return parts


def exchange_kernel(
    rows, cols, strips, wet, cls, fields, colh, rowh, cellh,
    held, wet_v, cls_v, col_msg, row_msg, cell_msg, load_sem,
    big_send, big_recv, col_send, col_recv, row_send, row_recv, cell_send, cell_recv,
):
    parts = rows * cols
    row, col = lax.axis_index("row"), lax.axis_index("col")
    me = row * cols + col
    band = strips.shape[4]
    tile_cols = fields.shape[3]
    full_cols = strips.shape[5]

    loads = [
        pltpu.make_async_copy(strips.at[0, :, :, 0], held, load_sem.at[0]),
        pltpu.make_async_copy(wet.at[0], wet_v, load_sem.at[1]),
        pltpu.make_async_copy(cls.at[0], cls_v, load_sem.at[2]),
    ]
    for load in loads:
        load.start()

    def place(q):
        return {"row": q // cols, "col": lax.rem(q, cols)}

    barrier = pltpu.get_barrier_semaphore()

    def greet(t, _):
        q = lax.rem(me + t, parts)
        pl.semaphore_signal(barrier, inc=1, device_id=place(q), device_id_type=MESH)
        return 0

    lax.fori_loop(1, parts, greet, 0)
    pl.semaphore_wait(barrier, parts - 1)

    def columns(c):
        return pl.ds(pl.multiple_of(c * tile_cols, LANES), tile_cols)

    def big(q):
        return pltpu.make_async_remote_copy(
            src_ref=strips.at[0, :, q // cols, 0, :, columns(lax.rem(q, cols))],
            dst_ref=fields.at[:, me],
            send_sem=big_send.at[q],
            recv_sem=big_recv.at[me],
            device_id=place(q),
            device_id_type=MESH,
        )

    def big_start(t, _):
        big(lax.rem(me + t, parts)).start()
        return 0

    lax.fori_loop(1, parts, big_start, 0)
    own = pltpu.make_async_copy(
        strips.at[0, :, row, 0, :, columns(col)], fields.at[:, me], big_recv.at[me]
    )
    own.start()

    for load in loads:
        load.wait()
    lane = iota((SUB, LANES), 1)
    sub = iota((SUB, LANES), 0)
    first = onehot(lane == 0)
    last = onehot(lane == LANES - 1)
    even = iota((SUB, band), 0)
    for j in range(rows):
        for c in range(cols):
            message = jnp.zeros((SUB, band), jnp.float32)
            for k in range(3):
                if c > 0:
                    for part in split(held[k, j, :, c * tile_cols - LANES : c * tile_cols], 3):
                        message += jnp.where(even == k, dot_t(last, part), 0.0)
                if c < cols - 1:
                    for part in split(
                        held[k, j, :, (c + 1) * tile_cols : (c + 1) * tile_cols + LANES], 3
                    ):
                        message += jnp.where(even == 3 + k, dot_t(first, part), 0.0)
            col_msg[j * cols + c, :, 0:band] = message
    for j in range(rows):
        for k in range(3):
            row_msg[0, j, k : k + 1, :] = held[k, j, band - 1 : band, :]
            row_msg[1, j, k : k + 1, :] = held[k, j, 0:1, :]
    cell_rows = wet_v.shape[0]
    for at, cells in enumerate((wet_v, cls_v)):
        cell_msg[0, at : at + 1, :] = cells[cell_rows - 1 : cell_rows, :]
        cell_msg[1, at : at + 1, :] = cells[0:1, :]
        across = cells[...].astype(jnp.float32).astype(jnp.bfloat16)
        width = across.shape[1]
        pick = iota((SUB, width), 1)
        cell_msg[2, at : at + 1, :] = dot_t(onehot(pick == width - 1), across)[0:1].astype(jnp.int32)
        cell_msg[3, at : at + 1, :] = dot_t(onehot(pick == 0), across)[0:1].astype(jnp.int32)

    def col_copy(q):
        return pltpu.make_async_remote_copy(
            src_ref=col_msg.at[q],
            dst_ref=colh.at[me],
            send_sem=col_send.at[q],
            recv_sem=col_recv.at[me],
            device_id=place(q),
            device_id_type=MESH,
        )

    def col_start(t, _):
        col_copy(lax.rem(me + t, parts)).start()
        return 0

    lax.fori_loop(1, parts, col_start, 0)
    own_col = pltpu.make_async_copy(col_msg.at[me], colh.at[me], col_recv.at[me])
    own_col.start()

    cell_links = (
        (0, row < rows - 1, {"row": row + 1, "col": col}, row > 0),
        (1, row > 0, {"row": row - 1, "col": col}, row < rows - 1),
        (2, col < cols - 1, {"row": row, "col": col + 1}, col > 0),
        (3, col > 0, {"row": row, "col": col - 1}, col < cols - 1),
    )

    def cell_copy(slot, target):
        return pltpu.make_async_remote_copy(
            src_ref=cell_msg.at[slot],
            dst_ref=cellh.at[slot],
            send_sem=cell_send.at[slot],
            recv_sem=cell_recv.at[slot],
            device_id=target,
            device_id_type=MESH,
        )

    for slot, sends, target, _ in cell_links:
        @pl.when(sends)
        def _(slot=slot, target=target):
            cell_copy(slot, target).start()

    def row_copy(slot, j, c):
        target_row = j + 1 if slot == 0 else j - 1
        return pltpu.make_async_remote_copy(
            src_ref=row_msg.at[slot, j, :, c * tile_cols : (c + 1) * tile_cols],
            dst_ref=rowh.at[slot],
            send_sem=row_send.at[slot, j, c],
            recv_sem=row_recv.at[slot],
            device_id={"row": target_row, "col": c},
            device_id_type=MESH,
        )

    def row_own(slot, j, c):
        return pltpu.make_async_copy(
            row_msg.at[slot, j, :, c * tile_cols : (c + 1) * tile_cols],
            rowh.at[slot],
            row_recv.at[slot],
        )

    owner = (rows * cols - 1, 0)
    for slot in range(2):
        @pl.when(me == owner[slot])
        def _(slot=slot):
            for j in range(rows):
                target_row = j + 1 if slot == 0 else j - 1
                if target_row < 0 or target_row >= rows:
                    continue
                for c in range(cols):
                    if target_row * cols + c == owner[slot]:
                        row_own(slot, j, c).start()
                    else:
                        row_copy(slot, j, c).start()

    def arrive(t, _):
        q = lax.rem(me + t, parts)
        pltpu.make_async_copy(fields.at[:, q], fields.at[:, q], big_recv.at[q]).wait()
        pltpu.make_async_copy(colh.at[q], colh.at[q], col_recv.at[q]).wait()
        return 0

    lax.fori_loop(0, parts, arrive, 0)
    for slot, _, target, receives in cell_links:
        @pl.when(receives)
        def _(slot=slot, target=target):
            cell_copy(slot, target).wait_recv()

    for slot, receives in ((0, row > 0), (1, row < rows - 1)):
        @pl.when(receives)
        def _(slot=slot):
            row_own(slot, 0, 0).wait()

    def leave(t, _):
        q = lax.rem(me + t, parts)
        big(q).wait_send()
        col_copy(q).wait_send()
        return 0

    lax.fori_loop(1, parts, leave, 0)
    for slot, sends, target, _ in cell_links:
        @pl.when(sends)
        def _(slot=slot, target=target):
            cell_copy(slot, target).wait_send()
    for slot in range(2):
        @pl.when(me == owner[slot])
        def _(slot=slot):
            for j in range(rows):
                target_row = j + 1 if slot == 0 else j - 1
                if target_row < 0 or target_row >= rows:
                    continue
                for c in range(cols):
                    if target_row * cols + c != owner[slot]:
                        row_copy(slot, j, c).wait_send()


def exchange(rows, cols, strips, wet, cls):
    parts = rows * cols
    blocks, band, full_cols = strips.shape[2], strips.shape[4], strips.shape[5]
    tile_cols = full_cols // cols
    any_spec = pl.BlockSpec(memory_space=pl.ANY)
    dma = pltpu.SemaphoreType.DMA
    f32 = jnp.float32
    return pl.pallas_call(
        functools.partial(exchange_kernel, rows, cols),
        out_shape=(
            jax.ShapeDtypeStruct((3, parts, band, tile_cols), f32),
            jax.ShapeDtypeStruct((parts, SUB, LANES), f32),
            jax.ShapeDtypeStruct((2, SUB, tile_cols), f32),
            jax.ShapeDtypeStruct((4, SUB, LANES), jnp.int32),
        ),
        in_specs=[any_spec] * 3,
        out_specs=(any_spec,) * 4,
        scratch_shapes=[
            pltpu.VMEM((3, blocks, band, full_cols), f32),
            pltpu.VMEM(wet.shape[1:], jnp.int32),
            pltpu.VMEM(cls.shape[1:], jnp.int32),
            pltpu.VMEM((parts, SUB, LANES), f32),
            pltpu.VMEM((2, blocks, SUB, full_cols), f32),
            pltpu.VMEM((4, SUB, LANES), jnp.int32),
            dma((3,)),
            dma((parts,)), dma((parts,)), dma((parts,)), dma((parts,)),
            dma((2, rows, cols)), dma((2,)), dma((4,)), dma((4,)),
        ],
        compiler_params=pltpu.CompilerParams(collective_id=0, has_side_effects=True),
        name="exchange",
    )(strips, wet, cls)


def step_kernel(
    rows, cols, chunk, anchor, levels, fields, edge_cols, rowh, wet, cls, cellh,
    fine, quads, pad, bed_v, wet_p, bed_p,
):
    nest, row, col = lax.axis_index("nest"), lax.axis_index("row"), lax.axis_index("col")
    tile_rows, tile_cols = fields.shape[1], fields.shape[2]
    cell_rows, cell_cols = wet.shape
    wide = tile_cols + LANES
    above, below = row > 0, row < rows - 1
    left, right = col > 0, col < cols - 1
    end = SUB + tile_rows

    def look(classes):
        bed = jnp.zeros(classes.shape, jnp.float32)
        for at in range(levels.shape[0]):
            bed = jnp.where(classes == at, levels[at], bed)
        return bed

    down = onehot(iota((tile_rows, cell_rows), 0) // 3 == iota((tile_rows, cell_rows), 1))
    across = onehot(iota((cell_cols, tile_cols), 1) // 3 == iota((cell_cols, tile_cols), 0))
    lane = iota((tile_rows, LANES), 1)

    def side(low, high):
        low = jnp.where(left, low, 0.0)
        high = jnp.where(right, high, 0.0)
        return jnp.where(lane == 0, high, jnp.where(lane == LANES - 1, low, 0.0))

    edge = cellh[...]
    edge_bed = [look(edge[slot]) for slot in range(4)]
    edge_wet = [edge[slot].astype(jnp.float32) for slot in range(4)]
    bed_v[...] = look(cls[...])
    for target, inner, edges, at, terms in (
        (wet_p, wet[...].astype(jnp.float32), edge_wet, 0, 1),
        (bed_p, bed_v[...], edge_bed, 1, 3),
    ):
        full = 0.0
        for part in split(inner, terms):
            full += dot(dot(down, part).astype(jnp.bfloat16), across)
        target[SUB:end, 0:tile_cols] = full

        def row_of(slot):
            total = 0.0
            for part in split(edges[slot], terms):
                total += dot(part, across)
            return total[at : at + 1]

        def col_of(slot):
            total = 0.0
            for part in split(edges[slot], terms):
                total += dot_t(down, part)
            return total[:, at : at + 1]

        zeros = jnp.zeros((SUB, wide), jnp.float32)
        target[0:SUB, :] = zeros
        target[end : end + SUB, :] = zeros
        target[SUB - 1 : SUB, 0:tile_cols] = jnp.where(above, row_of(0), 0.0)
        target[end : end + 1, 0:tile_cols] = jnp.where(below, row_of(1), 0.0)
        target[SUB:end, tile_cols:wide] = side(col_of(2), col_of(3))

    for k in range(3):
        pad[k, SUB:end, 0:tile_cols] = fields[k]
        pad[k, 0:SUB, :] = jnp.zeros((SUB, wide), jnp.float32)
        pad[k, end : end + SUB, :] = jnp.zeros((SUB, wide), jnp.float32)
        pad[k, SUB - 1 : SUB, 0:tile_cols] = jnp.where(above, rowh[0, k : k + 1, :], 0.0)
        pad[k, end : end + 1, 0:tile_cols] = jnp.where(below, rowh[1, k : k + 1, :], 0.0)
        pad[k, SUB:end, tile_cols:wide] = side(
            edge_cols[:, k : k + 1], edge_cols[:, 3 + k : 4 + k]
        )

    window = chunk + 2 * SUB

    def west(x):
        return pltpu.roll(x, 1, 1)

    def east(x):
        return pltpu.roll(x, wide - 1, 1)

    def north(x):
        return pltpu.roll(x, 1, 0)

    def south(x):
        return pltpu.roll(x, x.shape[0] - 1, 0)

    def body(step, _):
        base = pl.multiple_of(step * chunk, SUB)
        at = pl.ds(base, window)
        h, hu, hv = pad[0, at, :], pad[1, at, :], pad[2, at, :]
        wet_w, bed_w = wet_p[at, :], bed_p[at, :]
        safe = jnp.where(wet_w > 0.5, h, 1.0)
        inverse = 1.0 / safe
        u, v = hu * inverse, hv * inverse
        speed = safe * lax.rsqrt(safe)
        pressure = 0.5 * gravity * safe * safe
        cross = hu * v

        def mid(x):
            return x[SUB : SUB + chunk]

        def narrow(x):
            return x[:, 0:tile_cols]

        h_n, hu_n, hv_n, wet_n, bed_n = [narrow(x) for x in (h, hu, hv, wet_w, bed_w)]
        gate = (0.5 * courant) * (north(wet_n) * wet_n)
        reach = narrow(jnp.abs(v) + speed)
        bound = jnp.maximum(north(reach), reach)
        totals = []
        for state, flux in (
            (h_n, hv_n), (hu_n, narrow(cross)), (hv_n, narrow(hv * v + pressure)),
        ):
            face = gate * ((north(flux) + flux) - bound * (state - north(state)))
            totals.append(mid(face) - mid(south(face)))
        slope = gate * (bed_n - north(bed_n))
        centre = mid(h_n)
        totals[2] -= gravity * centre * (mid(slope) + mid(south(slope)))

        h_m, hu_m, hv_m, wet_m, bed_m = [mid(x) for x in (h, hu, hv, wet_w, bed_w)]
        gate = (0.5 * courant) * (west(wet_m) * wet_m)
        reach = mid(jnp.abs(u) + speed)
        bound = jnp.maximum(west(reach), reach)
        for k, (state, flux) in enumerate(
            ((h_m, hu_m), (hu_m, mid(hu * u + pressure)), (hv_m, mid(cross)))
        ):
            face = gate * ((west(flux) + flux) - bound * (state - west(state)))
            totals[k] += narrow(face - east(face))
        slope = gate * (bed_m - west(bed_m))
        totals[1] -= gravity * centre * narrow(slope + east(slope))
        out = pl.ds(base, chunk)
        for k, state in enumerate((h_m, hu_m, hv_m)):
            fine[0, k, out, :] = narrow(state) + totals[k]
        return 0

    lax.fori_loop(0, tile_rows // chunk, body, 0)

    shift_r, shift_c = anchor[nest, 0], anchor[nest, 1]
    low = onehot(
        iota((2 * cell_rows, tile_rows), 1) // 3 + shift_r == iota((2 * cell_rows, tile_rows), 0)
    )
    wide_pick = onehot(
        iota((tile_cols, 2 * cell_cols), 0) // 3 + shift_c == iota((tile_cols, 2 * cell_cols), 1)
    )
    for k in range(3):
        part_rows = 0.0
        for part in split(fine[0, k], 2):
            part_rows += dot(low, part)
        placed = 0.0
        for part in split(part_rows, 2):
            placed += dot(part, wide_pick)
        placed = placed * (1.0 / 9.0)
        for a in range(2):
            for b in range(2):
                quads[2 * a + b, k] = placed[
                    a * cell_rows : (a + 1) * cell_rows, b * cell_cols : (b + 1) * cell_cols
                ]


def step(rows, cols, anchor, levels, fields, edge_cols, rowh, wet, cls, cellh):
    tile_rows, tile_cols = fields.shape[1:]
    cell_rows, cell_cols = wet.shape
    smem = pl.BlockSpec(memory_space=pltpu.SMEM)
    vmem = pl.BlockSpec(memory_space=pltpu.VMEM)
    f32 = jnp.float32
    padded = (tile_rows + 2 * SUB, tile_cols + LANES)
    return pl.pallas_call(
        functools.partial(step_kernel, rows, cols, 48),
        out_shape=(
            jax.ShapeDtypeStruct((1, 3, tile_rows, tile_cols), f32),
            jax.ShapeDtypeStruct((4, 3, cell_rows, cell_cols), f32),
        ),
        in_specs=[smem, smem] + [vmem] * 6,
        out_specs=(vmem, vmem),
        scratch_shapes=[
            pltpu.VMEM((3,) + padded, f32),
            pltpu.VMEM(wet.shape, f32),
            pltpu.VMEM(padded, f32),
            pltpu.VMEM(padded, f32),
        ],
        compiler_params=pltpu.CompilerParams(vmem_limit_bytes=40 * 1024 * 1024),
        name="step",
    )(anchor, levels, fields, edge_cols, rowh, wet, cls, cellh)


def feedback_kernel(nests, rows, cols, anchor, quads, coarse, out, held, send_sem, recv_sem):
    nest, row, col = lax.axis_index("nest"), lax.axis_index("row"), lax.axis_index("col")
    block = nest * rows + row
    blocks = nests * rows
    cell_rows, cell_cols = coarse.shape[1], coarse.shape[2]

    def place(b, c):
        return {"nest": b // rows, "row": lax.rem(b, rows), "col": c}

    links = []
    for quad in (1, 2, 3):
        db, dc = quad // 2, quad % 2
        sends = jnp.logical_and(block + db < blocks, col + dc < cols)
        takes = jnp.logical_and(block - db >= 0, col - dc >= 0)
        links.append((quad, sends, place(block + db, col + dc), takes, place(block - db, col - dc)))

    barrier = pltpu.get_barrier_semaphore()
    for _, _, _, takes, source in links:
        @pl.when(takes)
        def _(source=source):
            pl.semaphore_signal(barrier, inc=1, device_id=source, device_id_type=MESH)
    targets = sum(jnp.where(sends, 1, 0) for _, sends, _, _, _ in links)

    @pl.when(targets > 0)
    def _():
        pl.semaphore_wait(barrier, targets)

    def copy(quad, target):
        return pltpu.make_async_remote_copy(
            src_ref=quads.at[quad],
            dst_ref=held.at[quad - 1],
            send_sem=send_sem.at[quad - 1],
            recv_sem=recv_sem.at[quad - 1],
            device_id=target,
            device_id_type=MESH,
        )

    for quad, sends, target, _, _ in links:
        @pl.when(sends)
        def _(quad=quad, target=target):
            copy(quad, target).start()

    at_row = block * cell_rows + iota((cell_rows, cell_cols), 0)
    at_col = col * cell_cols + iota((cell_rows, cell_cols), 1)
    count = jnp.ones((cell_rows, cell_cols), jnp.float32)
    for n in range(nests):
        from_row = at_row - (n * rows * cell_rows + anchor[n, 0])
        from_col = at_col - anchor[n, 1]
        inside = (from_row >= 0) & (from_row < rows * cell_rows)
        inside &= (from_col >= 0) & (from_col < cols * cell_cols)
        count += jnp.where(inside, 1.0, 0.0)
    weight = 1.0 / count
    for k in range(3):
        out[k] = coarse[k] + quads[0, k]
    for quad, _, target, takes, _ in links:
        @pl.when(takes)
        def _(quad=quad, target=target):
            copy(quad, target).wait_recv()
            for k in range(3):
                out[k] += held[quad - 1, k]
    for k in range(3):
        out[k] = out[k] * weight
    for quad, sends, target, _, _ in links:
        @pl.when(sends)
        def _(quad=quad, target=target):
            copy(quad, target).wait_send()


def feedback(nests, rows, cols, anchor, quads, coarse):
    smem = pl.BlockSpec(memory_space=pltpu.SMEM)
    vmem = pl.BlockSpec(memory_space=pltpu.VMEM)
    return pl.pallas_call(
        functools.partial(feedback_kernel, nests, rows, cols),
        out_shape=jax.ShapeDtypeStruct(coarse.shape, jnp.float32),
        in_specs=[smem, vmem, vmem],
        out_specs=vmem,
        scratch_shapes=[
            pltpu.VMEM((3,) + coarse.shape, jnp.float32),
            pltpu.SemaphoreType.DMA((3,)),
            pltpu.SemaphoreType.DMA((3,)),
        ],
        compiler_params=pltpu.CompilerParams(collective_id=1, has_side_effects=True),
        name="feedback",
    )(anchor, quads, coarse)


def fused_kernel(
    nests, rows, cols, anchor_in, levels_in, strips, wet, cls, coarse, fine, out,
    anchor, levels, fine_sem, held, wet_v, cls_v, coarse_v, pad, wet_p, bed_p, colh, rowh, cellh,
    col_msg, row_msg, cell_msg, rest, above, spill, taken, load_sem,
    big_send, big_recv, col_send, col_recv, row_send, row_recv, cell_send, cell_recv,
    down_send, down_recv, side_send, side_recv,
):
    parts = rows * cols
    nest, row, col = lax.axis_index("nest"), lax.axis_index("row"), lax.axis_index("col")
    me = row * cols + col
    block, blocks = nest * rows + row, nests * rows
    band = strips.shape[4]
    tile_rows, tile_cols = fine.shape[2], fine.shape[3]
    cell_rows, cell_cols = wet_v.shape
    group = band // 3
    wide = tile_cols + LANES
    end = SUB + tile_rows
    has_above, has_below = row > 0, row < rows - 1
    has_left, has_right = col > 0, col < cols - 1

    loads = [
        pltpu.make_async_copy(strips.at[0, :, :, 0], held, load_sem.at[0]),
        pltpu.make_async_copy(wet.at[0], wet_v, load_sem.at[1]),
        pltpu.make_async_copy(cls.at[0], cls_v, load_sem.at[2]),
        pltpu.make_async_copy(coarse, coarse_v, load_sem.at[3]),
        pltpu.make_async_copy(anchor_in, anchor, load_sem.at[4]),
        pltpu.make_async_copy(levels_in, levels, load_sem.at[5]),
    ]
    for load in loads:
        load.start()

    def place(q):
        return {"row": q // cols, "col": lax.rem(q, cols)}

    barrier = pltpu.get_barrier_semaphore()
    to_next = jnp.logical_and(row == rows - 1, nest < nests - 1)
    to_last = jnp.logical_and(row == 0, nest > 0)
    below_id = {"nest": (block + 1) // rows, "row": lax.rem(block + 1, rows), "col": col}

    def greet(t, _):
        q = lax.rem(me + t, parts)
        pl.semaphore_signal(barrier, inc=1, device_id=place(q), device_id_type=MESH)
        return 0

    lax.fori_loop(1, parts, greet, 0)

    @pl.when(to_next)
    def _():
        pl.semaphore_signal(barrier, inc=1, device_id=below_id, device_id_type=MESH)

    @pl.when(to_last)
    def _():
        pl.semaphore_signal(
            barrier, inc=1, device_id={"nest": nest - 1, "row": rows - 1, "col": col},
            device_id_type=MESH,
        )

    peers = parts - 1 + jnp.where(to_next, 1, 0) + jnp.where(to_last, 1, 0)
    pl.semaphore_wait(barrier, peers)

    def columns(c):
        return pl.ds(pl.multiple_of(c * tile_cols, LANES), tile_cols)

    def landing(p):
        return pad.at[:, pl.ds(pl.multiple_of(SUB + p * band, SUB), band), 0:tile_cols]

    def big(q):
        return pltpu.make_async_remote_copy(
            src_ref=strips.at[0, :, q // cols, 0, :, columns(lax.rem(q, cols))],
            dst_ref=landing(me),
            send_sem=big_send.at[q],
            recv_sem=big_recv.at[me],
            device_id=place(q),
            device_id_type=MESH,
        )

    def big_start(t, _):
        big(lax.rem(me + t, parts)).start()
        return 0

    early = min(parts, HEAD)
    lax.fori_loop(1, early, big_start, 0)
    own = pltpu.make_async_copy(
        strips.at[0, :, row, 0, :, columns(col)], landing(me), big_recv.at[me]
    )
    own.start()

    loads[1].wait()
    loads[2].wait()
    for at, cells in enumerate((wet_v, cls_v)):
        cell_msg[0, at : at + 1, :] = cells[cell_rows - 1 : cell_rows, :]
        cell_msg[1, at : at + 1, :] = cells[0:1, :]
        across = cells[...].astype(jnp.float32).astype(jnp.bfloat16)
        pick = iota((SUB, cell_cols), 1)
        cell_msg[2, at : at + 1, :] = dot_t(onehot(pick == cell_cols - 1), across)[0:1].astype(jnp.int32)
        cell_msg[3, at : at + 1, :] = dot_t(onehot(pick == 0), across)[0:1].astype(jnp.int32)
    loads[0].wait()
    for j in range(rows):
        for k in range(3):
            row_msg[0, j, k : k + 1, :] = held[k, j, band - 1 : band, :]
            row_msg[1, j, k : k + 1, :] = held[k, j, 0:1, :]
    lane = iota((SUB, LANES), 1)
    first = onehot(lane == 0)
    last = onehot(lane == LANES - 1)
    slot_of = iota((SUB, band), 0)
    col_msg[...] = jnp.zeros_like(col_msg)
    for j in range(rows):
        for c in range(cols):
            message = jnp.zeros((SUB, band), jnp.float32)
            for k in range(3):
                if c > 0:
                    for part in split(held[k, j, :, c * tile_cols - LANES : c * tile_cols], 3):
                        message += jnp.where(slot_of == k, dot_t(last, part), 0.0)
                if c < cols - 1:
                    for part in split(
                        held[k, j, :, (c + 1) * tile_cols : (c + 1) * tile_cols + LANES], 3
                    ):
                        message += jnp.where(slot_of == 3 + k, dot_t(first, part), 0.0)
            col_msg[j * cols + c, :, 0:band] = message

    cell_links = (
        (0, has_below, {"row": row + 1, "col": col}, has_above),
        (1, has_above, {"row": row - 1, "col": col}, has_below),
        (2, has_right, {"row": row, "col": col + 1}, has_left),
        (3, has_left, {"row": row, "col": col - 1}, has_right),
    )

    def cell_copy(slot, target):
        return pltpu.make_async_remote_copy(
            src_ref=cell_msg.at[slot],
            dst_ref=cellh.at[slot],
            send_sem=cell_send.at[slot],
            recv_sem=cell_recv.at[slot],
            device_id=target,
            device_id_type=MESH,
        )

    for slot, sends, target, _ in cell_links:
        @pl.when(sends)
        def _(slot=slot, target=target):
            cell_copy(slot, target).start()

    def row_copy(slot, j, c):
        return pltpu.make_async_remote_copy(
            src_ref=row_msg.at[slot, j, :, c * tile_cols : (c + 1) * tile_cols],
            dst_ref=rowh.at[slot],
            send_sem=row_send.at[slot, j, c],
            recv_sem=row_recv.at[slot],
            device_id={"row": j + 1 if slot == 0 else j - 1, "col": c},
            device_id_type=MESH,
        )

    def row_own(slot, j, c):
        return pltpu.make_async_copy(
            row_msg.at[slot, j, :, c * tile_cols : (c + 1) * tile_cols],
            rowh.at[slot],
            row_recv.at[slot],
        )

    owner = (parts - 1, 0)

    def row_targets(slot):
        for j in range(rows):
            target_row = j + 1 if slot == 0 else j - 1
            if 0 <= target_row < rows:
                for c in range(cols):
                    yield j, c, target_row * cols + c == owner[slot]

    for slot in range(2):
        @pl.when(me == owner[slot])
        def _(slot=slot):
            for j, c, mine in row_targets(slot):
                (row_own if mine else row_copy)(slot, j, c).start()

    def col_copy(q):
        return pltpu.make_async_remote_copy(
            src_ref=col_msg.at[q],
            dst_ref=colh.at[me],
            send_sem=col_send.at[q],
            recv_sem=col_recv.at[me],
            device_id=place(q),
            device_id_type=MESH,
        )

    def col_start(t, _):
        col_copy(lax.rem(me + t, parts)).start()
        return 0

    lax.fori_loop(1, parts, col_start, 0)
    pltpu.make_async_copy(col_msg.at[me], colh.at[me], col_recv.at[me]).start()
    if early < parts:
        lax.fori_loop(early, parts, big_start, 0)

    loads[4].wait()
    loads[5].wait()

    def look(classes):
        bed = jnp.zeros(classes.shape, jnp.float32)
        for at in range(levels.shape[0]):
            bed = jnp.where(classes == at, levels[at], bed)
        return bed

    down = onehot(iota((tile_rows, cell_rows), 0) // 3 == iota((tile_rows, cell_rows), 1))
    across = onehot(iota((cell_cols, tile_cols), 1) // 3 == iota((cell_cols, tile_cols), 0))

    def side(low, high):
        lane = iota((low.shape[0], LANES), 1)
        low = jnp.where(has_left, low, 0.0)
        high = jnp.where(has_right, high, 0.0)
        return jnp.where(lane == 0, high, jnp.where(lane == LANES - 1, low, 0.0))

    inner = (wet_v[...].astype(jnp.float32), look(cls_v[...]))
    zeros = jnp.zeros((SUB, wide), jnp.float32)
    for target, cells, terms in ((wet_p, inner[0], 1), (bed_p, inner[1], 3)):
        full = 0.0
        for part in split(cells, terms):
            full += dot(dot(down, part).astype(jnp.bfloat16), across)
        target[SUB:end, 0:tile_cols] = full
        target[0:SUB, :] = zeros
        target[end : end + SUB, :] = zeros
    for k in range(3):
        pad[k, 0:SUB, :] = zeros
        pad[k, end : end + SUB, :] = zeros
        pad[k, SUB:end, tile_cols:wide] = jnp.zeros((tile_rows, LANES), jnp.float32)

    for slot, _, target, receives in cell_links:
        @pl.when(jnp.logical_not(receives))
        def _(slot=slot):
            cellh[slot] = jnp.zeros((SUB, LANES), jnp.int32)

        @pl.when(receives)
        def _(slot=slot, target=target):
            cell_copy(slot, target).wait_recv()

    sub = iota((SUB, LANES), 0)
    for target, at, terms in ((wet_p, 0, 1), (bed_p, 1, 3)):
        def edge_of(slot, at=at):
            cells = jnp.where(sub < 2, cellh[slot], 0)
            return cells.astype(jnp.float32) if at == 0 else look(cells)

        def row_of(slot, at=at, terms=terms):
            total = 0.0
            for part in split(edge_of(slot), terms):
                total += dot(part, across)
            return total[at : at + 1]

        def col_of(slot, at=at, terms=terms):
            total = 0.0
            for part in split(edge_of(slot), terms):
                total += dot_t(down, part)
            return total[:, at : at + 1]

        target[SUB - 1 : SUB, 0:tile_cols] = jnp.where(has_above, row_of(0), 0.0)
        target[end : end + 1, 0:tile_cols] = jnp.where(has_below, row_of(1), 0.0)
        target[SUB:end, tile_cols:wide] = side(col_of(2), col_of(3))

    for slot, receives, at in ((0, has_above, SUB - 1), (1, has_below, end)):
        @pl.when(receives)
        def _(slot=slot, at=at):
            row_own(slot, 0, 0).wait()
            for k in range(3):
                pad[k, at : at + 1, 0:tile_cols] = rowh[slot, k : k + 1, :]

    third = onehot(iota((group, band), 1) // 3 == iota((group, band), 0))
    pick = onehot(iota((tile_cols, cell_cols), 0) // 3 == iota((tile_cols, cell_cols), 1))
    unit = onehot(iota((band, LANES), 0) == iota((band, LANES), 1))
    window = band + 2 * SUB

    def west(x):
        return pltpu.roll(x, 1, 1)

    def east(x):
        return pltpu.roll(x, wide - 1, 1)

    def north(x):
        return pltpu.roll(x, 1, 0)

    def south(x):
        return pltpu.roll(x, x.shape[0] - 1, 0)

    def mid(x):
        return x[SUB : SUB + band]

    def narrow(x):
        return x[:, 0:tile_cols]

    def big_wait(b):
        pltpu.make_async_copy(landing(b), landing(b), big_recv.at[b]).wait()

    def rest_rows(ref, b):
        return ref.at[:, pl.ds(pl.multiple_of(b * group, SUB), group), :]

    def down_copy(b):
        return pltpu.make_async_remote_copy(
            src_ref=rest_rows(rest, b),
            dst_ref=rest_rows(above, b),
            send_sem=down_send.at[b],
            recv_sem=down_recv.at[b],
            device_id=below_id,
            device_id_type=MESH,
        )

    def band_at(s):
        return lax.rem(me - 1 - s + 2 * parts, parts)

    def body(s, _):
        b = band_at(s)

        @pl.when(s == 0)
        def _():
            big_wait(me)
            big_wait(band_at(0))

        @pl.when(s < parts - 2)
        def _():
            big_wait(band_at(s + 1))

        pltpu.make_async_copy(colh.at[b], colh.at[b], col_recv.at[b]).wait()
        base = pl.multiple_of(b * band, SUB)
        inside = pl.ds(pl.multiple_of(base + SUB, SUB), band)
        edges = 0.0
        for part in split(colh[b], 3):
            edges += dot_t(unit, part)
        for k in range(3):
            pad[k, inside, tile_cols:wide] = side(edges[:, k : k + 1], edges[:, 3 + k : 4 + k])

        at = pl.ds(base, window)
        h, hu, hv = pad[0, at, :], pad[1, at, :], pad[2, at, :]
        wet_w, bed_w = wet_p[at, :], bed_p[at, :]
        safe = jnp.where(wet_w > 0.5, h, 1.0)
        inverse = 1.0 / safe
        u, v = hu * inverse, hv * inverse
        speed = safe * lax.rsqrt(safe)
        pressure = 0.5 * gravity * safe * safe
        cross = hu * v

        h_n, hu_n, hv_n, wet_n, bed_n = [narrow(x) for x in (h, hu, hv, wet_w, bed_w)]
        gate = (0.5 * courant) * (north(wet_n) * wet_n)
        reach = narrow(jnp.abs(v) + speed)
        bound = jnp.maximum(north(reach), reach)
        totals = []
        for state, flux in (
            (h_n, hv_n), (hu_n, narrow(cross)), (hv_n, narrow(hv * v + pressure)),
        ):
            face = gate * ((north(flux) + flux) - bound * (state - north(state)))
            totals.append(mid(face) - mid(south(face)))
        slope = gate * (bed_n - north(bed_n))
        centre = mid(h_n)
        totals[2] -= gravity * centre * (mid(slope) + mid(south(slope)))

        h_m, hu_m, hv_m, wet_m, bed_m = [mid(x) for x in (h, hu, hv, wet_w, bed_w)]
        gate = (0.5 * courant) * (west(wet_m) * wet_m)
        reach = mid(jnp.abs(u) + speed)
        bound = jnp.maximum(west(reach), reach)
        for k, (state, flux) in enumerate(
            ((h_m, hu_m), (hu_m, mid(hu * u + pressure)), (hv_m, mid(cross)))
        ):
            face = gate * ((west(flux) + flux) - bound * (state - west(state)))
            totals[k] += narrow(face - east(face))
        slope = gate * (bed_m - west(bed_m))
        totals[1] -= gravity * centre * narrow(slope + east(slope))
        cells = pl.ds(pl.multiple_of(b * group, SUB), group)
        for k, state in enumerate((h_m, hu_m, hv_m)):
            value = narrow(state) + totals[k]
            fine[0, k, pl.ds(base, band), :] = value
            summed = 0.0
            for part in split(value, 2):
                summed += dot(third, part)
            mean = 0.0
            for part in split(summed, 2):
                mean += dot(part, pick)
            rest[k, cells, :] = mean * (1.0 / 9.0)

        @pl.when(jnp.logical_and(s > 0, block < blocks - 1))
        def _():
            down_copy(band_at(s - 1)).start()

        return 0

    lax.fori_loop(0, parts, body, 0)

    at_row = block * cell_rows + iota((cell_rows, cell_cols), 0)
    at_col = col * cell_cols + iota((cell_rows, cell_cols), 1)
    count = jnp.ones((cell_rows, cell_cols), jnp.float32)
    for n in range(nests):
        from_row = at_row - (n * rows * cell_rows + anchor[n, 0])
        from_col = at_col - anchor[n, 1]
        covered = (from_row >= 0) & (from_row < rows * cell_rows)
        covered &= (from_col >= 0) & (from_col < cols * cell_cols)
        count += jnp.where(covered, 1.0, 0.0)
    weight = 1.0 / count

    @pl.when(block < blocks - 1)
    def _():
        down_copy(me).start()

    @pl.when(block == 0)
    def _():
        above[...] = jnp.zeros_like(above)

    def down_wait(b, _):
        down_copy(b).wait_recv()
        return 0

    @pl.when(block > 0)
    def _():
        lax.fori_loop(0, parts, down_wait, 0)

    source = jnp.maximum(block - 1, 0) // rows
    r_at, r_from = iota((cell_rows, cell_rows), 0), iota((cell_rows, cell_rows), 1)
    low_own = onehot(r_from + anchor[nest, 0] == r_at)
    low_above = onehot(r_from + anchor[source, 0] == r_at + cell_rows)
    c_from, c_at = iota((cell_cols, 2 * cell_cols), 0), iota((cell_cols, 2 * cell_cols), 1)
    over_own = onehot(c_from + anchor[nest, 1] == c_at)
    over_above = onehot(c_from + anchor[source, 1] == c_at)

    def side_copy(k):
        return pltpu.make_async_remote_copy(
            src_ref=spill.at[k],
            dst_ref=taken.at[k],
            send_sem=side_send.at[k],
            recv_sem=side_recv.at[k],
            device_id={"col": col + 1},
            device_id_type=MESH,
        )

    def side_start(k):
        @pl.when(has_right)
        def _():
            side_copy(k).start()

    loads[3].wait()
    for k in range(3):
        placed = 0.0
        for cells, low, over in ((rest, low_own, over_own), (above, low_above, over_above)):
            moved = 0.0
            for part in split(cells[k], 2):
                moved += dot(low, part)
            for part in split(moved, 2):
                placed += dot(part, over)
        spill[k] = placed[:, cell_cols:]
        if k > 0:
            side_start(k - 1)
        out[k] = coarse_v[k] + placed[:, :cell_cols]
    side_start(2)
    for k in range(3):
        @pl.when(has_left)
        def _(k=k):
            side_copy(k).wait_recv()
            out[k] = (out[k] + taken[k]) * weight

        @pl.when(jnp.logical_not(has_left))
        def _(k=k):
            out[k] = out[k] * weight

    def leave(t, _):
        q = lax.rem(me + t, parts)
        big(q).wait_send()
        col_copy(q).wait_send()
        return 0

    lax.fori_loop(1, parts, leave, 0)

    for slot, sends, target, _ in cell_links:
        @pl.when(sends)
        def _(slot=slot, target=target):
            cell_copy(slot, target).wait_send()
    for slot in range(2):
        @pl.when(me == owner[slot])
        def _(slot=slot):
            for j, c, mine in row_targets(slot):
                if not mine:
                    row_copy(slot, j, c).wait_send()

    def down_leave(b, _):
        down_copy(b).wait_send()
        return 0

    @pl.when(block < blocks - 1)
    def _():
        lax.fori_loop(0, parts, down_leave, 0)

    @pl.when(has_right)
    def _():
        for k in range(3):
            side_copy(k).wait_send()


def fused(nests, rows, cols, strips, anchor, wet, cls, levels, coarse):
    parts = rows * cols
    blocks, band, full_cols = strips.shape[2], strips.shape[4], strips.shape[5]
    tile_rows, tile_cols = parts * band, full_cols // cols
    cells = wet.shape[1:]
    vmem = pl.BlockSpec(memory_space=pltpu.VMEM)
    hbm = pl.BlockSpec(memory_space=pltpu.HBM)
    dma = pltpu.SemaphoreType.DMA
    f32, i32 = jnp.float32, jnp.int32
    padded = (tile_rows + 2 * SUB, tile_cols + LANES)
    results = 4 * (3 * tile_rows * tile_cols + coarse.size)
    return pl.pallas_call(
        functools.partial(fused_kernel, nests, rows, cols),
        out_shape=(
            pltpu.VMEM((1, 3, tile_rows, tile_cols), f32),
            pltpu.VMEM(coarse.shape, f32),
        ),
        in_specs=[hbm] * 6,
        out_specs=(vmem, vmem),
        scratch_shapes=[
            pltpu.SMEM(anchor.shape, i32),
            pltpu.SMEM(levels.shape, f32),
            dma((parts,)),
            pltpu.VMEM((3, blocks, band, full_cols), f32),
            pltpu.VMEM(cells, i32),
            pltpu.VMEM(cells, i32),
            pltpu.VMEM(coarse.shape, f32),
            pltpu.VMEM((3,) + padded, f32),
            pltpu.VMEM(padded, f32),
            pltpu.VMEM(padded, f32),
            pltpu.VMEM((parts, SUB, LANES), f32),
            pltpu.VMEM((2, SUB, tile_cols), f32),
            pltpu.VMEM((4, SUB, LANES), i32),
            pltpu.VMEM((parts, SUB, LANES), f32),
            pltpu.VMEM((2, blocks, SUB, full_cols), f32),
            pltpu.VMEM((4, SUB, LANES), i32),
            pltpu.VMEM(coarse.shape, f32),
            pltpu.VMEM(coarse.shape, f32),
            pltpu.VMEM(coarse.shape, f32),
            pltpu.VMEM(coarse.shape, f32),
            dma((6,)),
            dma((parts,)), dma((parts,)), dma((parts,)), dma((parts,)),
            dma((2, rows, cols)), dma((2,)), dma((4,)), dma((4,)),
            dma((parts,)), dma((parts,)), dma((3,)), dma((3,)),
        ],
        compiler_params=pltpu.CompilerParams(
            collective_id=2, has_side_effects=True, vmem_limit_bytes=VMEM_BYTES - results
        ),
        name="fused",
    )(anchor, levels, strips, wet, cls, coarse)


def emit_kernel(fine, coarse, fine_out, coarse_out, sems):
    copies = [
        pltpu.make_async_copy(fine, fine_out, sems.at[0]),
        pltpu.make_async_copy(coarse, coarse_out, sems.at[1]),
    ]
    for copy in copies:
        copy.start()
    for copy in copies:
        copy.wait()


def emit(fine, coarse):
    vmem = pl.BlockSpec(memory_space=pltpu.VMEM)
    hbm = pl.BlockSpec(memory_space=pl.ANY)
    return pl.pallas_call(
        emit_kernel,
        out_shape=(
            jax.ShapeDtypeStruct(fine.shape, jnp.float32),
            jax.ShapeDtypeStruct(coarse.shape, jnp.float32),
        ),
        in_specs=[vmem, vmem],
        out_specs=(hbm, hbm),
        scratch_shapes=[pltpu.SemaphoreType.DMA((2,))],
        compiler_params=pltpu.CompilerParams(vmem_limit_bytes=4 * 2**20),
        name="emit",
    )(fine, coarse)


def local(nests, rows, cols, strips, anchor, wet_mask, bathy_index, bed_levels, coarse):
    band = strips.shape[4]
    if band % (3 * SUB) == 0:
        return emit(*fused(
            nests, rows, cols, strips, anchor, wet_mask, bathy_index, bed_levels, coarse
        ))
    fields, colh, rowh, cellh = exchange(rows, cols, strips, wet_mask, bathy_index)
    fields = fields.reshape(3, -1, fields.shape[3])
    edge_cols = colh[:, :, :band].transpose(0, 2, 1).reshape(-1, SUB)
    updated, quads = step(
        rows, cols, anchor, bed_levels, fields, edge_cols, rowh, wet_mask[0], bathy_index[0], cellh
    )
    return updated, feedback(nests, rows, cols, anchor, quads, coarse)


def solution(mesh):
    sizes = (mesh.shape["nest"], mesh.shape["row"], mesh.shape["col"])
    return jax.shard_map(
        functools.partial(local, *sizes),
        mesh=mesh,
        in_specs=(
            P("nest", None, None, ("row", "col"), None, None),
            P(),
            P("nest", "row", "col"),
            P("nest", "row", "col"),
            P(),
            P(None, ("nest", "row"), "col"),
        ),
        out_specs=(P("nest", None, "row", "col"), P(None, ("nest", "row"), "col")),
        check_vma=False,
    )
```

```python
import functools

import jax
import jax.numpy as jnp
from jax import lax
from jax.experimental import pallas as pl
from jax.experimental.pallas import tpu as pltpu
from jax.sharding import PartitionSpec as P

gravity = 1.0
courant = 0.2
MESH = pl.DeviceIdType.MESH
LANES = 128
SUB = 8
HEAD = 3
VMEM_BYTES = 67043328


def onehot(cond):
    return jnp.where(cond, 1.0, 0.0).astype(jnp.bfloat16)


def iota(shape, dim):
    return lax.broadcasted_iota(jnp.int32, shape, dim)


def dot(a, b):
    return jnp.dot(a, b, preferred_element_type=jnp.float32)


def dot_t(a, b):
    return lax.dot_general(
        a, b, (((1,), (1,)), ((), ())), preferred_element_type=jnp.float32
    )


def split(x, terms):
    parts = []
    for _ in range(terms):
        part = x.astype(jnp.bfloat16)
        parts.append(part)
        x = x - part.astype(jnp.float32)
    return parts


def exchange_kernel(
    rows, cols, strips, wet, cls, fields, colh, rowh, cellh,
    held, wet_v, cls_v, col_msg, row_msg, cell_msg, load_sem,
    big_send, big_recv, col_send, col_recv, row_send, row_recv, cell_send, cell_recv,
):
    parts = rows * cols
    row, col = lax.axis_index("row"), lax.axis_index("col")
    me = row * cols + col
    band = strips.shape[4]
    tile_cols = fields.shape[3]
    full_cols = strips.shape[5]

    loads = [
        pltpu.make_async_copy(strips.at[0, :, :, 0], held, load_sem.at[0]),
        pltpu.make_async_copy(wet.at[0], wet_v, load_sem.at[1]),
        pltpu.make_async_copy(cls.at[0], cls_v, load_sem.at[2]),
    ]
    for load in loads:
        load.start()

    def place(q):
        return {"row": q // cols, "col": lax.rem(q, cols)}

    barrier = pltpu.get_barrier_semaphore()

    def greet(t, _):
        q = lax.rem(me + t, parts)
        pl.semaphore_signal(barrier, inc=1, device_id=place(q), device_id_type=MESH)
        return 0

    lax.fori_loop(1, parts, greet, 0)
    pl.semaphore_wait(barrier, parts - 1)

    def columns(c):
        return pl.ds(pl.multiple_of(c * tile_cols, LANES), tile_cols)

    def big(q):
        return pltpu.make_async_remote_copy(
            src_ref=strips.at[0, :, q // cols, 0, :, columns(lax.rem(q, cols))],
            dst_ref=fields.at[:, me],
            send_sem=big_send.at[q],
            recv_sem=big_recv.at[me],
            device_id=place(q),
            device_id_type=MESH,
        )

    def big_start(t, _):
        big(lax.rem(me + t, parts)).start()
        return 0

    lax.fori_loop(1, parts, big_start, 0)
    own = pltpu.make_async_copy(
        strips.at[0, :, row, 0, :, columns(col)], fields.at[:, me], big_recv.at[me]
    )
    own.start()

    for load in loads:
        load.wait()
    lane = iota((SUB, LANES), 1)
    sub = iota((SUB, LANES), 0)
    first = onehot(lane == 0)
    last = onehot(lane == LANES - 1)
    even = iota((SUB, band), 0)
    for j in range(rows):
        for c in range(cols):
            message = jnp.zeros((SUB, band), jnp.float32)
            for k in range(3):
                if c > 0:
                    for part in split(held[k, j, :, c * tile_cols - LANES : c * tile_cols], 3):
                        message += jnp.where(even == k, dot_t(last, part), 0.0)
                if c < cols - 1:
                    for part in split(
                        held[k, j, :, (c + 1) * tile_cols : (c + 1) * tile_cols + LANES], 3
                    ):
                        message += jnp.where(even == 3 + k, dot_t(first, part), 0.0)
            col_msg[j * cols + c, :, 0:band] = message
    for j in range(rows):
        for k in range(3):
            row_msg[0, j, k : k + 1, :] = held[k, j, band - 1 : band, :]
            row_msg[1, j, k : k + 1, :] = held[k, j, 0:1, :]
    cell_rows = wet_v.shape[0]
    for at, cells in enumerate((wet_v, cls_v)):
        cell_msg[0, at : at + 1, :] = cells[cell_rows - 1 : cell_rows, :]
        cell_msg[1, at : at + 1, :] = cells[0:1, :]
        across = cells[...].astype(jnp.float32).astype(jnp.bfloat16)
        width = across.shape[1]
        pick = iota((SUB, width), 1)
        cell_msg[2, at : at + 1, :] = dot_t(onehot(pick == width - 1), across)[0:1].astype(jnp.int32)
        cell_msg[3, at : at + 1, :] = dot_t(onehot(pick == 0), across)[0:1].astype(jnp.int32)

    def col_copy(q):
        return pltpu.make_async_remote_copy(
            src_ref=col_msg.at[q],
            dst_ref=colh.at[me],
            send_sem=col_send.at[q],
            recv_sem=col_recv.at[me],
            device_id=place(q),
            device_id_type=MESH,
        )

    def col_start(t, _):
        col_copy(lax.rem(me + t, parts)).start()
        return 0

    lax.fori_loop(1, parts, col_start, 0)
    own_col = pltpu.make_async_copy(col_msg.at[me], colh.at[me], col_recv.at[me])
    own_col.start()

    cell_links = (
        (0, row < rows - 1, {"row": row + 1, "col": col}, row > 0),
        (1, row > 0, {"row": row - 1, "col": col}, row < rows - 1),
        (2, col < cols - 1, {"row": row, "col": col + 1}, col > 0),
        (3, col > 0, {"row": row, "col": col - 1}, col < cols - 1),
    )

    def cell_copy(slot, target):
        return pltpu.make_async_remote_copy(
            src_ref=cell_msg.at[slot],
            dst_ref=cellh.at[slot],
            send_sem=cell_send.at[slot],
            recv_sem=cell_recv.at[slot],
            device_id=target,
            device_id_type=MESH,
        )

    for slot, sends, target, _ in cell_links:
        @pl.when(sends)
        def _(slot=slot, target=target):
            cell_copy(slot, target).start()

    def row_copy(slot, j, c):
        target_row = j + 1 if slot == 0 else j - 1
        return pltpu.make_async_remote_copy(
            src_ref=row_msg.at[slot, j, :, c * tile_cols : (c + 1) * tile_cols],
            dst_ref=rowh.at[slot],
            send_sem=row_send.at[slot, j, c],
            recv_sem=row_recv.at[slot],
            device_id={"row": target_row, "col": c},
            device_id_type=MESH,
        )

    def row_own(slot, j, c):
        return pltpu.make_async_copy(
            row_msg.at[slot, j, :, c * tile_cols : (c + 1) * tile_cols],
            rowh.at[slot],
            row_recv.at[slot],
        )

    owner = (rows * cols - 1, 0)
    for slot in range(2):
        @pl.when(me == owner[slot])
        def _(slot=slot):
            for j in range(rows):
                target_row = j + 1 if slot == 0 else j - 1
                if target_row < 0 or target_row >= rows:
                    continue
                for c in range(cols):
                    if target_row * cols + c == owner[slot]:
                        row_own(slot, j, c).start()
                    else:
                        row_copy(slot, j, c).start()

    def arrive(t, _):
        q = lax.rem(me + t, parts)
        pltpu.make_async_copy(fields.at[:, q], fields.at[:, q], big_recv.at[q]).wait()
        pltpu.make_async_copy(colh.at[q], colh.at[q], col_recv.at[q]).wait()
        return 0

    lax.fori_loop(0, parts, arrive, 0)
    for slot, _, target, receives in cell_links:
        @pl.when(receives)
        def _(slot=slot, target=target):
            cell_copy(slot, target).wait_recv()

    for slot, receives in ((0, row > 0), (1, row < rows - 1)):
        @pl.when(receives)
        def _(slot=slot):
            row_own(slot, 0, 0).wait()

    def leave(t, _):
        q = lax.rem(me + t, parts)
        big(q).wait_send()
        col_copy(q).wait_send()
        return 0

    lax.fori_loop(1, parts, leave, 0)
    for slot, sends, target, _ in cell_links:
        @pl.when(sends)
        def _(slot=slot, target=target):
            cell_copy(slot, target).wait_send()
    for slot in range(2):
        @pl.when(me == owner[slot])
        def _(slot=slot):
            for j in range(rows):
                target_row = j + 1 if slot == 0 else j - 1
                if target_row < 0 or target_row >= rows:
                    continue
                for c in range(cols):
                    if target_row * cols + c != owner[slot]:
                        row_copy(slot, j, c).wait_send()


def exchange(rows, cols, strips, wet, cls):
    parts = rows * cols
    blocks, band, full_cols = strips.shape[2], strips.shape[4], strips.shape[5]
    tile_cols = full_cols // cols
    any_spec = pl.BlockSpec(memory_space=pl.ANY)
    dma = pltpu.SemaphoreType.DMA
    f32 = jnp.float32
    return pl.pallas_call(
        functools.partial(exchange_kernel, rows, cols),
        out_shape=(
            jax.ShapeDtypeStruct((3, parts, band, tile_cols), f32),
            jax.ShapeDtypeStruct((parts, SUB, LANES), f32),
            jax.ShapeDtypeStruct((2, SUB, tile_cols), f32),
            jax.ShapeDtypeStruct((4, SUB, LANES), jnp.int32),
        ),
        in_specs=[any_spec] * 3,
        out_specs=(any_spec,) * 4,
        scratch_shapes=[
            pltpu.VMEM((3, blocks, band, full_cols), f32),
            pltpu.VMEM(wet.shape[1:], jnp.int32),
            pltpu.VMEM(cls.shape[1:], jnp.int32),
            pltpu.VMEM((parts, SUB, LANES), f32),
            pltpu.VMEM((2, blocks, SUB, full_cols), f32),
            pltpu.VMEM((4, SUB, LANES), jnp.int32),
            dma((3,)),
            dma((parts,)), dma((parts,)), dma((parts,)), dma((parts,)),
            dma((2, rows, cols)), dma((2,)), dma((4,)), dma((4,)),
        ],
        compiler_params=pltpu.CompilerParams(collective_id=0, has_side_effects=True),
        name="exchange",
    )(strips, wet, cls)


def step_kernel(
    rows, cols, chunk, anchor, levels, fields, edge_cols, rowh, wet, cls, cellh,
    fine, quads, pad, bed_v, wet_p, bed_p,
):
    nest, row, col = lax.axis_index("nest"), lax.axis_index("row"), lax.axis_index("col")
    tile_rows, tile_cols = fields.shape[1], fields.shape[2]
    cell_rows, cell_cols = wet.shape
    wide = tile_cols + LANES
    above, below = row > 0, row < rows - 1
    left, right = col > 0, col < cols - 1
    end = SUB + tile_rows

    def look(classes):
        bed = jnp.zeros(classes.shape, jnp.float32)
        for at in range(levels.shape[0]):
            bed = jnp.where(classes == at, levels[at], bed)
        return bed

    down = onehot(iota((tile_rows, cell_rows), 0) // 3 == iota((tile_rows, cell_rows), 1))
    across = onehot(iota((cell_cols, tile_cols), 1) // 3 == iota((cell_cols, tile_cols), 0))
    lane = iota((tile_rows, LANES), 1)

    def side(low, high):
        low = jnp.where(left, low, 0.0)
        high = jnp.where(right, high, 0.0)
        return jnp.where(lane == 0, high, jnp.where(lane == LANES - 1, low, 0.0))

    edge = cellh[...]
    edge_bed = [look(edge[slot]) for slot in range(4)]
    edge_wet = [edge[slot].astype(jnp.float32) for slot in range(4)]
    bed_v[...] = look(cls[...])
    for target, inner, edges, at, terms in (
        (wet_p, wet[...].astype(jnp.float32), edge_wet, 0, 1),
        (bed_p, bed_v[...], edge_bed, 1, 3),
    ):
        full = 0.0
        for part in split(inner, terms):
            full += dot(dot(down, part).astype(jnp.bfloat16), across)
        target[SUB:end, 0:tile_cols] = full

        def row_of(slot):
            total = 0.0
            for part in split(edges[slot], terms):
                total += dot(part, across)
            return total[at : at + 1]

        def col_of(slot):
            total = 0.0
            for part in split(edges[slot], terms):
                total += dot_t(down, part)
            return total[:, at : at + 1]

        zeros = jnp.zeros((SUB, wide), jnp.float32)
        target[0:SUB, :] = zeros
        target[end : end + SUB, :] = zeros
        target[SUB - 1 : SUB, 0:tile_cols] = jnp.where(above, row_of(0), 0.0)
        target[end : end + 1, 0:tile_cols] = jnp.where(below, row_of(1), 0.0)
        target[SUB:end, tile_cols:wide] = side(col_of(2), col_of(3))

    for k in range(3):
        pad[k, SUB:end, 0:tile_cols] = fields[k]
        pad[k, 0:SUB, :] = jnp.zeros((SUB, wide), jnp.float32)
        pad[k, end : end + SUB, :] = jnp.zeros((SUB, wide), jnp.float32)
        pad[k, SUB - 1 : SUB, 0:tile_cols] = jnp.where(above, rowh[0, k : k + 1, :], 0.0)
        pad[k, end : end + 1, 0:tile_cols] = jnp.where(below, rowh[1, k : k + 1, :], 0.0)
        pad[k, SUB:end, tile_cols:wide] = side(
            edge_cols[:, k : k + 1], edge_cols[:, 3 + k : 4 + k]
        )

    window = chunk + 2 * SUB

    def west(x):
        return pltpu.roll(x, 1, 1)

    def east(x):
        return pltpu.roll(x, wide - 1, 1)

    def north(x):
        return pltpu.roll(x, 1, 0)

    def south(x):
        return pltpu.roll(x, x.shape[0] - 1, 0)

    def body(step, _):
        base = pl.multiple_of(step * chunk, SUB)
        at = pl.ds(base, window)
        h, hu, hv = pad[0, at, :], pad[1, at, :], pad[2, at, :]
        wet_w, bed_w = wet_p[at, :], bed_p[at, :]
        safe = jnp.where(wet_w > 0.5, h, 1.0)
        inverse = 1.0 / safe
        u, v = hu * inverse, hv * inverse
        speed = safe * lax.rsqrt(safe)
        pressure = 0.5 * gravity * safe * safe
        cross = hu * v

        def mid(x):
            return x[SUB : SUB + chunk]

        def narrow(x):
            return x[:, 0:tile_cols]

        h_n, hu_n, hv_n, wet_n, bed_n = [narrow(x) for x in (h, hu, hv, wet_w, bed_w)]
        gate = (0.5 * courant) * (north(wet_n) * wet_n)
        reach = narrow(jnp.abs(v) + speed)
        bound = jnp.maximum(north(reach), reach)
        totals = []
        for state, flux in (
            (h_n, hv_n), (hu_n, narrow(cross)), (hv_n, narrow(hv * v + pressure)),
        ):
            face = gate * ((north(flux) + flux) - bound * (state - north(state)))
            totals.append(mid(face) - mid(south(face)))
        slope = gate * (bed_n - north(bed_n))
        centre = mid(h_n)
        totals[2] -= gravity * centre * (mid(slope) + mid(south(slope)))

        h_m, hu_m, hv_m, wet_m, bed_m = [mid(x) for x in (h, hu, hv, wet_w, bed_w)]
        gate = (0.5 * courant) * (west(wet_m) * wet_m)
        reach = mid(jnp.abs(u) + speed)
        bound = jnp.maximum(west(reach), reach)
        for k, (state, flux) in enumerate(
            ((h_m, hu_m), (hu_m, mid(hu * u + pressure)), (hv_m, mid(cross)))
        ):
            face = gate * ((west(flux) + flux) - bound * (state - west(state)))
            totals[k] += narrow(face - east(face))
        slope = gate * (bed_m - west(bed_m))
        totals[1] -= gravity * centre * narrow(slope + east(slope))
        out = pl.ds(base, chunk)
        for k, state in enumerate((h_m, hu_m, hv_m)):
            fine[0, k, out, :] = narrow(state) + totals[k]
        return 0

    lax.fori_loop(0, tile_rows // chunk, body, 0)

    shift_r, shift_c = anchor[nest, 0], anchor[nest, 1]
    low = onehot(
        iota((2 * cell_rows, tile_rows), 1) // 3 + shift_r == iota((2 * cell_rows, tile_rows), 0)
    )
    wide_pick = onehot(
        iota((tile_cols, 2 * cell_cols), 0) // 3 + shift_c == iota((tile_cols, 2 * cell_cols), 1)
    )
    for k in range(3):
        part_rows = 0.0
        for part in split(fine[0, k], 2):
            part_rows += dot(low, part)
        placed = 0.0
        for part in split(part_rows, 2):
            placed += dot(part, wide_pick)
        placed = placed * (1.0 / 9.0)
        for a in range(2):
            for b in range(2):
                quads[2 * a + b, k] = placed[
                    a * cell_rows : (a + 1) * cell_rows, b * cell_cols : (b + 1) * cell_cols
                ]


def step(rows, cols, anchor, levels, fields, edge_cols, rowh, wet, cls, cellh):
    tile_rows, tile_cols = fields.shape[1:]
    cell_rows, cell_cols = wet.shape
    smem = pl.BlockSpec(memory_space=pltpu.SMEM)
    vmem = pl.BlockSpec(memory_space=pltpu.VMEM)
    f32 = jnp.float32
    padded = (tile_rows + 2 * SUB, tile_cols + LANES)
    return pl.pallas_call(
        functools.partial(step_kernel, rows, cols, 48),
        out_shape=(
            jax.ShapeDtypeStruct((1, 3, tile_rows, tile_cols), f32),
            jax.ShapeDtypeStruct((4, 3, cell_rows, cell_cols), f32),
        ),
        in_specs=[smem, smem] + [vmem] * 6,
        out_specs=(vmem, vmem),
        scratch_shapes=[
            pltpu.VMEM((3,) + padded, f32),
            pltpu.VMEM(wet.shape, f32),
            pltpu.VMEM(padded, f32),
            pltpu.VMEM(padded, f32),
        ],
        compiler_params=pltpu.CompilerParams(vmem_limit_bytes=40 * 1024 * 1024),
        name="step",
    )(anchor, levels, fields, edge_cols, rowh, wet, cls, cellh)


def feedback_kernel(nests, rows, cols, anchor, quads, coarse, out, held, send_sem, recv_sem):
    nest, row, col = lax.axis_index("nest"), lax.axis_index("row"), lax.axis_index("col")
    block = nest * rows + row
    blocks = nests * rows
    cell_rows, cell_cols = coarse.shape[1], coarse.shape[2]

    def place(b, c):
        return {"nest": b // rows, "row": lax.rem(b, rows), "col": c}

    links = []
    for quad in (1, 2, 3):
        db, dc = quad // 2, quad % 2
        sends = jnp.logical_and(block + db < blocks, col + dc < cols)
        takes = jnp.logical_and(block - db >= 0, col - dc >= 0)
        links.append((quad, sends, place(block + db, col + dc), takes, place(block - db, col - dc)))

    barrier = pltpu.get_barrier_semaphore()
    for _, _, _, takes, source in links:
        @pl.when(takes)
        def _(source=source):
            pl.semaphore_signal(barrier, inc=1, device_id=source, device_id_type=MESH)
    targets = sum(jnp.where(sends, 1, 0) for _, sends, _, _, _ in links)

    @pl.when(targets > 0)
    def _():
        pl.semaphore_wait(barrier, targets)

    def copy(quad, target):
        return pltpu.make_async_remote_copy(
            src_ref=quads.at[quad],
            dst_ref=held.at[quad - 1],
            send_sem=send_sem.at[quad - 1],
            recv_sem=recv_sem.at[quad - 1],
            device_id=target,
            device_id_type=MESH,
        )

    for quad, sends, target, _, _ in links:
        @pl.when(sends)
        def _(quad=quad, target=target):
            copy(quad, target).start()

    at_row = block * cell_rows + iota((cell_rows, cell_cols), 0)
    at_col = col * cell_cols + iota((cell_rows, cell_cols), 1)
    count = jnp.ones((cell_rows, cell_cols), jnp.float32)
    for n in range(nests):
        from_row = at_row - (n * rows * cell_rows + anchor[n, 0])
        from_col = at_col - anchor[n, 1]
        inside = (from_row >= 0) & (from_row < rows * cell_rows)
        inside &= (from_col >= 0) & (from_col < cols * cell_cols)
        count += jnp.where(inside, 1.0, 0.0)
    weight = 1.0 / count
    for k in range(3):
        out[k] = coarse[k] + quads[0, k]
    for quad, _, target, takes, _ in links:
        @pl.when(takes)
        def _(quad=quad, target=target):
            copy(quad, target).wait_recv()
            for k in range(3):
                out[k] += held[quad - 1, k]
    for k in range(3):
        out[k] = out[k] * weight
    for quad, sends, target, _, _ in links:
        @pl.when(sends)
        def _(quad=quad, target=target):
            copy(quad, target).wait_send()


def feedback(nests, rows, cols, anchor, quads, coarse):
    smem = pl.BlockSpec(memory_space=pltpu.SMEM)
    vmem = pl.BlockSpec(memory_space=pltpu.VMEM)
    return pl.pallas_call(
        functools.partial(feedback_kernel, nests, rows, cols),
        out_shape=jax.ShapeDtypeStruct(coarse.shape, jnp.float32),
        in_specs=[smem, vmem, vmem],
        out_specs=vmem,
        scratch_shapes=[
            pltpu.VMEM((3,) + coarse.shape, jnp.float32),
            pltpu.SemaphoreType.DMA((3,)),
            pltpu.SemaphoreType.DMA((3,)),
        ],
        compiler_params=pltpu.CompilerParams(collective_id=1, has_side_effects=True),
        name="feedback",
    )(anchor, quads, coarse)


def fused_kernel(
    nests, rows, cols, anchor_in, levels_in, strips, wet, cls, coarse, fine, out,
    anchor, levels, fine_sem, held, wet_v, cls_v, coarse_v, pad, wet_p, bed_p, colh, rowh, cellh,
    col_msg, row_msg, cell_msg, rest, left, above, corner, weight, load_sem,
    big_send, big_recv, col_send, col_recv, row_send, row_recv, cell_send, cell_recv,
    side_send, side_recv, down_send, down_recv, far_send, far_recv, ready,
):
    parts = rows * cols
    nest, row, col = lax.axis_index("nest"), lax.axis_index("row"), lax.axis_index("col")
    me = row * cols + col
    block, blocks = nest * rows + row, nests * rows
    band = strips.shape[4]
    tile_rows, tile_cols = fine.shape[2], fine.shape[3]
    cell_rows, cell_cols = wet_v.shape
    group = band // 3
    wide = tile_cols + LANES
    end = SUB + tile_rows
    has_above, has_below = row > 0, row < rows - 1
    has_left, has_right = col > 0, col < cols - 1
    has_last, has_next = block > 0, block < blocks - 1

    loads = [
        pltpu.make_async_copy(strips.at[0, :, :, 0], held, load_sem.at[0]),
        pltpu.make_async_copy(wet.at[0], wet_v, load_sem.at[1]),
        pltpu.make_async_copy(cls.at[0], cls_v, load_sem.at[2]),
        pltpu.make_async_copy(coarse, coarse_v, load_sem.at[3]),
        pltpu.make_async_copy(anchor_in, anchor, load_sem.at[4]),
        pltpu.make_async_copy(levels_in, levels, load_sem.at[5]),
    ]
    for load in loads:
        load.start()

    def place(q):
        return {"row": q // cols, "col": lax.rem(q, cols)}

    barrier = pltpu.get_barrier_semaphore()
    to_next = jnp.logical_and(row == rows - 1, nest < nests - 1)
    to_last = jnp.logical_and(row == 0, nest > 0)
    below_id = {"nest": (block + 1) // rows, "row": lax.rem(block + 1, rows), "col": col}

    def rank(q):
        r = q // cols
        return (r // 2 + lax.rem(r, 2) + lax.rem(q, cols)) * parts + q

    mine = rank(me)

    def greet(t, count):
        q = lax.rem(me + t, parts)
        later = rank(q) > mine

        @pl.when(later)
        def _():
            pl.semaphore_signal(barrier, inc=1, device_id=place(q), device_id_type=MESH)

        return count + jnp.where(later, 0, 1)

    for at, takes in ((col, to_last), (col - 1, jnp.logical_and(to_last, has_left))):
        @pl.when(takes)
        def _(at=at):
            pl.semaphore_signal(
                barrier, inc=1, device_id={"nest": nest - 1, "row": rows - 1, "col": at},
                device_id_type=MESH,
            )

    earlier = lax.fori_loop(1, parts, greet, 0) + jnp.where(to_next, 1, 0)
    earlier = earlier + jnp.where(jnp.logical_and(to_next, has_right), 1, 0)

    @pl.when(earlier > 0)
    def _():
        pl.semaphore_wait(barrier, earlier)

    def answer(t, _):
        q = lax.rem(me + t, parts)

        @pl.when(rank(q) < mine)
        def _():
            pl.semaphore_signal(ready.at[me], inc=1, device_id=place(q), device_id_type=MESH)

        return 0

    lax.fori_loop(1, parts, answer, 0)

    def meet(q):
        @pl.when(rank(q) > mine)
        def _():
            pl.semaphore_wait(ready.at[q], 1)

    def columns(c):
        return pl.ds(pl.multiple_of(c * tile_cols, LANES), tile_cols)

    def landing(p):
        return pad.at[:, pl.ds(pl.multiple_of(SUB + p * band, SUB), band), 0:tile_cols]

    def big(q):
        return pltpu.make_async_remote_copy(
            src_ref=strips.at[0, :, q // cols, 0, :, columns(lax.rem(q, cols))],
            dst_ref=landing(me),
            send_sem=big_send.at[0],
            recv_sem=big_recv.at[me],
            device_id=place(q),
            device_id_type=MESH,
        )

    def big_start(t, _):
        big(lax.rem(me + t, parts)).start()
        return 0

    def stride(n):
        if cols != 4:
            return n
        m = jnp.maximum(n - 2 * rows, 0)
        near = jnp.where(col == 0, 1, 3) + cols * (n - 1)
        far = jnp.where(col == 0, 2, 1) + lax.rem(m, 2) + cols * (m // 2)
        t = jnp.where(n <= rows, near, jnp.where(n < 2 * rows, cols * (n - rows), far))
        return jnp.where(jnp.logical_or(col == 1, col == 2), n, t)

    def first_start(n, _):
        t = stride(n)
        meet(lax.rem(me + t, parts))
        return big_start(t, 0)

    def next_start(n, _):
        return big_start(stride(n), 0)

    early = min(parts, HEAD)
    lax.fori_loop(1, early, first_start, 0)
    own = pltpu.make_async_copy(
        strips.at[0, :, row, 0, :, columns(col)], landing(me), big_recv.at[me]
    )
    own.start()

    loads[1].wait()
    loads[2].wait()
    for at, cells in enumerate((wet_v, cls_v)):
        cell_msg[0, at : at + 1, :] = cells[cell_rows - 1 : cell_rows, :]
        cell_msg[1, at : at + 1, :] = cells[0:1, :]
        across = cells[...].astype(jnp.float32).astype(jnp.bfloat16)
        pick = iota((SUB, cell_cols), 1)
        cell_msg[2, at : at + 1, :] = dot_t(onehot(pick == cell_cols - 1), across)[0:1].astype(jnp.int32)
        cell_msg[3, at : at + 1, :] = dot_t(onehot(pick == 0), across)[0:1].astype(jnp.int32)
    loads[0].wait()
    for j in range(rows):
        for k in range(3):
            row_msg[0, j, k : k + 1, :] = held[k, j, band - 1 : band, :]
            row_msg[1, j, k : k + 1, :] = held[k, j, 0:1, :]
    col_msg[...] = jnp.zeros_like(col_msg)
    lane = iota((3 * band, LANES), 1)
    for j in range(rows):
        for c in range(1, cols):
            at = c * tile_cols
            low = jnp.concatenate([held[k, j, :, at - LANES : at] for k in range(3)], axis=0)
            high = jnp.concatenate([held[k, j, :, at : at + LANES] for k in range(3)], axis=0)
            both = jnp.where(lane == 0, high, low).T
            col_msg[j * cols + c, 0:1, 0 : 3 * band] = both[LANES - 1 : LANES]
            col_msg[j * cols + c - 1, 1:2, 0 : 3 * band] = both[0:1]

    def rest_meet(n, _):
        meet(lax.rem(me + stride(n), parts))
        return 0

    if early < parts:
        lax.fori_loop(early, parts, rest_meet, 0)

    cell_links = (
        (0, has_below, {"row": row + 1, "col": col}, has_above),
        (1, has_above, {"row": row - 1, "col": col}, has_below),
        (2, has_right, {"row": row, "col": col + 1}, has_left),
        (3, has_left, {"row": row, "col": col - 1}, has_right),
    )

    def cell_copy(slot, target):
        return pltpu.make_async_remote_copy(
            src_ref=cell_msg.at[slot],
            dst_ref=cellh.at[slot],
            send_sem=cell_send.at[slot],
            recv_sem=cell_recv.at[slot],
            device_id=target,
            device_id_type=MESH,
        )

    for slot, sends, target, _ in cell_links:
        @pl.when(sends)
        def _(slot=slot, target=target):
            cell_copy(slot, target).start()

    def row_copy(slot, j, c):
        return pltpu.make_async_remote_copy(
            src_ref=row_msg.at[slot, j, :, c * tile_cols : (c + 1) * tile_cols],
            dst_ref=rowh.at[slot],
            send_sem=row_send.at[slot, j, c],
            recv_sem=row_recv.at[slot],
            device_id={"row": j + 1 if slot == 0 else j - 1, "col": c},
            device_id_type=MESH,
        )

    def row_own(slot, j, c):
        return pltpu.make_async_copy(
            row_msg.at[slot, j, :, c * tile_cols : (c + 1) * tile_cols],
            rowh.at[slot],
            row_recv.at[slot],
        )

    owner = (parts - 1, 0)

    def row_targets(slot):
        for j in range(rows):
            target_row = j + 1 if slot == 0 else j - 1
            if 0 <= target_row < rows:
                for c in range(cols):
                    yield j, c, target_row * cols + c == owner[slot]

    for slot in range(2):
        @pl.when(me == owner[slot])
        def _(slot=slot):
            for j, c, mine in row_targets(slot):
                (row_own if mine else row_copy)(slot, j, c).start()

    def col_copy(q):
        return pltpu.make_async_remote_copy(
            src_ref=col_msg.at[q],
            dst_ref=colh.at[me],
            send_sem=col_send.at[0],
            recv_sem=col_recv.at[me],
            device_id=place(q),
            device_id_type=MESH,
        )

    def col_start(n, _):
        col_copy(lax.rem(me + stride(n), parts)).start()
        return 0

    lax.fori_loop(1, parts, col_start, 0)
    pltpu.make_async_copy(col_msg.at[me], colh.at[me], col_recv.at[me]).start()
    if early < parts:
        lax.fori_loop(early, parts, next_start, 0)

    loads[4].wait()
    loads[5].wait()

    def look(classes):
        bed = jnp.zeros(classes.shape, jnp.float32)
        for at in range(levels.shape[0]):
            bed = jnp.where(classes == at, levels[at], bed)
        return bed

    down = onehot(iota((tile_rows, cell_rows), 0) // 3 == iota((tile_rows, cell_rows), 1))
    across = onehot(iota((cell_cols, tile_cols), 1) // 3 == iota((cell_cols, tile_cols), 0))

    def side(low, high):
        lane = iota((low.shape[0], LANES), 1)
        low = jnp.where(has_left, low, 0.0)
        high = jnp.where(has_right, high, 0.0)
        return jnp.where(lane == 0, high, jnp.where(lane == LANES - 1, low, 0.0))

    inner = (wet_v[...].astype(jnp.float32), look(cls_v[...]))
    zeros = jnp.zeros((SUB, wide), jnp.float32)
    for target, cells, terms in ((wet_p, inner[0], 1), (bed_p, inner[1], 3)):
        full = 0.0
        for part in split(cells, terms):
            full += dot(dot(down, part).astype(jnp.bfloat16), across)
        target[SUB:end, 0:tile_cols] = full
        target[0:SUB, :] = zeros
        target[end : end + SUB, :] = zeros
    for k in range(3):
        pad[k, 0:SUB, :] = zeros
        pad[k, end : end + SUB, :] = zeros
        pad[k, SUB:end, tile_cols:wide] = jnp.zeros((tile_rows, LANES), jnp.float32)

    for slot, _, target, receives in cell_links:
        @pl.when(jnp.logical_not(receives))
        def _(slot=slot):
            cellh[slot] = jnp.zeros((2, LANES), jnp.int32)

        @pl.when(receives)
        def _(slot=slot, target=target):
            cell_copy(slot, target).wait_recv()

    for target, at, terms in ((wet_p, 0, 1), (bed_p, 1, 3)):
        def edge_of(slot, at=at):
            cells = jnp.concatenate([cellh[slot], jnp.zeros((SUB - 2, LANES), jnp.int32)], axis=0)
            return cells.astype(jnp.float32) if at == 0 else look(cells)

        def row_of(slot, at=at, terms=terms):
            total = 0.0
            for part in split(edge_of(slot), terms):
                total += dot(part, across)
            return total[at : at + 1]

        def col_of(slot, at=at, terms=terms):
            total = 0.0
            for part in split(edge_of(slot), terms):
                total += dot_t(down, part)
            return total[:, at : at + 1]

        target[SUB - 1 : SUB, 0:tile_cols] = jnp.where(has_above, row_of(0), 0.0)
        target[end : end + 1, 0:tile_cols] = jnp.where(has_below, row_of(1), 0.0)
        target[SUB:end, tile_cols:wide] = side(col_of(2), col_of(3))

    at_row = block * cell_rows + iota((cell_rows, cell_cols), 0)
    at_col = col * cell_cols + iota((cell_rows, cell_cols), 1)
    count = jnp.ones((cell_rows, cell_cols), jnp.float32)
    for n in range(nests):
        from_row = at_row - (n * rows * cell_rows + anchor[n, 0])
        from_col = at_col - anchor[n, 1]
        covered = (from_row >= 0) & (from_row < rows * cell_rows)
        covered &= (from_col >= 0) & (from_col < cols * cell_cols)
        count += jnp.where(covered, 1.0, 0.0)
    weight[...] = 1.0 / count

    third = onehot(iota((3 * group, 3 * band), 1) // 3 == iota((3 * group, 3 * band), 0))
    pick = onehot(iota((tile_cols, cell_cols), 0) // 3 == iota((tile_cols, cell_cols), 1))
    window = band + 2 * SUB

    def west(x):
        return pltpu.roll(x, 1, 1)

    def east(x):
        return pltpu.roll(x, wide - 1, 1)

    def north(x):
        return pltpu.roll(x, 1, 0)

    def south(x):
        return pltpu.roll(x, x.shape[0] - 1, 0)

    def mid(x):
        return x[SUB : SUB + band]

    def narrow(x):
        return x[:, 0:tile_cols]

    def big_wait(b):
        pltpu.make_async_copy(landing(b), landing(b), big_recv.at[b]).wait()

    def rest_rows(ref, b):
        return ref.at[:, pl.ds(pl.multiple_of(b * group, SUB), group), :]

    def side_copy(b):
        return pltpu.make_async_remote_copy(
            src_ref=rest_rows(rest, b),
            dst_ref=rest_rows(left, b),
            send_sem=side_send.at[0],
            recv_sem=side_recv.at[0],
            device_id={"col": col + 1},
            device_id_type=MESH,
        )

    def down_copy(b):
        return pltpu.make_async_remote_copy(
            src_ref=rest_rows(rest, b),
            dst_ref=rest_rows(above, b),
            send_sem=down_send.at[0],
            recv_sem=down_recv.at[0],
            device_id=below_id,
            device_id_type=MESH,
        )

    def far_copy(b):
        return pltpu.make_async_remote_copy(
            src_ref=rest_rows(rest, b),
            dst_ref=rest_rows(corner, b),
            send_sem=far_send.at[0],
            recv_sem=far_recv.at[0],
            device_id={**below_id, "col": col + 1},
            device_id_type=MESH,
        )

    def share(s):
        b = band_at(s)

        @pl.when(has_right)
        def _():
            side_copy(b).start()

        @pl.when(has_next)
        def _():
            down_copy(b).start()

        @pl.when(jnp.logical_and(has_right, has_next))
        def _():
            far_copy(b).start()

    last_three = parts - 2
    if cols == 4:
        last_three = jnp.where(col == 1, parts - 2, jnp.where(col == 2, parts - 4, parts - 3))

    def turn(s, first):
        t = jnp.where(s < first - 1, s + 1, s + 4)
        return jnp.where(s < parts - 3, t, first + s - (parts - 3))

    def band_at(s):
        return lax.rem(me + parts - turn(s, last_three), parts)

    def restrict(b):
        rows_of = pl.ds(pl.multiple_of(b * band, SUB), band)
        value = jnp.concatenate([fine[0, k, rows_of, :] for k in range(3)], axis=0)
        narrowed = dot(jnp.concatenate(split(value, 2), axis=0), pick)
        mean = 0.0
        for part in split(narrowed[: 3 * band] + narrowed[3 * band :], 2):
            mean += dot(third, part)
        mean = mean * (1.0 / 9.0)
        cells = pl.ds(pl.multiple_of(b * group, SUB), group)
        for k in range(3):
            rest[k, cells, :] = mean[k * group : (k + 1) * group]

    def arrived(t):
        big_wait(lax.rem(me + parts - t, parts))

    def body(s, _):
        b = band_at(s)

        @pl.when(s > 1)
        def _():
            share(s - 2)

        @pl.when(s == 0)
        def _():
            big_wait(me)
            arrived(1)

        @pl.when(s < last_three - 1)
        def _():
            arrived(s + 2)

        @pl.when(s == last_three - 1)
        def _():
            def others(t, _):
                arrived(t)
                return 0

            lax.fori_loop(last_three + 2, parts, others, 0)

        @pl.when(s == parts - 3)
        def _():
            arrived(last_three + 1)

        pltpu.make_async_copy(colh.at[b], colh.at[b], col_recv.at[b]).wait()
        for slot, owner_band, receives, at in (
            (0, 0, has_above, SUB - 1), (1, parts - 1, has_below, end)
        ):
            @pl.when(jnp.logical_and(b == owner_band, receives))
            def _(slot=slot, at=at):
                row_own(slot, 0, 0).wait()
                for k in range(3):
                    pad[k, at : at + 1, 0:tile_cols] = rowh[slot, k : k + 1, :]

        base = pl.multiple_of(b * band, SUB)
        inside = pl.ds(pl.multiple_of(base + SUB, SUB), band)
        edges = jnp.concatenate([colh[b], jnp.zeros((SUB - 2, LANES), jnp.float32)], axis=0).T
        for k in range(3):
            edge = edges[k * band : (k + 1) * band]
            pad[k, inside, tile_cols:wide] = side(edge[:, 0:1], edge[:, 1:2])

        at = pl.ds(base, window)
        h, hu, hv = pad[0, at, :], pad[1, at, :], pad[2, at, :]
        wet_w, bed_w = wet_p[at, :], bed_p[at, :]
        safe = jnp.where(wet_w > 0.5, h, 1.0)
        inverse = 1.0 / safe
        u, v = hu * inverse, hv * inverse
        speed = safe * lax.rsqrt(safe)
        pressure = 0.5 * gravity * safe * safe
        cross = hu * v

        h_n, hu_n, hv_n, wet_n, bed_n = [narrow(x) for x in (h, hu, hv, wet_w, bed_w)]
        gate = (0.5 * courant) * (north(wet_n) * wet_n)
        reach = narrow(jnp.abs(v) + speed)
        bound = jnp.maximum(north(reach), reach)
        totals = []
        for state, flux in (
            (h_n, hv_n), (hu_n, narrow(cross)), (hv_n, narrow(hv * v + pressure)),
        ):
            face = gate * ((north(flux) + flux) - bound * (state - north(state)))
            totals.append(mid(face) - mid(south(face)))
        slope = gate * (bed_n - north(bed_n))
        centre = mid(h_n)
        totals[2] -= gravity * centre * (mid(slope) + mid(south(slope)))

        h_m, hu_m, hv_m, wet_m, bed_m = [mid(x) for x in (h, hu, hv, wet_w, bed_w)]
        gate = (0.5 * courant) * (west(wet_m) * wet_m)
        reach = mid(jnp.abs(u) + speed)
        bound = jnp.maximum(west(reach), reach)
        for k, (state, flux) in enumerate(
            ((h_m, hu_m), (hu_m, mid(hu * u + pressure)), (hv_m, mid(cross)))
        ):
            face = gate * ((west(flux) + flux) - bound * (state - west(state)))
            totals[k] += narrow(face - east(face))
        slope = gate * (bed_m - west(bed_m))
        totals[1] -= gravity * centre * narrow(slope + east(slope))
        for k, state in enumerate((h_m, hu_m, hv_m)):
            fine[0, k, pl.ds(base, band), :] = narrow(state) + totals[k]
        restrict(band_at(jnp.maximum(s - 1, 0)))
        return 0

    lax.fori_loop(0, parts, body, 0)
    share(parts - 2)
    restrict(band_at(parts - 1))

    source = jnp.maximum(block - 1, 0) // rows
    row_own, col_own = anchor[nest, 0], anchor[nest, 1]
    row_last, col_last = anchor[source, 0], anchor[source, 1]
    cell_row = iota((cell_rows, cell_cols), 0)
    cell_col = iota((cell_rows, cell_cols), 1)
    share(parts - 1)

    def settle(ref, sem):
        pltpu.make_async_copy(ref, ref, sem.at[0]).wait()

    def moved(cells, keep, by_col, from_row, by_row):
        cells = jnp.where(keep, pltpu.roll(cells, by_col, 1), 0.0)
        return jnp.where(from_row, pltpu.roll(cells, by_row, 0), 0.0)

    loads[3].wait()
    for k in range(3):
        out[k] = coarse_v[k] + moved(
            rest[k], cell_col >= col_own, col_own, cell_row >= row_own, row_own
        )

    @pl.when(has_left)
    def _():
        settle(left, side_recv)
        for k in range(3):
            out[k] += moved(left[k], cell_col < col_own, col_own, cell_row >= row_own, row_own)

    @pl.when(has_last)
    def _():
        settle(above, down_recv)
        for k in range(3):
            out[k] += moved(above[k], cell_col >= col_last, col_last, cell_row < row_last, row_last)

    @pl.when(jnp.logical_and(has_last, has_left))
    def _():
        settle(corner, far_recv)
        for k in range(3):
            out[k] += moved(corner[k], cell_col < col_last, col_last, cell_row < row_last, row_last)

    for k in range(3):
        out[k] = out[k] * weight[...]

    settle(pad.at[:, SUB : SUB + (parts - 1) * band, 0:tile_cols], big_send)
    settle(colh.at[0 : parts - 1], col_send)
    for slot, sends, target, _ in cell_links:
        @pl.when(sends)
        def _(slot=slot, target=target):
            cell_copy(slot, target).wait_send()
    for slot in range(2):
        @pl.when(me == owner[slot])
        def _(slot=slot):
            for j, c, mine in row_targets(slot):
                if not mine:
                    row_copy(slot, j, c).wait_send()

    @pl.when(has_right)
    def _():
        settle(rest, side_send)

    @pl.when(has_next)
    def _():
        settle(rest, down_send)

    @pl.when(jnp.logical_and(has_next, has_right))
    def _():
        settle(rest, far_send)


def fused(nests, rows, cols, strips, anchor, wet, cls, levels, coarse):
    parts = rows * cols
    blocks, band, full_cols = strips.shape[2], strips.shape[4], strips.shape[5]
    tile_rows, tile_cols = parts * band, full_cols // cols
    cells = wet.shape[1:]
    vmem = pl.BlockSpec(memory_space=pltpu.VMEM)
    hbm = pl.BlockSpec(memory_space=pltpu.HBM)
    dma = pltpu.SemaphoreType.DMA
    f32, i32 = jnp.float32, jnp.int32
    padded = (tile_rows + 2 * SUB, tile_cols + LANES)
    results = 4 * (3 * tile_rows * tile_cols + coarse.size)
    return pl.pallas_call(
        functools.partial(fused_kernel, nests, rows, cols),
        out_shape=(
            pltpu.VMEM((1, 3, tile_rows, tile_cols), f32),
            pltpu.VMEM(coarse.shape, f32),
        ),
        in_specs=[hbm] * 6,
        out_specs=(vmem, vmem),
        scratch_shapes=[
            pltpu.SMEM(anchor.shape, i32),
            pltpu.SMEM(levels.shape, f32),
            dma((parts,)),
            pltpu.VMEM((3, blocks, band, full_cols), f32),
            pltpu.VMEM(cells, i32),
            pltpu.VMEM(cells, i32),
            pltpu.VMEM(coarse.shape, f32),
            pltpu.VMEM((3,) + padded, f32),
            pltpu.VMEM(padded, f32),
            pltpu.VMEM(padded, f32),
            pltpu.VMEM((parts, 2, LANES), f32),
            pltpu.VMEM((2, 4, tile_cols), f32),
            pltpu.VMEM((4, 2, LANES), i32),
            pltpu.VMEM((parts, 2, LANES), f32),
            pltpu.VMEM((2, blocks, 4, full_cols), f32),
            pltpu.VMEM((4, 2, LANES), i32),
            pltpu.VMEM(coarse.shape, f32),
            pltpu.VMEM(coarse.shape, f32),
            pltpu.VMEM(coarse.shape, f32),
            pltpu.VMEM(coarse.shape, f32),
            pltpu.VMEM(cells, f32),
            dma((6,)),
            dma((1,)), dma((parts,)), dma((1,)), dma((parts,)),
            dma((2, rows, cols)), dma((2,)), dma((4,)), dma((4,)),
            dma((1,)), dma((1,)), dma((1,)), dma((1,)), dma((1,)), dma((1,)),
            pltpu.SemaphoreType.REGULAR((parts,)),
        ],
        compiler_params=pltpu.CompilerParams(
            collective_id=2, has_side_effects=True, vmem_limit_bytes=VMEM_BYTES - results
        ),
        name="fused",
    )(anchor, levels, strips, wet, cls, coarse)


def emit_kernel(fine, coarse, fine_out, coarse_out, sems):
    copies = [
        pltpu.make_async_copy(fine, fine_out, sems.at[0]),
        pltpu.make_async_copy(coarse, coarse_out, sems.at[1]),
    ]
    for copy in copies:
        copy.start()
    for copy in copies:
        copy.wait()


def emit(fine, coarse):
    vmem = pl.BlockSpec(memory_space=pltpu.VMEM)
    hbm = pl.BlockSpec(memory_space=pl.ANY)
    return pl.pallas_call(
        emit_kernel,
        out_shape=(
            jax.ShapeDtypeStruct(fine.shape, jnp.float32),
            jax.ShapeDtypeStruct(coarse.shape, jnp.float32),
        ),
        in_specs=[vmem, vmem],
        out_specs=(hbm, hbm),
        scratch_shapes=[pltpu.SemaphoreType.DMA((2,))],
        compiler_params=pltpu.CompilerParams(vmem_limit_bytes=4 * 2**20),
        name="emit",
    )(fine, coarse)


def local(nests, rows, cols, strips, anchor, wet_mask, bathy_index, bed_levels, coarse):
    band = strips.shape[4]
    if band % (3 * SUB) == 0 and 3 * band <= LANES and rows * cols > 4:
        return emit(*fused(
            nests, rows, cols, strips, anchor, wet_mask, bathy_index, bed_levels, coarse
        ))
    fields, colh, rowh, cellh = exchange(rows, cols, strips, wet_mask, bathy_index)
    fields = fields.reshape(3, -1, fields.shape[3])
    edge_cols = colh[:, :, :band].transpose(0, 2, 1).reshape(-1, SUB)
    updated, quads = step(
        rows, cols, anchor, bed_levels, fields, edge_cols, rowh, wet_mask[0], bathy_index[0], cellh
    )
    return updated, feedback(nests, rows, cols, anchor, quads, coarse)


def solution(mesh):
    sizes = (mesh.shape["nest"], mesh.shape["row"], mesh.shape["col"])
    return jax.shard_map(
        functools.partial(local, *sizes),
        mesh=mesh,
        in_specs=(
            P("nest", None, None, ("row", "col"), None, None),
            P(),
            P("nest", "row", "col"),
            P("nest", "row", "col"),
            P(),
            P(None, ("nest", "row"), "col"),
        ),
        out_specs=(P("nest", None, "row", "col"), P(None, ("nest", "row"), "col")),
        check_vma=False,
    )
```

```python
import functools

import jax
import jax.numpy as jnp
from jax import lax
from jax.experimental import pallas as pl
from jax.experimental.pallas import tpu as pltpu
from jax.sharding import PartitionSpec as P

gravity = 1.0
courant = 0.2
MESH = pl.DeviceIdType.MESH
LANES = 128
SUB = 8
HEAD = 3
DIRECT = 9
VMEM_BYTES = 67043328


def onehot(cond):
    return jnp.where(cond, 1.0, 0.0).astype(jnp.bfloat16)


def iota(shape, dim):
    return lax.broadcasted_iota(jnp.int32, shape, dim)


def dot(a, b):
    return jnp.dot(a, b, preferred_element_type=jnp.float32)


def dot_t(a, b):
    return lax.dot_general(
        a, b, (((1,), (1,)), ((), ())), preferred_element_type=jnp.float32
    )


def split(x, terms):
    parts = []
    for _ in range(terms):
        part = x.astype(jnp.bfloat16)
        parts.append(part)
        x = x - part.astype(jnp.float32)
    return parts


def exchange_kernel(
    rows, cols, strips, wet, cls, fields, colh, rowh, cellh,
    held, wet_v, cls_v, col_msg, row_msg, cell_msg, load_sem,
    big_send, big_recv, col_send, col_recv, row_send, row_recv, cell_send, cell_recv,
):
    parts = rows * cols
    row, col = lax.axis_index("row"), lax.axis_index("col")
    me = row * cols + col
    band = strips.shape[4]
    tile_cols = fields.shape[3]
    full_cols = strips.shape[5]

    loads = [
        pltpu.make_async_copy(strips.at[0, :, :, 0], held, load_sem.at[0]),
        pltpu.make_async_copy(wet.at[0], wet_v, load_sem.at[1]),
        pltpu.make_async_copy(cls.at[0], cls_v, load_sem.at[2]),
    ]
    for load in loads:
        load.start()

    def place(q):
        return {"row": q // cols, "col": lax.rem(q, cols)}

    barrier = pltpu.get_barrier_semaphore()

    def greet(t, _):
        q = lax.rem(me + t, parts)
        pl.semaphore_signal(barrier, inc=1, device_id=place(q), device_id_type=MESH)
        return 0

    lax.fori_loop(1, parts, greet, 0)
    pl.semaphore_wait(barrier, parts - 1)

    def columns(c):
        return pl.ds(pl.multiple_of(c * tile_cols, LANES), tile_cols)

    def big(q):
        return pltpu.make_async_remote_copy(
            src_ref=strips.at[0, :, q // cols, 0, :, columns(lax.rem(q, cols))],
            dst_ref=fields.at[:, me],
            send_sem=big_send.at[q],
            recv_sem=big_recv.at[me],
            device_id=place(q),
            device_id_type=MESH,
        )

    def big_start(t, _):
        big(lax.rem(me + t, parts)).start()
        return 0

    lax.fori_loop(1, parts, big_start, 0)
    own = pltpu.make_async_copy(
        strips.at[0, :, row, 0, :, columns(col)], fields.at[:, me], big_recv.at[me]
    )
    own.start()

    for load in loads:
        load.wait()
    lane = iota((SUB, LANES), 1)
    sub = iota((SUB, LANES), 0)
    first = onehot(lane == 0)
    last = onehot(lane == LANES - 1)
    even = iota((SUB, band), 0)
    for j in range(rows):
        for c in range(cols):
            message = jnp.zeros((SUB, band), jnp.float32)
            for k in range(3):
                if c > 0:
                    for part in split(held[k, j, :, c * tile_cols - LANES : c * tile_cols], 3):
                        message += jnp.where(even == k, dot_t(last, part), 0.0)
                if c < cols - 1:
                    for part in split(
                        held[k, j, :, (c + 1) * tile_cols : (c + 1) * tile_cols + LANES], 3
                    ):
                        message += jnp.where(even == 3 + k, dot_t(first, part), 0.0)
            col_msg[j * cols + c, :, 0:band] = message
    for j in range(rows):
        for k in range(3):
            row_msg[0, j, k : k + 1, :] = held[k, j, band - 1 : band, :]
            row_msg[1, j, k : k + 1, :] = held[k, j, 0:1, :]
    cell_rows = wet_v.shape[0]
    for at, cells in enumerate((wet_v, cls_v)):
        cell_msg[0, at : at + 1, :] = cells[cell_rows - 1 : cell_rows, :]
        cell_msg[1, at : at + 1, :] = cells[0:1, :]
        across = cells[...].astype(jnp.float32).astype(jnp.bfloat16)
        width = across.shape[1]
        pick = iota((SUB, width), 1)
        cell_msg[2, at : at + 1, :] = dot_t(onehot(pick == width - 1), across)[0:1].astype(jnp.int32)
        cell_msg[3, at : at + 1, :] = dot_t(onehot(pick == 0), across)[0:1].astype(jnp.int32)

    def col_copy(q):
        return pltpu.make_async_remote_copy(
            src_ref=col_msg.at[q],
            dst_ref=colh.at[me],
            send_sem=col_send.at[q],
            recv_sem=col_recv.at[me],
            device_id=place(q),
            device_id_type=MESH,
        )

    def col_start(t, _):
        col_copy(lax.rem(me + t, parts)).start()
        return 0

    lax.fori_loop(1, parts, col_start, 0)
    own_col = pltpu.make_async_copy(col_msg.at[me], colh.at[me], col_recv.at[me])
    own_col.start()

    cell_links = (
        (0, row < rows - 1, {"row": row + 1, "col": col}, row > 0),
        (1, row > 0, {"row": row - 1, "col": col}, row < rows - 1),
        (2, col < cols - 1, {"row": row, "col": col + 1}, col > 0),
        (3, col > 0, {"row": row, "col": col - 1}, col < cols - 1),
    )

    def cell_copy(slot, target):
        return pltpu.make_async_remote_copy(
            src_ref=cell_msg.at[slot],
            dst_ref=cellh.at[slot],
            send_sem=cell_send.at[slot],
            recv_sem=cell_recv.at[slot],
            device_id=target,
            device_id_type=MESH,
        )

    for slot, sends, target, _ in cell_links:
        @pl.when(sends)
        def _(slot=slot, target=target):
            cell_copy(slot, target).start()

    def row_copy(slot, j, c):
        target_row = j + 1 if slot == 0 else j - 1
        return pltpu.make_async_remote_copy(
            src_ref=row_msg.at[slot, j, :, c * tile_cols : (c + 1) * tile_cols],
            dst_ref=rowh.at[slot],
            send_sem=row_send.at[slot, j, c],
            recv_sem=row_recv.at[slot],
            device_id={"row": target_row, "col": c},
            device_id_type=MESH,
        )

    def row_own(slot, j, c):
        return pltpu.make_async_copy(
            row_msg.at[slot, j, :, c * tile_cols : (c + 1) * tile_cols],
            rowh.at[slot],
            row_recv.at[slot],
        )

    owner = (rows * cols - 1, 0)
    for slot in range(2):
        @pl.when(me == owner[slot])
        def _(slot=slot):
            for j in range(rows):
                target_row = j + 1 if slot == 0 else j - 1
                if target_row < 0 or target_row >= rows:
                    continue
                for c in range(cols):
                    if target_row * cols + c == owner[slot]:
                        row_own(slot, j, c).start()
                    else:
                        row_copy(slot, j, c).start()

    def arrive(t, _):
        q = lax.rem(me + t, parts)
        pltpu.make_async_copy(fields.at[:, q], fields.at[:, q], big_recv.at[q]).wait()
        pltpu.make_async_copy(colh.at[q], colh.at[q], col_recv.at[q]).wait()
        return 0

    lax.fori_loop(0, parts, arrive, 0)
    for slot, _, target, receives in cell_links:
        @pl.when(receives)
        def _(slot=slot, target=target):
            cell_copy(slot, target).wait_recv()

    for slot, receives in ((0, row > 0), (1, row < rows - 1)):
        @pl.when(receives)
        def _(slot=slot):
            row_own(slot, 0, 0).wait()

    def leave(t, _):
        q = lax.rem(me + t, parts)
        big(q).wait_send()
        col_copy(q).wait_send()
        return 0

    lax.fori_loop(1, parts, leave, 0)
    for slot, sends, target, _ in cell_links:
        @pl.when(sends)
        def _(slot=slot, target=target):
            cell_copy(slot, target).wait_send()
    for slot in range(2):
        @pl.when(me == owner[slot])
        def _(slot=slot):
            for j in range(rows):
                target_row = j + 1 if slot == 0 else j - 1
                if target_row < 0 or target_row >= rows:
                    continue
                for c in range(cols):
                    if target_row * cols + c != owner[slot]:
                        row_copy(slot, j, c).wait_send()


def exchange(rows, cols, strips, wet, cls):
    parts = rows * cols
    blocks, band, full_cols = strips.shape[2], strips.shape[4], strips.shape[5]
    tile_cols = full_cols // cols
    any_spec = pl.BlockSpec(memory_space=pl.ANY)
    dma = pltpu.SemaphoreType.DMA
    f32 = jnp.float32
    return pl.pallas_call(
        functools.partial(exchange_kernel, rows, cols),
        out_shape=(
            jax.ShapeDtypeStruct((3, parts, band, tile_cols), f32),
            jax.ShapeDtypeStruct((parts, SUB, LANES), f32),
            jax.ShapeDtypeStruct((2, SUB, tile_cols), f32),
            jax.ShapeDtypeStruct((4, SUB, LANES), jnp.int32),
        ),
        in_specs=[any_spec] * 3,
        out_specs=(any_spec,) * 4,
        scratch_shapes=[
            pltpu.VMEM((3, blocks, band, full_cols), f32),
            pltpu.VMEM(wet.shape[1:], jnp.int32),
            pltpu.VMEM(cls.shape[1:], jnp.int32),
            pltpu.VMEM((parts, SUB, LANES), f32),
            pltpu.VMEM((2, blocks, SUB, full_cols), f32),
            pltpu.VMEM((4, SUB, LANES), jnp.int32),
            dma((3,)),
            dma((parts,)), dma((parts,)), dma((parts,)), dma((parts,)),
            dma((2, rows, cols)), dma((2,)), dma((4,)), dma((4,)),
        ],
        compiler_params=pltpu.CompilerParams(collective_id=0, has_side_effects=True),
        name="exchange",
    )(strips, wet, cls)


def step_kernel(
    rows, cols, chunk, anchor, levels, fields, edge_cols, rowh, wet, cls, cellh,
    fine, quads, pad, bed_v, wet_p, bed_p,
):
    nest, row, col = lax.axis_index("nest"), lax.axis_index("row"), lax.axis_index("col")
    tile_rows, tile_cols = fields.shape[1], fields.shape[2]
    cell_rows, cell_cols = wet.shape
    wide = tile_cols + LANES
    above, below = row > 0, row < rows - 1
    left, right = col > 0, col < cols - 1
    end = SUB + tile_rows

    def look(classes):
        bed = jnp.zeros(classes.shape, jnp.float32)
        for at in range(levels.shape[0]):
            bed = jnp.where(classes == at, levels[at], bed)
        return bed

    down = onehot(iota((tile_rows, cell_rows), 0) // 3 == iota((tile_rows, cell_rows), 1))
    across = onehot(iota((cell_cols, tile_cols), 1) // 3 == iota((cell_cols, tile_cols), 0))
    lane = iota((tile_rows, LANES), 1)

    def side(low, high):
        low = jnp.where(left, low, 0.0)
        high = jnp.where(right, high, 0.0)
        return jnp.where(lane == 0, high, jnp.where(lane == LANES - 1, low, 0.0))

    edge = cellh[...]
    edge_bed = [look(edge[slot]) for slot in range(4)]
    edge_wet = [edge[slot].astype(jnp.float32) for slot in range(4)]
    bed_v[...] = look(cls[...])
    for target, inner, edges, at, terms in (
        (wet_p, wet[...].astype(jnp.float32), edge_wet, 0, 1),
        (bed_p, bed_v[...], edge_bed, 1, 3),
    ):
        full = 0.0
        for part in split(inner, terms):
            full += dot(dot(down, part).astype(jnp.bfloat16), across)
        target[SUB:end, 0:tile_cols] = full

        def row_of(slot):
            total = 0.0
            for part in split(edges[slot], terms):
                total += dot(part, across)
            return total[at : at + 1]

        def col_of(slot):
            total = 0.0
            for part in split(edges[slot], terms):
                total += dot_t(down, part)
            return total[:, at : at + 1]

        zeros = jnp.zeros((SUB, wide), jnp.float32)
        target[0:SUB, :] = zeros
        target[end : end + SUB, :] = zeros
        target[SUB - 1 : SUB, 0:tile_cols] = jnp.where(above, row_of(0), 0.0)
        target[end : end + 1, 0:tile_cols] = jnp.where(below, row_of(1), 0.0)
        target[SUB:end, tile_cols:wide] = side(col_of(2), col_of(3))

    for k in range(3):
        pad[k, SUB:end, 0:tile_cols] = fields[k]
        pad[k, 0:SUB, :] = jnp.zeros((SUB, wide), jnp.float32)
        pad[k, end : end + SUB, :] = jnp.zeros((SUB, wide), jnp.float32)
        pad[k, SUB - 1 : SUB, 0:tile_cols] = jnp.where(above, rowh[0, k : k + 1, :], 0.0)
        pad[k, end : end + 1, 0:tile_cols] = jnp.where(below, rowh[1, k : k + 1, :], 0.0)
        pad[k, SUB:end, tile_cols:wide] = side(
            edge_cols[:, k : k + 1], edge_cols[:, 3 + k : 4 + k]
        )

    window = chunk + 2 * SUB

    def west(x):
        return pltpu.roll(x, 1, 1)

    def east(x):
        return pltpu.roll(x, wide - 1, 1)

    def north(x):
        return pltpu.roll(x, 1, 0)

    def south(x):
        return pltpu.roll(x, x.shape[0] - 1, 0)

    def body(step, _):
        base = pl.multiple_of(step * chunk, SUB)
        at = pl.ds(base, window)
        h, hu, hv = pad[0, at, :], pad[1, at, :], pad[2, at, :]
        wet_w, bed_w = wet_p[at, :], bed_p[at, :]
        safe = jnp.where(wet_w > 0.5, h, 1.0)
        inverse = 1.0 / safe
        u, v = hu * inverse, hv * inverse
        speed = safe * lax.rsqrt(safe)
        pressure = 0.5 * gravity * safe * safe
        cross = hu * v

        def mid(x):
            return x[SUB : SUB + chunk]

        def narrow(x):
            return x[:, 0:tile_cols]

        h_n, hu_n, hv_n, wet_n, bed_n = [narrow(x) for x in (h, hu, hv, wet_w, bed_w)]
        gate = (0.5 * courant) * (north(wet_n) * wet_n)
        reach = narrow(jnp.abs(v) + speed)
        bound = jnp.maximum(north(reach), reach)
        totals = []
        for state, flux in (
            (h_n, hv_n), (hu_n, narrow(cross)), (hv_n, narrow(hv * v + pressure)),
        ):
            face = gate * ((north(flux) + flux) - bound * (state - north(state)))
            totals.append(mid(face) - mid(south(face)))
        slope = gate * (bed_n - north(bed_n))
        centre = mid(h_n)
        totals[2] -= gravity * centre * (mid(slope) + mid(south(slope)))

        h_m, hu_m, hv_m, wet_m, bed_m = [mid(x) for x in (h, hu, hv, wet_w, bed_w)]
        gate = (0.5 * courant) * (west(wet_m) * wet_m)
        reach = mid(jnp.abs(u) + speed)
        bound = jnp.maximum(west(reach), reach)
        for k, (state, flux) in enumerate(
            ((h_m, hu_m), (hu_m, mid(hu * u + pressure)), (hv_m, mid(cross)))
        ):
            face = gate * ((west(flux) + flux) - bound * (state - west(state)))
            totals[k] += narrow(face - east(face))
        slope = gate * (bed_m - west(bed_m))
        totals[1] -= gravity * centre * narrow(slope + east(slope))
        out = pl.ds(base, chunk)
        for k, state in enumerate((h_m, hu_m, hv_m)):
            fine[0, k, out, :] = narrow(state) + totals[k]
        return 0

    lax.fori_loop(0, tile_rows // chunk, body, 0)

    shift_r, shift_c = anchor[nest, 0], anchor[nest, 1]
    low = onehot(
        iota((2 * cell_rows, tile_rows), 1) // 3 + shift_r == iota((2 * cell_rows, tile_rows), 0)
    )
    wide_pick = onehot(
        iota((tile_cols, 2 * cell_cols), 0) // 3 + shift_c == iota((tile_cols, 2 * cell_cols), 1)
    )
    for k in range(3):
        part_rows = 0.0
        for part in split(fine[0, k], 2):
            part_rows += dot(low, part)
        placed = 0.0
        for part in split(part_rows, 2):
            placed += dot(part, wide_pick)
        placed = placed * (1.0 / 9.0)
        for a in range(2):
            for b in range(2):
                quads[2 * a + b, k] = placed[
                    a * cell_rows : (a + 1) * cell_rows, b * cell_cols : (b + 1) * cell_cols
                ]


def step(rows, cols, anchor, levels, fields, edge_cols, rowh, wet, cls, cellh):
    tile_rows, tile_cols = fields.shape[1:]
    cell_rows, cell_cols = wet.shape
    smem = pl.BlockSpec(memory_space=pltpu.SMEM)
    vmem = pl.BlockSpec(memory_space=pltpu.VMEM)
    f32 = jnp.float32
    padded = (tile_rows + 2 * SUB, tile_cols + LANES)
    return pl.pallas_call(
        functools.partial(step_kernel, rows, cols, 48),
        out_shape=(
            jax.ShapeDtypeStruct((1, 3, tile_rows, tile_cols), f32),
            jax.ShapeDtypeStruct((4, 3, cell_rows, cell_cols), f32),
        ),
        in_specs=[smem, smem] + [vmem] * 6,
        out_specs=(vmem, vmem),
        scratch_shapes=[
            pltpu.VMEM((3,) + padded, f32),
            pltpu.VMEM(wet.shape, f32),
            pltpu.VMEM(padded, f32),
            pltpu.VMEM(padded, f32),
        ],
        compiler_params=pltpu.CompilerParams(vmem_limit_bytes=40 * 1024 * 1024),
        name="step",
    )(anchor, levels, fields, edge_cols, rowh, wet, cls, cellh)


def feedback_kernel(nests, rows, cols, anchor, quads, coarse, out, held, send_sem, recv_sem):
    nest, row, col = lax.axis_index("nest"), lax.axis_index("row"), lax.axis_index("col")
    block = nest * rows + row
    blocks = nests * rows
    cell_rows, cell_cols = coarse.shape[1], coarse.shape[2]

    def place(b, c):
        return {"nest": b // rows, "row": lax.rem(b, rows), "col": c}

    links = []
    for quad in (1, 2, 3):
        db, dc = quad // 2, quad % 2
        sends = jnp.logical_and(block + db < blocks, col + dc < cols)
        takes = jnp.logical_and(block - db >= 0, col - dc >= 0)
        links.append((quad, sends, place(block + db, col + dc), takes, place(block - db, col - dc)))

    barrier = pltpu.get_barrier_semaphore()
    for _, _, _, takes, source in links:
        @pl.when(takes)
        def _(source=source):
            pl.semaphore_signal(barrier, inc=1, device_id=source, device_id_type=MESH)
    targets = sum(jnp.where(sends, 1, 0) for _, sends, _, _, _ in links)

    @pl.when(targets > 0)
    def _():
        pl.semaphore_wait(barrier, targets)

    def copy(quad, target):
        return pltpu.make_async_remote_copy(
            src_ref=quads.at[quad],
            dst_ref=held.at[quad - 1],
            send_sem=send_sem.at[quad - 1],
            recv_sem=recv_sem.at[quad - 1],
            device_id=target,
            device_id_type=MESH,
        )

    for quad, sends, target, _, _ in links:
        @pl.when(sends)
        def _(quad=quad, target=target):
            copy(quad, target).start()

    at_row = block * cell_rows + iota((cell_rows, cell_cols), 0)
    at_col = col * cell_cols + iota((cell_rows, cell_cols), 1)
    count = jnp.ones((cell_rows, cell_cols), jnp.float32)
    for n in range(nests):
        from_row = at_row - (n * rows * cell_rows + anchor[n, 0])
        from_col = at_col - anchor[n, 1]
        inside = (from_row >= 0) & (from_row < rows * cell_rows)
        inside &= (from_col >= 0) & (from_col < cols * cell_cols)
        count += jnp.where(inside, 1.0, 0.0)
    weight = 1.0 / count
    for k in range(3):
        out[k] = coarse[k] + quads[0, k]
    for quad, _, target, takes, _ in links:
        @pl.when(takes)
        def _(quad=quad, target=target):
            copy(quad, target).wait_recv()
            for k in range(3):
                out[k] += held[quad - 1, k]
    for k in range(3):
        out[k] = out[k] * weight
    for quad, sends, target, _, _ in links:
        @pl.when(sends)
        def _(quad=quad, target=target):
            copy(quad, target).wait_send()


def feedback(nests, rows, cols, anchor, quads, coarse):
    smem = pl.BlockSpec(memory_space=pltpu.SMEM)
    vmem = pl.BlockSpec(memory_space=pltpu.VMEM)
    return pl.pallas_call(
        functools.partial(feedback_kernel, nests, rows, cols),
        out_shape=jax.ShapeDtypeStruct(coarse.shape, jnp.float32),
        in_specs=[smem, vmem, vmem],
        out_specs=vmem,
        scratch_shapes=[
            pltpu.VMEM((3,) + coarse.shape, jnp.float32),
            pltpu.SemaphoreType.DMA((3,)),
            pltpu.SemaphoreType.DMA((3,)),
        ],
        compiler_params=pltpu.CompilerParams(collective_id=1, has_side_effects=True),
        name="feedback",
    )(anchor, quads, coarse)


def fused_kernel(
    nests, rows, cols, anchor_in, levels_in, strips, wet, cls, coarse, fine, out,
    anchor, levels, fine_sem, held, wet_v, cls_v, coarse_v, pad, wet_p, bed_p, colh, rowh, cellh,
    col_msg, row_msg, cell_msg, rest, left, above, corner, weight, load_sem,
    big_send, big_recv, col_send, col_recv, row_send, row_recv, cell_send, cell_recv,
    side_send, side_recv, down_send, down_recv, far_send, far_recv, relay_send, ready,
):
    parts = rows * cols
    nest, row, col = lax.axis_index("nest"), lax.axis_index("row"), lax.axis_index("col")
    me = row * cols + col
    block, blocks = nest * rows + row, nests * rows
    band = strips.shape[4]
    tile_rows, tile_cols = fine.shape[2], fine.shape[3]
    cell_rows, cell_cols = wet_v.shape
    group = band // 3
    wide = tile_cols + LANES
    end = SUB + tile_rows
    has_above, has_below = row > 0, row < rows - 1
    has_left, has_right = col > 0, col < cols - 1
    has_last, has_next = block > 0, block < blocks - 1

    loads = [
        pltpu.make_async_copy(strips.at[0, :, :, 0], held, load_sem.at[0]),
        pltpu.make_async_copy(wet.at[0], wet_v, load_sem.at[1]),
        pltpu.make_async_copy(cls.at[0], cls_v, load_sem.at[2]),
        pltpu.make_async_copy(coarse, coarse_v, load_sem.at[3]),
        pltpu.make_async_copy(anchor_in, anchor, load_sem.at[4]),
        pltpu.make_async_copy(levels_in, levels, load_sem.at[5]),
    ]
    for load in loads:
        load.start()

    def place(q):
        return {"row": q // cols, "col": lax.rem(q, cols)}

    barrier = pltpu.get_barrier_semaphore()
    to_next = jnp.logical_and(row == rows - 1, nest < nests - 1)
    to_last = jnp.logical_and(row == 0, nest > 0)
    below_id = {"nest": (block + 1) // rows, "row": lax.rem(block + 1, rows), "col": col}

    def rank(q):
        r = q // cols
        return (r // 2 + lax.rem(r, 2) + lax.rem(q, cols)) * parts + q

    mine = rank(me)

    def stride(n, col=col):
        if cols != 4:
            return n
        m = jnp.maximum(n - 2 * rows, 0)
        near = jnp.where(col == 0, 1, 3) + cols * (n - 1)
        far = jnp.where(col == 0, 2, 1) + lax.rem(m, 2) + cols * (m // 2)
        t = jnp.where(n <= rows, near, jnp.where(n < 2 * rows, cols * (n - rows), far))
        first = jnp.where(lax.rem(n, cols) == 0, n + 1 - cols, n + 1)
        first = jnp.where(n == parts - 1, parts + 1 - cols, first)
        return jnp.where(col == 1, n, jnp.where(col == 2, first, t))

    early = min(parts, HEAD)

    def turn_of(source, q):
        at = early - 1
        for n in range(early - 1, 0, -1):
            hit = lax.rem(source + stride(n, lax.rem(source, cols)), parts) == q
            at = jnp.where(hit, n - 1, at)
        return at

    def greet(t, count):
        q = lax.rem(me + t, parts)
        later = rank(q) > mine

        @pl.when(later)
        def _():
            pl.semaphore_signal(barrier, inc=1, device_id=place(q), device_id_type=MESH)

        return count + jnp.where(later, 0, 1)

    for at, takes in ((col, to_last), (col - 1, jnp.logical_and(to_last, has_left))):
        @pl.when(takes)
        def _(at=at):
            pl.semaphore_signal(
                barrier, inc=1, device_id={"nest": nest - 1, "row": rows - 1, "col": at},
                device_id_type=MESH,
            )

    earlier = lax.fori_loop(1, parts, greet, 0) + jnp.where(to_next, 1, 0)
    earlier = earlier + jnp.where(jnp.logical_and(to_next, has_right), 1, 0)

    @pl.when(earlier > 0)
    def _():
        pl.semaphore_wait(barrier, earlier)

    def answer(t, _):
        q = lax.rem(me + t, parts)

        @pl.when(rank(q) < mine)
        def _():
            pl.semaphore_signal(
                ready.at[turn_of(q, me)], inc=1, device_id=place(q), device_id_type=MESH
            )

        return 0

    lax.fori_loop(1, parts, answer, 0)

    def meet(n):
        @pl.when(rank(lax.rem(me + stride(n), parts)) > mine)
        def _():
            pl.semaphore_wait(ready.at[n - 1], 1)

    def columns(c):
        return pl.ds(pl.multiple_of(c * tile_cols, LANES), tile_cols)

    def landing(p):
        return pad.at[:, pl.ds(pl.multiple_of(SUB + p * band, SUB), band), 0:tile_cols]

    def big(q):
        return pltpu.make_async_remote_copy(
            src_ref=strips.at[0, :, q // cols, 0, :, columns(lax.rem(q, cols))],
            dst_ref=landing(me),
            send_sem=big_send.at[0],
            recv_sem=big_recv.at[me],
            device_id=place(q),
            device_id_type=MESH,
        )

    def big_start(t, _):
        big(lax.rem(me + t, parts)).start()
        return 0

    def first_start(n, _):
        meet(n)
        return big_start(stride(n), 0)

    def next_start(n, _):
        return big_start(stride(n), 0)

    lax.fori_loop(1, early, first_start, 0)
    own = pltpu.make_async_copy(
        strips.at[0, :, row, 0, :, columns(col)], landing(me), big_recv.at[me]
    )
    own.start()

    loads[1].wait()
    loads[2].wait()
    for at, cells in enumerate((wet_v, cls_v)):
        cell_msg[0, at : at + 1, :] = cells[cell_rows - 1 : cell_rows, :]
        cell_msg[1, at : at + 1, :] = cells[0:1, :]
        across = cells[...].astype(jnp.float32).astype(jnp.bfloat16)
        pick = iota((SUB, cell_cols), 1)
        cell_msg[2, at : at + 1, :] = dot_t(onehot(pick == cell_cols - 1), across)[0:1].astype(jnp.int32)
        cell_msg[3, at : at + 1, :] = dot_t(onehot(pick == 0), across)[0:1].astype(jnp.int32)
    loads[0].wait()
    for j in range(rows):
        for k in range(3):
            row_msg[0, j, k : k + 1, :] = held[k, j, band - 1 : band, :]
            row_msg[1, j, k : k + 1, :] = held[k, j, 0:1, :]
    col_msg[...] = jnp.zeros_like(col_msg)
    lane = iota((3 * band, LANES), 1)
    for j in range(rows):
        for c in range(1, cols):
            at = c * tile_cols
            low = jnp.concatenate([held[k, j, :, at - LANES : at] for k in range(3)], axis=0)
            high = jnp.concatenate([held[k, j, :, at : at + LANES] for k in range(3)], axis=0)
            both = jnp.where(lane == 0, high, low).T
            col_msg[j * cols + c, 0:1, 0 : 3 * band] = both[LANES - 1 : LANES]
            col_msg[j * cols + c - 1, 1:2, 0 : 3 * band] = both[0:1]

    def later(n, count):
        return count + jnp.where(rank(lax.rem(me + stride(n), parts)) > mine, 1, 0)

    rest_of = lax.fori_loop(early, parts, later, 0)

    @pl.when(rest_of > 0)
    def _():
        pl.semaphore_wait(ready.at[early - 1], rest_of)

    cell_links = (
        (0, has_below, {"row": row + 1, "col": col}, has_above),
        (1, has_above, {"row": row - 1, "col": col}, has_below),
        (2, has_right, {"row": row, "col": col + 1}, has_left),
        (3, has_left, {"row": row, "col": col - 1}, has_right),
    )

    def cell_copy(slot, target):
        return pltpu.make_async_remote_copy(
            src_ref=cell_msg.at[slot],
            dst_ref=cellh.at[slot],
            send_sem=cell_send.at[slot],
            recv_sem=cell_recv.at[slot],
            device_id=target,
            device_id_type=MESH,
        )

    for slot, sends, target, _ in cell_links:
        @pl.when(sends)
        def _(slot=slot, target=target):
            cell_copy(slot, target).start()

    def row_copy(slot, j, c):
        return pltpu.make_async_remote_copy(
            src_ref=row_msg.at[slot, j, :, c * tile_cols : (c + 1) * tile_cols],
            dst_ref=rowh.at[slot],
            send_sem=row_send.at[j],
            recv_sem=row_recv.at[slot],
            device_id={"row": j + 1 if slot == 0 else j - 1, "col": c},
            device_id_type=MESH,
        )

    def row_own(slot, j, c):
        return pltpu.make_async_copy(
            row_msg.at[slot, j, :, c * tile_cols : (c + 1) * tile_cols],
            rowh.at[slot],
            row_recv.at[slot],
        )

    owner = (parts - 1, 0)

    def row_targets(slot):
        for j in range(rows):
            target_row = j + 1 if slot == 0 else j - 1
            if 0 <= target_row < rows:
                for c in range(cols):
                    yield j, c, target_row * cols + c == owner[slot]

    for slot in range(2):
        @pl.when(me == owner[slot])
        def _(slot=slot):
            for j, c, mine in row_targets(slot):
                (row_own if mine else row_copy)(slot, j, c).start()

    def col_copy(q):
        return pltpu.make_async_remote_copy(
            src_ref=col_msg.at[q],
            dst_ref=colh.at[me],
            send_sem=col_send.at[0],
            recv_sem=col_recv.at[0],
            device_id=place(q),
            device_id_type=MESH,
        )

    def col_start(n, _):
        col_copy(lax.rem(me + stride(n), parts)).start()
        return 0

    lax.fori_loop(1, parts, col_start, 0)
    pltpu.make_async_copy(col_msg.at[me], colh.at[me], col_recv.at[0]).start()
    if early < parts:
        lax.fori_loop(early, parts, next_start, 0)

    loads[4].wait()
    loads[5].wait()

    def look(classes):
        bed = jnp.zeros(classes.shape, jnp.float32)
        for at in range(levels.shape[0]):
            bed = jnp.where(classes == at, levels[at], bed)
        return bed

    down = onehot(iota((tile_rows, cell_rows), 0) // 3 == iota((tile_rows, cell_rows), 1))
    across = onehot(iota((cell_cols, tile_cols), 1) // 3 == iota((cell_cols, tile_cols), 0))

    def side(low, high):
        lane = iota((low.shape[0], LANES), 1)
        low = jnp.where(has_left, low, 0.0)
        high = jnp.where(has_right, high, 0.0)
        return jnp.where(lane == 0, high, jnp.where(lane == LANES - 1, low, 0.0))

    inner = (wet_v[...].astype(jnp.float32), look(cls_v[...]))
    zeros = jnp.zeros((SUB, wide), jnp.float32)
    for target, cells, terms in ((wet_p, inner[0], 1), (bed_p, inner[1], 3)):
        full = 0.0
        for part in split(cells, terms):
            full += dot(dot(down, part).astype(jnp.bfloat16), across)
        target[SUB:end, 0:tile_cols] = full
        target[0:SUB, :] = zeros
        target[end : end + SUB, :] = zeros
    for k in range(3):
        pad[k, 0:SUB, :] = zeros
        pad[k, end : end + SUB, :] = zeros

    for slot, _, target, receives in cell_links:
        @pl.when(jnp.logical_not(receives))
        def _(slot=slot):
            cellh[slot] = jnp.zeros((2, LANES), jnp.int32)

        @pl.when(receives)
        def _(slot=slot, target=target):
            cell_copy(slot, target).wait_recv()

    for target, at, terms in ((wet_p, 0, 1), (bed_p, 1, 3)):
        def edge_of(slot, at=at):
            cells = jnp.concatenate([cellh[slot], jnp.zeros((SUB - 2, LANES), jnp.int32)], axis=0)
            return cells.astype(jnp.float32) if at == 0 else look(cells)

        def row_of(slot, at=at, terms=terms):
            total = 0.0
            for part in split(edge_of(slot), terms):
                total += dot(part, across)
            return total[at : at + 1]

        def col_of(slot, at=at, terms=terms):
            total = 0.0
            for part in split(edge_of(slot), terms):
                total += dot_t(down, part)
            return total[:, at : at + 1]

        target[SUB - 1 : SUB, 0:tile_cols] = jnp.where(has_above, row_of(0), 0.0)
        target[end : end + 1, 0:tile_cols] = jnp.where(has_below, row_of(1), 0.0)
        target[SUB:end, tile_cols:wide] = side(col_of(2), col_of(3))

    def settle(ref, sem):
        pltpu.make_async_copy(ref, ref, sem.at[0]).wait()

    settle(colh, col_recv)
    edges = jnp.concatenate([colh[b] for b in range(parts)], axis=0).T
    for k in range(3):
        edge = edges[k * band : (k + 1) * band]
        for b in range(parts):
            top = SUB + b * band
            pad[k, top : top + band, tile_cols:wide] = side(
                edge[:, 2 * b : 2 * b + 1], edge[:, 2 * b + 1 : 2 * b + 2]
            )

    at_row = block * cell_rows + iota((cell_rows, cell_cols), 0)
    at_col = col * cell_cols + iota((cell_rows, cell_cols), 1)
    count = jnp.ones((cell_rows, cell_cols), jnp.float32)
    for n in range(nests):
        from_row = at_row - (n * rows * cell_rows + anchor[n, 0])
        from_col = at_col - anchor[n, 1]
        covered = (from_row >= 0) & (from_row < rows * cell_rows)
        covered &= (from_col >= 0) & (from_col < cols * cell_cols)
        count += jnp.where(covered, 1.0, 0.0)
    weight[...] = 1.0 / count

    pick = onehot(iota((tile_cols, cell_cols), 0) // 3 == iota((tile_cols, cell_cols), 1))

    def west(x):
        return pltpu.roll(x, 1, 1)

    def east(x):
        return pltpu.roll(x, wide - 1, 1)

    def north(x):
        return pltpu.roll(x, 1, 0)

    def south(x):
        return pltpu.roll(x, x.shape[0] - 1, 0)

    def narrow(x):
        return x[:, 0:tile_cols]

    def big_wait(b):
        pltpu.make_async_copy(landing(b), landing(b), big_recv.at[b]).wait()

    def rest_rows(ref, b):
        return ref.at[:, pl.ds(pl.multiple_of(b * group, SUB), group), :]

    middle = cols // 2

    def side_copy(b, slot):
        return pltpu.make_async_remote_copy(
            src_ref=rest_rows(rest, b),
            dst_ref=rest_rows(left, b),
            send_sem=side_send.at[0],
            recv_sem=side_recv.at[slot],
            device_id={"col": col + 1},
            device_id_type=MESH,
        )

    def down_copy(b):
        return pltpu.make_async_remote_copy(
            src_ref=rest_rows(rest, b),
            dst_ref=rest_rows(above, b),
            send_sem=down_send.at[0],
            recv_sem=down_recv.at[0],
            device_id=below_id,
            device_id_type=MESH,
        )

    def far_copy(b):
        return pltpu.make_async_remote_copy(
            src_ref=rest_rows(rest, b),
            dst_ref=rest_rows(corner, b),
            send_sem=far_send.at[0],
            recv_sem=far_recv.at[0],
            device_id={**below_id, "col": col + 1},
            device_id_type=MESH,
        )

    def relay_copy(b):
        return pltpu.make_async_remote_copy(
            src_ref=rest_rows(left, b),
            dst_ref=rest_rows(corner, b),
            send_sem=relay_send.at[0],
            recv_sem=far_recv.at[0],
            device_id=below_id,
            device_id_type=MESH,
        )

    def share(s):
        b = band_at(s)

        @pl.when(jnp.logical_and(has_right, col + 1 != middle))
        def _():
            side_copy(b, parts).start()

        @pl.when(has_next)
        def _():
            down_copy(b).start()

        @pl.when(jnp.logical_and(jnp.logical_and(has_right, has_next), col + 1 != middle))
        def _():
            far_copy(b).start()

    def share_middle(first, last):
        def one(s, _):
            b = band_at(s)
            side_copy(b, jnp.where(s < parts - DIRECT, b, parts)).start()

            @pl.when(jnp.logical_and(has_next, s >= parts - DIRECT))
            def _():
                far_copy(b).start()

            return 0

        @pl.when(col + 1 == middle)
        def _():
            lax.fori_loop(first, last, one, 0)

    last_three = parts - 2
    if cols == 4:
        last_three = jnp.where(col == 1, parts - 2, jnp.where(col == 2, parts - 4, parts - 3))

    def turn(s, first):
        t = jnp.where(s < first - 1, s + 1, s + 4)
        return jnp.where(s < parts - 3, t, first + s - (parts - 3))

    def band_at(s):
        return lax.rem(me + parts - turn(s, last_three), parts)

    def advance(base, count):
        def mid(x):
            return x[SUB : SUB + count]

        base = pl.multiple_of(base, SUB)
        at = pl.ds(base, count + 2 * SUB)
        h, hu, hv = pad[0, at, :], pad[1, at, :], pad[2, at, :]
        wet_w, bed_w = wet_p[at, :], bed_p[at, :]
        safe = jnp.where(wet_w > 0.5, h, 1.0)
        inverse = 1.0 / safe
        u, v = hu * inverse, hv * inverse
        speed = safe * lax.rsqrt(safe)
        pressure = 0.5 * gravity * safe * safe
        cross = hu * v

        h_n, hu_n, hv_n, wet_n, bed_n = [narrow(x) for x in (h, hu, hv, wet_w, bed_w)]
        gate = (0.5 * courant) * (north(wet_n) * wet_n)
        reach = narrow(jnp.abs(v) + speed)
        bound = jnp.maximum(north(reach), reach)
        totals = []
        for state, flux in (
            (h_n, hv_n), (hu_n, narrow(cross)), (hv_n, narrow(hv * v + pressure)),
        ):
            face = gate * ((north(flux) + flux) - bound * (state - north(state)))
            totals.append(mid(face) - mid(south(face)))
        slope = gate * (bed_n - north(bed_n))
        centre = mid(h_n)
        totals[2] -= gravity * centre * (mid(slope) + mid(south(slope)))

        h_m, hu_m, hv_m, wet_m, bed_m = [mid(x) for x in (h, hu, hv, wet_w, bed_w)]
        gate = (0.5 * courant) * (west(wet_m) * wet_m)
        reach = mid(jnp.abs(u) + speed)
        bound = jnp.maximum(west(reach), reach)
        for k, (state, flux) in enumerate(
            ((h_m, hu_m), (hu_m, mid(hu * u + pressure)), (hv_m, mid(cross)))
        ):
            face = gate * ((west(flux) + flux) - bound * (state - west(state)))
            totals[k] += narrow(face - east(face))
        slope = gate * (bed_m - west(bed_m))
        totals[1] -= gravity * centre * narrow(slope + east(slope))
        for k, state in enumerate((h_m, hu_m, hv_m)):
            fine[0, k, pl.ds(base, count), :] = narrow(state) + totals[k]

    def restrict(base, count):
        rows_of = pl.ds(pl.multiple_of(base, SUB), count)
        value = jnp.concatenate([fine[0, k, rows_of, :] for k in range(3)], axis=0)
        narrowed = dot(jnp.concatenate(split(value, 2), axis=0), pick)
        third = onehot(iota((count, 3 * count), 1) // 3 == iota((count, 3 * count), 0))
        mean = 0.0
        for part in split(narrowed[: 3 * count] + narrowed[3 * count :], 2):
            mean += dot(third, part)
        mean = mean * (1.0 / 9.0)
        cells = pl.ds(pl.multiple_of(base // 3, SUB), count // 3)
        for k in range(3):
            rest[k, cells, :] = mean[k * count // 3 : (k + 1) * count // 3]

    def arrived(t):
        big_wait(lax.rem(me + parts - t, parts))

    def halo(lowest, highest):
        for slot, edge, receives, at in ((0, 0, has_above, SUB - 1), (1, parts - 1, has_below, end)):
            here = jnp.logical_and(lowest <= edge, edge <= highest)

            @pl.when(jnp.logical_and(here, receives))
            def _(slot=slot, at=at):
                row_own(slot, 0, 0).wait()
                for k in range(3):
                    pad[k, at : at + 1, 0:tile_cols] = rowh[slot, k : k + 1, :]

    def body(s, _):
        b = band_at(s)

        @pl.when(s > 1)
        def _():
            share(s - 2)

        @pl.when(s == 0)
        def _():
            big_wait(me)
            arrived(1)

        @pl.when(s < last_three - 1)
        def _():
            arrived(s + 2)

        @pl.when(s == last_three - 1)
        def _():
            def others(t, _):
                arrived(t)
                return 0

            lax.fori_loop(last_three + 2, parts, others, 0)

        halo(b, b)
        advance(b * band, band)
        restrict(band_at(jnp.maximum(s - 1, 0)) * band, band)
        return 0

    lax.fori_loop(0, parts - 3, body, 0)
    share(parts - 5)
    share_middle(0, parts - 4)
    restrict(band_at(parts - 4) * band, band)
    arrived(last_three + 1)
    share(parts - 4)
    share_middle(parts - 4, parts - 3)
    lowest = band_at(parts - 1)
    halo(lowest, lowest + 2)
    advance(lowest * band, 3 * band)
    restrict(lowest * band, 3 * band)
    for s in range(parts - 3, parts):
        share(s)
    share_middle(parts - 3, parts)

    source = jnp.maximum(block - 1, 0) // rows
    row_own, col_own = anchor[nest, 0], anchor[nest, 1]
    row_last, col_last = anchor[source, 0], anchor[source, 1]
    cell_row = iota((cell_rows, cell_cols), 0)
    cell_col = iota((cell_rows, cell_cols), 1)
    def moved(cells, keep, by_col, from_row, by_row):
        cells = jnp.where(keep, pltpu.roll(cells, by_col, 1), 0.0)
        return jnp.where(from_row, pltpu.roll(cells, by_row, 0), 0.0)

    loads[3].wait()
    for k in range(3):
        out[k] = coarse_v[k] + moved(
            rest[k], cell_col >= col_own, col_own, cell_row >= row_own, row_own
        )

    left_three = parts - 2 if cols == 4 else last_three

    def relay(t, _):
        b = lax.rem(me + 2 * parts - 1 - turn(t, left_three), parts)
        pltpu.make_async_copy(rest_rows(left, b), rest_rows(left, b), side_recv.at[b]).wait()

        @pl.when(has_next)
        def _():
            relay_copy(b).start()

        return 0

    few = DIRECT * group

    @pl.when(jnp.logical_and(has_left, col == middle))
    def _():
        lax.fori_loop(0, parts - DIRECT, relay, 0)
        pltpu.make_async_copy(rest.at[:, :few], left.at[:, :few], side_recv.at[parts]).wait()

    @pl.when(jnp.logical_and(has_left, col != middle))
    def _():
        pltpu.make_async_copy(rest, left, side_recv.at[parts]).wait()

    @pl.when(has_left)
    def _():
        for k in range(3):
            out[k] += moved(left[k], cell_col < col_own, col_own, cell_row >= row_own, row_own)

    @pl.when(has_last)
    def _():
        settle(above, down_recv)
        for k in range(3):
            out[k] += moved(above[k], cell_col >= col_last, col_last, cell_row < row_last, row_last)

    @pl.when(jnp.logical_and(has_last, has_left))
    def _():
        settle(corner, far_recv)
        for k in range(3):
            out[k] += moved(corner[k], cell_col < col_last, col_last, cell_row < row_last, row_last)

    for k in range(3):
        out[k] = out[k] * weight[...]

    settle(pad.at[:, SUB : SUB + (parts - 1) * band, 0:tile_cols], big_send)
    settle(colh.at[0 : parts - 1], col_send)
    for slot, sends, target, _ in cell_links:
        @pl.when(sends)
        def _(slot=slot, target=target):
            cell_copy(slot, target).wait_send()
    for slot in range(2):
        @pl.when(me == owner[slot])
        def _(slot=slot):
            for row_at in range(rows):
                n = sum(j == row_at and not mine for j, _, mine in row_targets(slot))
                if n > 0:
                    sent = row_msg.at[slot, row_at, :, 0 : n * tile_cols]
                    pltpu.make_async_copy(sent, sent, row_send.at[row_at]).wait()

    @pl.when(has_right)
    def _():
        settle(rest, side_send)

    @pl.when(has_next)
    def _():
        settle(rest, down_send)

    @pl.when(jnp.logical_and(jnp.logical_and(has_next, has_right), col + 1 != middle))
    def _():
        settle(rest, far_send)

    @pl.when(jnp.logical_and(jnp.logical_and(has_next, has_right), col + 1 == middle))
    def _():
        settle(rest.at[:, :few], far_send)

    @pl.when(jnp.logical_and(jnp.logical_and(has_next, has_left), col == middle))
    def _():
        settle(rest.at[:, few:], relay_send)


def fused(nests, rows, cols, strips, anchor, wet, cls, levels, coarse):
    parts = rows * cols
    blocks, band, full_cols = strips.shape[2], strips.shape[4], strips.shape[5]
    tile_rows, tile_cols = parts * band, full_cols // cols
    cells = wet.shape[1:]
    vmem = pl.BlockSpec(memory_space=pltpu.VMEM)
    hbm = pl.BlockSpec(memory_space=pltpu.HBM)
    dma = pltpu.SemaphoreType.DMA
    f32, i32 = jnp.float32, jnp.int32
    padded = (tile_rows + 2 * SUB, tile_cols + LANES)
    results = 4 * (3 * tile_rows * tile_cols + coarse.size)
    return pl.pallas_call(
        functools.partial(fused_kernel, nests, rows, cols),
        out_shape=(
            pltpu.VMEM((1, 3, tile_rows, tile_cols), f32),
            pltpu.VMEM(coarse.shape, f32),
        ),
        in_specs=[hbm] * 6,
        out_specs=(vmem, vmem),
        scratch_shapes=[
            pltpu.SMEM(anchor.shape, i32),
            pltpu.SMEM(levels.shape, f32),
            dma((parts,)),
            pltpu.VMEM((3, blocks, band, full_cols), f32),
            pltpu.VMEM(cells, i32),
            pltpu.VMEM(cells, i32),
            pltpu.VMEM(coarse.shape, f32),
            pltpu.VMEM((3,) + padded, f32),
            pltpu.VMEM(padded, f32),
            pltpu.VMEM(padded, f32),
            pltpu.VMEM((parts, 2, LANES), f32),
            pltpu.VMEM((2, 4, tile_cols), f32),
            pltpu.VMEM((4, 2, LANES), i32),
            pltpu.VMEM((parts, 2, LANES), f32),
            pltpu.VMEM((2, blocks, 4, full_cols), f32),
            pltpu.VMEM((4, 2, LANES), i32),
            pltpu.VMEM(coarse.shape, f32),
            pltpu.VMEM(coarse.shape, f32),
            pltpu.VMEM(coarse.shape, f32),
            pltpu.VMEM(coarse.shape, f32),
            pltpu.VMEM(cells, f32),
            dma((6,)),
            dma((1,)), dma((parts,)), dma((1,)), dma((1,)),
            dma((rows,)), dma((2,)), dma((4,)), dma((4,)),
            dma((1,)), dma((parts + 1,)), dma((1,)), dma((1,)), dma((1,)), dma((1,)), dma((1,)),
            pltpu.SemaphoreType.REGULAR((HEAD,)),
        ],
        compiler_params=pltpu.CompilerParams(
            collective_id=2, has_side_effects=True, vmem_limit_bytes=VMEM_BYTES - results
        ),
        name="fused",
    )(anchor, levels, strips, wet, cls, coarse)


def emit_kernel(fine, coarse, fine_out, coarse_out, sems):
    copies = [
        pltpu.make_async_copy(fine, fine_out, sems.at[0]),
        pltpu.make_async_copy(coarse, coarse_out, sems.at[1]),
    ]
    for copy in copies:
        copy.start()
    for copy in copies:
        copy.wait()


def emit(fine, coarse):
    vmem = pl.BlockSpec(memory_space=pltpu.VMEM)
    hbm = pl.BlockSpec(memory_space=pl.ANY)
    return pl.pallas_call(
        emit_kernel,
        out_shape=(
            jax.ShapeDtypeStruct(fine.shape, jnp.float32),
            jax.ShapeDtypeStruct(coarse.shape, jnp.float32),
        ),
        in_specs=[vmem, vmem],
        out_specs=(hbm, hbm),
        scratch_shapes=[pltpu.SemaphoreType.DMA((2,))],
        compiler_params=pltpu.CompilerParams(vmem_limit_bytes=4 * 2**20),
        name="emit",
    )(fine, coarse)


def local(nests, rows, cols, strips, anchor, wet_mask, bathy_index, bed_levels, coarse):
    band = strips.shape[4]
    if band % (3 * SUB) == 0 and 3 * band <= LANES and rows > 1 and cols == 4:
        return emit(*fused(
            nests, rows, cols, strips, anchor, wet_mask, bathy_index, bed_levels, coarse
        ))
    fields, colh, rowh, cellh = exchange(rows, cols, strips, wet_mask, bathy_index)
    fields = fields.reshape(3, -1, fields.shape[3])
    edge_cols = colh[:, :, :band].transpose(0, 2, 1).reshape(-1, SUB)
    updated, quads = step(
        rows, cols, anchor, bed_levels, fields, edge_cols, rowh, wet_mask[0], bathy_index[0], cellh
    )
    return updated, feedback(nests, rows, cols, anchor, quads, coarse)


def solution(mesh):
    sizes = (mesh.shape["nest"], mesh.shape["row"], mesh.shape["col"])
    return jax.shard_map(
        functools.partial(local, *sizes),
        mesh=mesh,
        in_specs=(
            P("nest", None, None, ("row", "col"), None, None),
            P(),
            P("nest", "row", "col"),
            P("nest", "row", "col"),
            P(),
            P(None, ("nest", "row"), "col"),
        ),
        out_specs=(P("nest", None, "row", "col"), P(None, ("nest", "row"), "col")),
        check_vma=False,
    )
```

```python
import functools

import jax
import jax.numpy as jnp
from jax import lax
from jax.experimental import pallas as pl
from jax.experimental.pallas import tpu as pltpu
from jax.sharding import PartitionSpec as P

gravity = 1.0
courant = 0.2
MESH = pl.DeviceIdType.MESH
LANES = 128
SUB = 8
HEAD = 3
DIRECT = 9
VMEM_BYTES = 67043328


def onehot(cond):
    return jnp.where(cond, 1.0, 0.0).astype(jnp.bfloat16)


def iota(shape, dim):
    return lax.broadcasted_iota(jnp.int32, shape, dim)


def dot(a, b):
    return jnp.dot(a, b, preferred_element_type=jnp.float32)


def dot_t(a, b):
    return lax.dot_general(
        a, b, (((1,), (1,)), ((), ())), preferred_element_type=jnp.float32
    )


def split(x, terms):
    parts = []
    for _ in range(terms):
        part = x.astype(jnp.bfloat16)
        parts.append(part)
        x = x - part.astype(jnp.float32)
    return parts


def exchange_kernel(
    rows, cols, strips, wet, cls, fields, colh, rowh, cellh,
    held, wet_v, cls_v, col_msg, row_msg, cell_msg, load_sem,
    big_send, big_recv, col_send, col_recv, row_send, row_recv, cell_send, cell_recv,
):
    parts = rows * cols
    row, col = lax.axis_index("row"), lax.axis_index("col")
    me = row * cols + col
    band = strips.shape[4]
    tile_cols = fields.shape[3]
    full_cols = strips.shape[5]

    loads = [
        pltpu.make_async_copy(strips.at[0, :, :, 0], held, load_sem.at[0]),
        pltpu.make_async_copy(wet.at[0], wet_v, load_sem.at[1]),
        pltpu.make_async_copy(cls.at[0], cls_v, load_sem.at[2]),
    ]
    for load in loads:
        load.start()

    def place(q):
        return {"row": q // cols, "col": lax.rem(q, cols)}

    barrier = pltpu.get_barrier_semaphore()

    def greet(t, _):
        q = lax.rem(me + t, parts)
        pl.semaphore_signal(barrier, inc=1, device_id=place(q), device_id_type=MESH)
        return 0

    lax.fori_loop(1, parts, greet, 0)
    pl.semaphore_wait(barrier, parts - 1)

    def columns(c):
        return pl.ds(pl.multiple_of(c * tile_cols, LANES), tile_cols)

    def big(q):
        return pltpu.make_async_remote_copy(
            src_ref=strips.at[0, :, q // cols, 0, :, columns(lax.rem(q, cols))],
            dst_ref=fields.at[:, me],
            send_sem=big_send.at[q],
            recv_sem=big_recv.at[me],
            device_id=place(q),
            device_id_type=MESH,
        )

    def big_start(t, _):
        big(lax.rem(me + t, parts)).start()
        return 0

    lax.fori_loop(1, parts, big_start, 0)
    own = pltpu.make_async_copy(
        strips.at[0, :, row, 0, :, columns(col)], fields.at[:, me], big_recv.at[me]
    )
    own.start()

    for load in loads:
        load.wait()
    lane = iota((SUB, LANES), 1)
    sub = iota((SUB, LANES), 0)
    first = onehot(lane == 0)
    last = onehot(lane == LANES - 1)
    even = iota((SUB, band), 0)
    for j in range(rows):
        for c in range(cols):
            message = jnp.zeros((SUB, band), jnp.float32)
            for k in range(3):
                if c > 0:
                    for part in split(held[k, j, :, c * tile_cols - LANES : c * tile_cols], 3):
                        message += jnp.where(even == k, dot_t(last, part), 0.0)
                if c < cols - 1:
                    for part in split(
                        held[k, j, :, (c + 1) * tile_cols : (c + 1) * tile_cols + LANES], 3
                    ):
                        message += jnp.where(even == 3 + k, dot_t(first, part), 0.0)
            col_msg[j * cols + c, :, 0:band] = message
    for j in range(rows):
        for k in range(3):
            row_msg[0, j, k : k + 1, :] = held[k, j, band - 1 : band, :]
            row_msg[1, j, k : k + 1, :] = held[k, j, 0:1, :]
    cell_rows = wet_v.shape[0]
    for at, cells in enumerate((wet_v, cls_v)):
        cell_msg[0, at : at + 1, :] = cells[cell_rows - 1 : cell_rows, :]
        cell_msg[1, at : at + 1, :] = cells[0:1, :]
        across = cells[...].astype(jnp.float32).astype(jnp.bfloat16)
        width = across.shape[1]
        pick = iota((SUB, width), 1)
        cell_msg[2, at : at + 1, :] = dot_t(onehot(pick == width - 1), across)[0:1].astype(jnp.int32)
        cell_msg[3, at : at + 1, :] = dot_t(onehot(pick == 0), across)[0:1].astype(jnp.int32)

    def col_copy(q):
        return pltpu.make_async_remote_copy(
            src_ref=col_msg.at[q],
            dst_ref=colh.at[me],
            send_sem=col_send.at[q],
            recv_sem=col_recv.at[me],
            device_id=place(q),
            device_id_type=MESH,
        )

    def col_start(t, _):
        col_copy(lax.rem(me + t, parts)).start()
        return 0

    lax.fori_loop(1, parts, col_start, 0)
    own_col = pltpu.make_async_copy(col_msg.at[me], colh.at[me], col_recv.at[me])
    own_col.start()

    cell_links = (
        (0, row < rows - 1, {"row": row + 1, "col": col}, row > 0),
        (1, row > 0, {"row": row - 1, "col": col}, row < rows - 1),
        (2, col < cols - 1, {"row": row, "col": col + 1}, col > 0),
        (3, col > 0, {"row": row, "col": col - 1}, col < cols - 1),
    )

    def cell_copy(slot, target):
        return pltpu.make_async_remote_copy(
            src_ref=cell_msg.at[slot],
            dst_ref=cellh.at[slot],
            send_sem=cell_send.at[slot],
            recv_sem=cell_recv.at[slot],
            device_id=target,
            device_id_type=MESH,
        )

    for slot, sends, target, _ in cell_links:
        @pl.when(sends)
        def _(slot=slot, target=target):
            cell_copy(slot, target).start()

    def row_copy(slot, j, c):
        target_row = j + 1 if slot == 0 else j - 1
        return pltpu.make_async_remote_copy(
            src_ref=row_msg.at[slot, j, :, c * tile_cols : (c + 1) * tile_cols],
            dst_ref=rowh.at[slot],
            send_sem=row_send.at[slot, j, c],
            recv_sem=row_recv.at[slot],
            device_id={"row": target_row, "col": c},
            device_id_type=MESH,
        )

    def row_own(slot, j, c):
        return pltpu.make_async_copy(
            row_msg.at[slot, j, :, c * tile_cols : (c + 1) * tile_cols],
            rowh.at[slot],
            row_recv.at[slot],
        )

    owner = (rows * cols - 1, 0)
    for slot in range(2):
        @pl.when(me == owner[slot])
        def _(slot=slot):
            for j in range(rows):
                target_row = j + 1 if slot == 0 else j - 1
                if target_row < 0 or target_row >= rows:
                    continue
                for c in range(cols):
                    if target_row * cols + c == owner[slot]:
                        row_own(slot, j, c).start()
                    else:
                        row_copy(slot, j, c).start()

    def arrive(t, _):
        q = lax.rem(me + t, parts)
        pltpu.make_async_copy(fields.at[:, q], fields.at[:, q], big_recv.at[q]).wait()
        pltpu.make_async_copy(colh.at[q], colh.at[q], col_recv.at[q]).wait()
        return 0

    lax.fori_loop(0, parts, arrive, 0)
    for slot, _, target, receives in cell_links:
        @pl.when(receives)
        def _(slot=slot, target=target):
            cell_copy(slot, target).wait_recv()

    for slot, receives in ((0, row > 0), (1, row < rows - 1)):
        @pl.when(receives)
        def _(slot=slot):
            row_own(slot, 0, 0).wait()

    def leave(t, _):
        q = lax.rem(me + t, parts)
        big(q).wait_send()
        col_copy(q).wait_send()
        return 0

    lax.fori_loop(1, parts, leave, 0)
    for slot, sends, target, _ in cell_links:
        @pl.when(sends)
        def _(slot=slot, target=target):
            cell_copy(slot, target).wait_send()
    for slot in range(2):
        @pl.when(me == owner[slot])
        def _(slot=slot):
            for j in range(rows):
                target_row = j + 1 if slot == 0 else j - 1
                if target_row < 0 or target_row >= rows:
                    continue
                for c in range(cols):
                    if target_row * cols + c != owner[slot]:
                        row_copy(slot, j, c).wait_send()


def exchange(rows, cols, strips, wet, cls):
    parts = rows * cols
    blocks, band, full_cols = strips.shape[2], strips.shape[4], strips.shape[5]
    tile_cols = full_cols // cols
    any_spec = pl.BlockSpec(memory_space=pl.ANY)
    dma = pltpu.SemaphoreType.DMA
    f32 = jnp.float32
    return pl.pallas_call(
        functools.partial(exchange_kernel, rows, cols),
        out_shape=(
            jax.ShapeDtypeStruct((3, parts, band, tile_cols), f32),
            jax.ShapeDtypeStruct((parts, SUB, LANES), f32),
            jax.ShapeDtypeStruct((2, SUB, tile_cols), f32),
            jax.ShapeDtypeStruct((4, SUB, LANES), jnp.int32),
        ),
        in_specs=[any_spec] * 3,
        out_specs=(any_spec,) * 4,
        scratch_shapes=[
            pltpu.VMEM((3, blocks, band, full_cols), f32),
            pltpu.VMEM(wet.shape[1:], jnp.int32),
            pltpu.VMEM(cls.shape[1:], jnp.int32),
            pltpu.VMEM((parts, SUB, LANES), f32),
            pltpu.VMEM((2, blocks, SUB, full_cols), f32),
            pltpu.VMEM((4, SUB, LANES), jnp.int32),
            dma((3,)),
            dma((parts,)), dma((parts,)), dma((parts,)), dma((parts,)),
            dma((2, rows, cols)), dma((2,)), dma((4,)), dma((4,)),
        ],
        compiler_params=pltpu.CompilerParams(collective_id=0, has_side_effects=True),
        name="exchange",
    )(strips, wet, cls)


def step_kernel(
    rows, cols, chunk, anchor, levels, fields, edge_cols, rowh, wet, cls, cellh,
    fine, quads, pad, bed_v, wet_p, bed_p,
):
    nest, row, col = lax.axis_index("nest"), lax.axis_index("row"), lax.axis_index("col")
    tile_rows, tile_cols = fields.shape[1], fields.shape[2]
    cell_rows, cell_cols = wet.shape
    wide = tile_cols + LANES
    above, below = row > 0, row < rows - 1
    left, right = col > 0, col < cols - 1
    end = SUB + tile_rows

    def look(classes):
        bed = jnp.zeros(classes.shape, jnp.float32)
        for at in range(levels.shape[0]):
            bed = jnp.where(classes == at, levels[at], bed)
        return bed

    down = onehot(iota((tile_rows, cell_rows), 0) // 3 == iota((tile_rows, cell_rows), 1))
    across = onehot(iota((cell_cols, tile_cols), 1) // 3 == iota((cell_cols, tile_cols), 0))
    lane = iota((tile_rows, LANES), 1)

    def side(low, high):
        low = jnp.where(left, low, 0.0)
        high = jnp.where(right, high, 0.0)
        return jnp.where(lane == 0, high, jnp.where(lane == LANES - 1, low, 0.0))

    edge = cellh[...]
    edge_bed = [look(edge[slot]) for slot in range(4)]
    edge_wet = [edge[slot].astype(jnp.float32) for slot in range(4)]
    bed_v[...] = look(cls[...])
    for target, inner, edges, at, terms in (
        (wet_p, wet[...].astype(jnp.float32), edge_wet, 0, 1),
        (bed_p, bed_v[...], edge_bed, 1, 3),
    ):
        full = 0.0
        for part in split(inner, terms):
            full += dot(dot(down, part).astype(jnp.bfloat16), across)
        target[SUB:end, 0:tile_cols] = full

        def row_of(slot):
            total = 0.0
            for part in split(edges[slot], terms):
                total += dot(part, across)
            return total[at : at + 1]

        def col_of(slot):
            total = 0.0
            for part in split(edges[slot], terms):
                total += dot_t(down, part)
            return total[:, at : at + 1]

        zeros = jnp.zeros((SUB, wide), jnp.float32)
        target[0:SUB, :] = zeros
        target[end : end + SUB, :] = zeros
        target[SUB - 1 : SUB, 0:tile_cols] = jnp.where(above, row_of(0), 0.0)
        target[end : end + 1, 0:tile_cols] = jnp.where(below, row_of(1), 0.0)
        target[SUB:end, tile_cols:wide] = side(col_of(2), col_of(3))

    for k in range(3):
        pad[k, SUB:end, 0:tile_cols] = fields[k]
        pad[k, 0:SUB, :] = jnp.zeros((SUB, wide), jnp.float32)
        pad[k, end : end + SUB, :] = jnp.zeros((SUB, wide), jnp.float32)
        pad[k, SUB - 1 : SUB, 0:tile_cols] = jnp.where(above, rowh[0, k : k + 1, :], 0.0)
        pad[k, end : end + 1, 0:tile_cols] = jnp.where(below, rowh[1, k : k + 1, :], 0.0)
        pad[k, SUB:end, tile_cols:wide] = side(
            edge_cols[:, k : k + 1], edge_cols[:, 3 + k : 4 + k]
        )

    window = chunk + 2 * SUB

    def west(x):
        return pltpu.roll(x, 1, 1)

    def east(x):
        return pltpu.roll(x, wide - 1, 1)

    def north(x):
        return pltpu.roll(x, 1, 0)

    def south(x):
        return pltpu.roll(x, x.shape[0] - 1, 0)

    def body(step, _):
        base = pl.multiple_of(step * chunk, SUB)
        at = pl.ds(base, window)
        h, hu, hv = pad[0, at, :], pad[1, at, :], pad[2, at, :]
        wet_w, bed_w = wet_p[at, :], bed_p[at, :]
        safe = jnp.where(wet_w > 0.5, h, 1.0)
        inverse = 1.0 / safe
        u, v = hu * inverse, hv * inverse
        speed = safe * lax.rsqrt(safe)
        pressure = 0.5 * gravity * safe * safe
        cross = hu * v

        def mid(x):
            return x[SUB : SUB + chunk]

        def narrow(x):
            return x[:, 0:tile_cols]

        h_n, hu_n, hv_n, wet_n, bed_n = [narrow(x) for x in (h, hu, hv, wet_w, bed_w)]
        gate = (0.5 * courant) * (north(wet_n) * wet_n)
        reach = narrow(jnp.abs(v) + speed)
        bound = jnp.maximum(north(reach), reach)
        totals = []
        for state, flux in (
            (h_n, hv_n), (hu_n, narrow(cross)), (hv_n, narrow(hv * v + pressure)),
        ):
            face = gate * ((north(flux) + flux) - bound * (state - north(state)))
            totals.append(mid(face) - mid(south(face)))
        slope = gate * (bed_n - north(bed_n))
        centre = mid(h_n)
        totals[2] -= gravity * centre * (mid(slope) + mid(south(slope)))

        h_m, hu_m, hv_m, wet_m, bed_m = [mid(x) for x in (h, hu, hv, wet_w, bed_w)]
        gate = (0.5 * courant) * (west(wet_m) * wet_m)
        reach = mid(jnp.abs(u) + speed)
        bound = jnp.maximum(west(reach), reach)
        for k, (state, flux) in enumerate(
            ((h_m, hu_m), (hu_m, mid(hu * u + pressure)), (hv_m, mid(cross)))
        ):
            face = gate * ((west(flux) + flux) - bound * (state - west(state)))
            totals[k] += narrow(face - east(face))
        slope = gate * (bed_m - west(bed_m))
        totals[1] -= gravity * centre * narrow(slope + east(slope))
        out = pl.ds(base, chunk)
        for k, state in enumerate((h_m, hu_m, hv_m)):
            fine[0, k, out, :] = narrow(state) + totals[k]
        return 0

    lax.fori_loop(0, tile_rows // chunk, body, 0)

    shift_r, shift_c = anchor[nest, 0], anchor[nest, 1]
    low = onehot(
        iota((2 * cell_rows, tile_rows), 1) // 3 + shift_r == iota((2 * cell_rows, tile_rows), 0)
    )
    wide_pick = onehot(
        iota((tile_cols, 2 * cell_cols), 0) // 3 + shift_c == iota((tile_cols, 2 * cell_cols), 1)
    )
    for k in range(3):
        part_rows = 0.0
        for part in split(fine[0, k], 2):
            part_rows += dot(low, part)
        placed = 0.0
        for part in split(part_rows, 2):
            placed += dot(part, wide_pick)
        placed = placed * (1.0 / 9.0)
        for a in range(2):
            for b in range(2):
                quads[2 * a + b, k] = placed[
                    a * cell_rows : (a + 1) * cell_rows, b * cell_cols : (b + 1) * cell_cols
                ]


def step(rows, cols, anchor, levels, fields, edge_cols, rowh, wet, cls, cellh):
    tile_rows, tile_cols = fields.shape[1:]
    cell_rows, cell_cols = wet.shape
    smem = pl.BlockSpec(memory_space=pltpu.SMEM)
    vmem = pl.BlockSpec(memory_space=pltpu.VMEM)
    f32 = jnp.float32
    padded = (tile_rows + 2 * SUB, tile_cols + LANES)
    return pl.pallas_call(
        functools.partial(step_kernel, rows, cols, 48),
        out_shape=(
            jax.ShapeDtypeStruct((1, 3, tile_rows, tile_cols), f32),
            jax.ShapeDtypeStruct((4, 3, cell_rows, cell_cols), f32),
        ),
        in_specs=[smem, smem] + [vmem] * 6,
        out_specs=(vmem, vmem),
        scratch_shapes=[
            pltpu.VMEM((3,) + padded, f32),
            pltpu.VMEM(wet.shape, f32),
            pltpu.VMEM(padded, f32),
            pltpu.VMEM(padded, f32),
        ],
        compiler_params=pltpu.CompilerParams(vmem_limit_bytes=40 * 1024 * 1024),
        name="step",
    )(anchor, levels, fields, edge_cols, rowh, wet, cls, cellh)


def feedback_kernel(nests, rows, cols, anchor, quads, coarse, out, held, send_sem, recv_sem):
    nest, row, col = lax.axis_index("nest"), lax.axis_index("row"), lax.axis_index("col")
    block = nest * rows + row
    blocks = nests * rows
    cell_rows, cell_cols = coarse.shape[1], coarse.shape[2]

    def place(b, c):
        return {"nest": b // rows, "row": lax.rem(b, rows), "col": c}

    links = []
    for quad in (1, 2, 3):
        db, dc = quad // 2, quad % 2
        sends = jnp.logical_and(block + db < blocks, col + dc < cols)
        takes = jnp.logical_and(block - db >= 0, col - dc >= 0)
        links.append((quad, sends, place(block + db, col + dc), takes, place(block - db, col - dc)))

    barrier = pltpu.get_barrier_semaphore()
    for _, _, _, takes, source in links:
        @pl.when(takes)
        def _(source=source):
            pl.semaphore_signal(barrier, inc=1, device_id=source, device_id_type=MESH)
    targets = sum(jnp.where(sends, 1, 0) for _, sends, _, _, _ in links)

    @pl.when(targets > 0)
    def _():
        pl.semaphore_wait(barrier, targets)

    def copy(quad, target):
        return pltpu.make_async_remote_copy(
            src_ref=quads.at[quad],
            dst_ref=held.at[quad - 1],
            send_sem=send_sem.at[quad - 1],
            recv_sem=recv_sem.at[quad - 1],
            device_id=target,
            device_id_type=MESH,
        )

    for quad, sends, target, _, _ in links:
        @pl.when(sends)
        def _(quad=quad, target=target):
            copy(quad, target).start()

    at_row = block * cell_rows + iota((cell_rows, cell_cols), 0)
    at_col = col * cell_cols + iota((cell_rows, cell_cols), 1)
    count = jnp.ones((cell_rows, cell_cols), jnp.float32)
    for n in range(nests):
        from_row = at_row - (n * rows * cell_rows + anchor[n, 0])
        from_col = at_col - anchor[n, 1]
        inside = (from_row >= 0) & (from_row < rows * cell_rows)
        inside &= (from_col >= 0) & (from_col < cols * cell_cols)
        count += jnp.where(inside, 1.0, 0.0)
    weight = 1.0 / count
    for k in range(3):
        out[k] = coarse[k] + quads[0, k]
    for quad, _, target, takes, _ in links:
        @pl.when(takes)
        def _(quad=quad, target=target):
            copy(quad, target).wait_recv()
            for k in range(3):
                out[k] += held[quad - 1, k]
    for k in range(3):
        out[k] = out[k] * weight
    for quad, sends, target, _, _ in links:
        @pl.when(sends)
        def _(quad=quad, target=target):
            copy(quad, target).wait_send()


def feedback(nests, rows, cols, anchor, quads, coarse):
    smem = pl.BlockSpec(memory_space=pltpu.SMEM)
    vmem = pl.BlockSpec(memory_space=pltpu.VMEM)
    return pl.pallas_call(
        functools.partial(feedback_kernel, nests, rows, cols),
        out_shape=jax.ShapeDtypeStruct(coarse.shape, jnp.float32),
        in_specs=[smem, vmem, vmem],
        out_specs=vmem,
        scratch_shapes=[
            pltpu.VMEM((3,) + coarse.shape, jnp.float32),
            pltpu.SemaphoreType.DMA((3,)),
            pltpu.SemaphoreType.DMA((3,)),
        ],
        compiler_params=pltpu.CompilerParams(collective_id=1, has_side_effects=True),
        name="feedback",
    )(anchor, quads, coarse)


def fused_kernel(
    nests, rows, cols, anchor_in, levels_in, strips, wet, cls, coarse, fine, out,
    anchor, levels, fine_sem, held, wet_v, cls_v, coarse_v, pad, wet_p, bed_p, colh, rowh, cellh,
    col_msg, row_msg, cell_msg, rest, left, above, corner, weight, load_sem,
    big_send, big_recv, col_send, col_recv, row_send, row_recv, cell_send, cell_recv,
    side_send, side_recv, down_send, down_recv, far_send, far_recv, relay_send, ready,
):
    parts = rows * cols
    nest, row, col = lax.axis_index("nest"), lax.axis_index("row"), lax.axis_index("col")
    me = row * cols + col
    block, blocks = nest * rows + row, nests * rows
    band = strips.shape[4]
    tile_rows, tile_cols = fine.shape[2], fine.shape[3]
    cell_rows, cell_cols = wet_v.shape
    group = band // 3
    wide = tile_cols + LANES
    end = SUB + tile_rows
    has_above, has_below = row > 0, row < rows - 1
    has_left, has_right = col > 0, col < cols - 1
    has_last, has_next = block > 0, block < blocks - 1

    loads = [
        pltpu.make_async_copy(strips.at[0, :, :, 0], held, load_sem.at[0]),
        pltpu.make_async_copy(wet.at[0], wet_v, load_sem.at[1]),
        pltpu.make_async_copy(cls.at[0], cls_v, load_sem.at[2]),
        pltpu.make_async_copy(coarse, coarse_v, load_sem.at[3]),
        pltpu.make_async_copy(anchor_in, anchor, load_sem.at[4]),
        pltpu.make_async_copy(levels_in, levels, load_sem.at[5]),
    ]
    for load in loads:
        load.start()

    def place(q):
        return {"row": q // cols, "col": lax.rem(q, cols)}

    barrier = pltpu.get_barrier_semaphore()
    to_next = jnp.logical_and(row == rows - 1, nest < nests - 1)
    to_last = jnp.logical_and(row == 0, nest > 0)
    below_id = {"nest": (block + 1) // rows, "row": lax.rem(block + 1, rows), "col": col}

    def rank(q):
        r = q // cols
        c = lax.rem(q, cols)
        return (2 * (r // 2 + lax.rem(r, 2) + c) + jnp.where(c == 2, 0, 1)) * parts + q

    mine = rank(me)

    def stride(n, col=col):
        if cols != 4:
            return n
        m = jnp.maximum(n - 2 * rows, 0)
        near = jnp.where(col == 0, 1, 3) + cols * (n - 1)
        far = jnp.where(col == 0, 2, 1) + lax.rem(m, 2) + cols * (m // 2)
        t = jnp.where(n <= rows, near, jnp.where(n < 2 * rows, cols * (n - rows), far))
        first = jnp.where(lax.rem(n, cols) == 0, n + 1 - cols, n + 1)
        first = jnp.where(n == parts - 1, parts + 1 - cols, first)
        return jnp.where(col == 1, n, jnp.where(col == 2, first, t))

    early = min(parts, HEAD)

    def turn_of(source, q):
        at = early - 1
        for n in range(early - 1, 0, -1):
            hit = lax.rem(source + stride(n, lax.rem(source, cols)), parts) == q
            at = jnp.where(hit, n - 1, at)
        return at

    def greet(t, count):
        q = lax.rem(me + t, parts)
        later = rank(q) > mine

        @pl.when(later)
        def _():
            pl.semaphore_signal(barrier, inc=1, device_id=place(q), device_id_type=MESH)

        return count + jnp.where(later, 0, 1)

    for at, takes in ((col, to_last), (col - 1, jnp.logical_and(to_last, has_left))):
        @pl.when(takes)
        def _(at=at):
            pl.semaphore_signal(
                barrier, inc=1, device_id={"nest": nest - 1, "row": rows - 1, "col": at},
                device_id_type=MESH,
            )

    earlier = lax.fori_loop(1, parts, greet, 0) + jnp.where(to_next, 1, 0)
    earlier = earlier + jnp.where(jnp.logical_and(to_next, has_right), 1, 0)

    @pl.when(earlier > 0)
    def _():
        pl.semaphore_wait(barrier, earlier)

    def answer(t, _):
        q = lax.rem(me + t, parts)

        @pl.when(rank(q) < mine)
        def _():
            pl.semaphore_signal(
                ready.at[turn_of(q, me)], inc=1, device_id=place(q), device_id_type=MESH
            )

        return 0

    lax.fori_loop(1, parts, answer, 0)

    def meet(n):
        @pl.when(rank(lax.rem(me + stride(n), parts)) > mine)
        def _():
            pl.semaphore_wait(ready.at[n - 1], 1)

    def columns(c):
        return pl.ds(pl.multiple_of(c * tile_cols, LANES), tile_cols)

    def landing(p):
        return pad.at[:, pl.ds(pl.multiple_of(SUB + p * band, SUB), band), 0:tile_cols]

    def big(q):
        return pltpu.make_async_remote_copy(
            src_ref=strips.at[0, :, q // cols, 0, :, columns(lax.rem(q, cols))],
            dst_ref=landing(me),
            send_sem=big_send.at[0],
            recv_sem=big_recv.at[me],
            device_id=place(q),
            device_id_type=MESH,
        )

    def big_start(t, _):
        big(lax.rem(me + t, parts)).start()
        return 0

    def first_start(n, _):
        meet(n)
        return big_start(stride(n), 0)

    def next_start(n, _):
        return big_start(stride(n), 0)

    lax.fori_loop(1, early, first_start, 0)
    own = pltpu.make_async_copy(
        strips.at[0, :, row, 0, :, columns(col)], landing(me), big_recv.at[me]
    )
    own.start()

    loads[1].wait()
    loads[2].wait()
    for at, cells in enumerate((wet_v, cls_v)):
        cell_msg[0, at : at + 1, :] = cells[cell_rows - 1 : cell_rows, :]
        cell_msg[1, at : at + 1, :] = cells[0:1, :]
        across = cells[...].astype(jnp.float32).astype(jnp.bfloat16)
        pick = iota((SUB, cell_cols), 1)
        cell_msg[2, at : at + 1, :] = dot_t(onehot(pick == cell_cols - 1), across)[0:1].astype(jnp.int32)
        cell_msg[3, at : at + 1, :] = dot_t(onehot(pick == 0), across)[0:1].astype(jnp.int32)
    loads[0].wait()
    for j in range(rows):
        for k in range(3):
            row_msg[0, j, k : k + 1, :] = held[k, j, band - 1 : band, :]
            row_msg[1, j, k : k + 1, :] = held[k, j, 0:1, :]
    col_msg[...] = jnp.zeros_like(col_msg)
    lane = iota((3 * band, LANES), 1)
    for j in range(rows):
        for c in range(1, cols):
            at = c * tile_cols
            low = jnp.concatenate([held[k, j, :, at - LANES : at] for k in range(3)], axis=0)
            high = jnp.concatenate([held[k, j, :, at : at + LANES] for k in range(3)], axis=0)
            both = jnp.where(lane == 0, high, low).T
            col_msg[j * cols + c, 0:1, 0 : 3 * band] = both[LANES - 1 : LANES]
            col_msg[j * cols + c - 1, 1:2, 0 : 3 * band] = both[0:1]

    def later(n, count):
        return count + jnp.where(rank(lax.rem(me + stride(n), parts)) > mine, 1, 0)

    rest_of = lax.fori_loop(early, parts, later, 0)

    @pl.when(rest_of > 0)
    def _():
        pl.semaphore_wait(ready.at[early - 1], rest_of)

    cell_links = (
        (0, has_below, {"row": row + 1, "col": col}, has_above),
        (1, has_above, {"row": row - 1, "col": col}, has_below),
        (2, has_right, {"row": row, "col": col + 1}, has_left),
        (3, has_left, {"row": row, "col": col - 1}, has_right),
    )

    def cell_copy(slot, target):
        return pltpu.make_async_remote_copy(
            src_ref=cell_msg.at[slot],
            dst_ref=cellh.at[slot],
            send_sem=cell_send.at[slot],
            recv_sem=cell_recv.at[slot],
            device_id=target,
            device_id_type=MESH,
        )

    for slot, sends, target, _ in cell_links:
        @pl.when(sends)
        def _(slot=slot, target=target):
            cell_copy(slot, target).start()

    def row_copy(slot, j, c):
        return pltpu.make_async_remote_copy(
            src_ref=row_msg.at[slot, j, :, c * tile_cols : (c + 1) * tile_cols],
            dst_ref=rowh.at[slot],
            send_sem=row_send.at[j],
            recv_sem=row_recv.at[slot],
            device_id={"row": j + 1 if slot == 0 else j - 1, "col": c},
            device_id_type=MESH,
        )

    def row_own(slot, j, c):
        return pltpu.make_async_copy(
            row_msg.at[slot, j, :, c * tile_cols : (c + 1) * tile_cols],
            rowh.at[slot],
            row_recv.at[slot],
        )

    owner = (parts - 1, 0)

    def row_targets(slot):
        for j in range(rows):
            target_row = j + 1 if slot == 0 else j - 1
            if 0 <= target_row < rows:
                for c in range(cols):
                    yield j, c, target_row * cols + c == owner[slot]

    for slot in range(2):
        @pl.when(me == owner[slot])
        def _(slot=slot):
            for j, c, mine in row_targets(slot):
                (row_own if mine else row_copy)(slot, j, c).start()

    def col_copy(q):
        return pltpu.make_async_remote_copy(
            src_ref=col_msg.at[q],
            dst_ref=colh.at[me],
            send_sem=col_send.at[0],
            recv_sem=col_recv.at[0],
            device_id=place(q),
            device_id_type=MESH,
        )

    def col_start(n, _):
        col_copy(lax.rem(me + stride(n), parts)).start()
        return 0

    lax.fori_loop(1, parts, col_start, 0)
    pltpu.make_async_copy(col_msg.at[me], colh.at[me], col_recv.at[0]).start()
    if early < parts:
        lax.fori_loop(early, parts, next_start, 0)

    loads[4].wait()
    loads[5].wait()

    def look(classes):
        bed = jnp.zeros(classes.shape, jnp.float32)
        for at in range(levels.shape[0]):
            bed = jnp.where(classes == at, levels[at], bed)
        return bed

    down = onehot(iota((tile_rows, cell_rows), 0) // 3 == iota((tile_rows, cell_rows), 1))
    across = onehot(iota((cell_cols, tile_cols), 1) // 3 == iota((cell_cols, tile_cols), 0))

    def side(low, high):
        lane = iota((low.shape[0], LANES), 1)
        low = jnp.where(has_left, low, 0.0)
        high = jnp.where(has_right, high, 0.0)
        return jnp.where(lane == 0, high, jnp.where(lane == LANES - 1, low, 0.0))

    inner = (wet_v[...].astype(jnp.float32), look(cls_v[...]))
    zeros = jnp.zeros((SUB, wide), jnp.float32)
    for target, cells, terms in ((wet_p, inner[0], 1), (bed_p, inner[1], 3)):
        full = 0.0
        for part in split(cells, terms):
            full += dot(dot(down, part).astype(jnp.bfloat16), across)
        target[SUB:end, 0:tile_cols] = full
        target[0:SUB, :] = zeros
        target[end : end + SUB, :] = zeros
    for k in range(3):
        pad[k, 0:SUB, :] = zeros
        pad[k, end : end + SUB, :] = zeros

    for slot, _, target, receives in cell_links:
        @pl.when(jnp.logical_not(receives))
        def _(slot=slot):
            cellh[slot] = jnp.zeros((2, LANES), jnp.int32)

        @pl.when(receives)
        def _(slot=slot, target=target):
            cell_copy(slot, target).wait_recv()

    for target, at, terms in ((wet_p, 0, 1), (bed_p, 1, 3)):
        def edge_of(slot, at=at):
            cells = jnp.concatenate([cellh[slot], jnp.zeros((SUB - 2, LANES), jnp.int32)], axis=0)
            return cells.astype(jnp.float32) if at == 0 else look(cells)

        def row_of(slot, at=at, terms=terms):
            total = 0.0
            for part in split(edge_of(slot), terms):
                total += dot(part, across)
            return total[at : at + 1]

        def col_of(slot, at=at, terms=terms):
            total = 0.0
            for part in split(edge_of(slot), terms):
                total += dot_t(down, part)
            return total[:, at : at + 1]

        target[SUB - 1 : SUB, 0:tile_cols] = jnp.where(has_above, row_of(0), 0.0)
        target[end : end + 1, 0:tile_cols] = jnp.where(has_below, row_of(1), 0.0)
        target[SUB:end, tile_cols:wide] = side(col_of(2), col_of(3))

    def settle(ref, sem):
        pltpu.make_async_copy(ref, ref, sem.at[0]).wait()

    settle(colh, col_recv)
    edges = jnp.concatenate([colh[b] for b in range(parts)], axis=0).T
    for k in range(3):
        edge = edges[k * band : (k + 1) * band]
        for b in range(parts):
            top = SUB + b * band
            pad[k, top : top + band, tile_cols:wide] = side(
                edge[:, 2 * b : 2 * b + 1], edge[:, 2 * b + 1 : 2 * b + 2]
            )

    at_row = block * cell_rows + iota((cell_rows, cell_cols), 0)
    at_col = col * cell_cols + iota((cell_rows, cell_cols), 1)
    count = jnp.ones((cell_rows, cell_cols), jnp.float32)
    for n in range(nests):
        from_row = at_row - (n * rows * cell_rows + anchor[n, 0])
        from_col = at_col - anchor[n, 1]
        covered = (from_row >= 0) & (from_row < rows * cell_rows)
        covered &= (from_col >= 0) & (from_col < cols * cell_cols)
        count += jnp.where(covered, 1.0, 0.0)
    weight[...] = 1.0 / count

    pick = onehot(iota((tile_cols, cell_cols), 0) // 3 == iota((tile_cols, cell_cols), 1))

    def west(x):
        return pltpu.roll(x, 1, 1)

    def east(x):
        return pltpu.roll(x, wide - 1, 1)

    def north(x):
        return pltpu.roll(x, 1, 0)

    def south(x):
        return pltpu.roll(x, x.shape[0] - 1, 0)

    def narrow(x):
        return x[:, 0:tile_cols]

    def big_wait(b):
        pltpu.make_async_copy(landing(b), landing(b), big_recv.at[b]).wait()

    def rest_rows(ref, b):
        return ref.at[:, pl.ds(pl.multiple_of(b * group, SUB), group), :]

    middle = cols // 2

    def side_copy(b, slot):
        return pltpu.make_async_remote_copy(
            src_ref=rest_rows(rest, b),
            dst_ref=rest_rows(left, b),
            send_sem=side_send.at[0],
            recv_sem=side_recv.at[slot],
            device_id={"col": col + 1},
            device_id_type=MESH,
        )

    def down_copy(b):
        return pltpu.make_async_remote_copy(
            src_ref=rest_rows(rest, b),
            dst_ref=rest_rows(above, b),
            send_sem=down_send.at[0],
            recv_sem=down_recv.at[0],
            device_id=below_id,
            device_id_type=MESH,
        )

    def far_copy(b):
        return pltpu.make_async_remote_copy(
            src_ref=rest_rows(rest, b),
            dst_ref=rest_rows(corner, b),
            send_sem=far_send.at[0],
            recv_sem=far_recv.at[0],
            device_id={**below_id, "col": col + 1},
            device_id_type=MESH,
        )

    def relay_copy(b):
        return pltpu.make_async_remote_copy(
            src_ref=rest_rows(left, b),
            dst_ref=rest_rows(corner, b),
            send_sem=relay_send.at[0],
            recv_sem=far_recv.at[0],
            device_id=below_id,
            device_id_type=MESH,
        )

    def share(s):
        b = band_at(s)

        @pl.when(jnp.logical_and(has_right, col + 1 != middle))
        def _():
            side_copy(b, parts - DIRECT).start()

        @pl.when(has_next)
        def _():
            down_copy(b).start()

        @pl.when(jnp.logical_and(jnp.logical_and(has_right, has_next), col + 1 != middle))
        def _():
            far_copy(b).start()

    def share_middle(first, last):
        def one(s, _):
            b = band_at(s)
            side_copy(b, jnp.minimum(s, parts - DIRECT)).start()

            @pl.when(jnp.logical_and(has_next, s >= parts - DIRECT))
            def _():
                far_copy(b).start()

            return 0

        @pl.when(col + 1 == middle)
        def _():
            lax.fori_loop(first, last, one, 0)

    last_three = parts - 2
    if cols == 4:
        last_three = jnp.where(col == 1, parts - 2, jnp.where(col == 2, parts - 4, parts - 3))

    def turn(s, first):
        t = jnp.where(s < first - 1, s + 1, s + 4)
        return jnp.where(s < parts - 3, t, first + s - (parts - 3))

    def band_at(s):
        return lax.rem(me + parts - turn(s, last_three), parts)

    def advance(base, count):
        def mid(x):
            return x[SUB : SUB + count]

        base = pl.multiple_of(base, SUB)
        at = pl.ds(base, count + 2 * SUB)
        h, hu, hv = pad[0, at, :], pad[1, at, :], pad[2, at, :]
        wet_w, bed_w = wet_p[at, :], bed_p[at, :]
        safe = jnp.where(wet_w > 0.5, h, 1.0)
        inverse = 1.0 / safe
        u, v = hu * inverse, hv * inverse
        speed = safe * lax.rsqrt(safe)
        pressure = 0.5 * gravity * safe * safe
        cross = hu * v

        h_n, hu_n, hv_n, wet_n, bed_n = [narrow(x) for x in (h, hu, hv, wet_w, bed_w)]
        gate = (0.5 * courant) * (north(wet_n) * wet_n)
        reach = narrow(jnp.abs(v) + speed)
        bound = jnp.maximum(north(reach), reach)
        totals = []
        for state, flux in (
            (h_n, hv_n), (hu_n, narrow(cross)), (hv_n, narrow(hv * v + pressure)),
        ):
            face = gate * ((north(flux) + flux) - bound * (state - north(state)))
            totals.append(mid(face) - mid(south(face)))
        slope = gate * (bed_n - north(bed_n))
        centre = mid(h_n)
        totals[2] -= gravity * centre * (mid(slope) + mid(south(slope)))

        h_m, hu_m, hv_m, wet_m, bed_m = [mid(x) for x in (h, hu, hv, wet_w, bed_w)]
        gate = (0.5 * courant) * (west(wet_m) * wet_m)
        reach = mid(jnp.abs(u) + speed)
        bound = jnp.maximum(west(reach), reach)
        for k, (state, flux) in enumerate(
            ((h_m, hu_m), (hu_m, mid(hu * u + pressure)), (hv_m, mid(cross)))
        ):
            face = gate * ((west(flux) + flux) - bound * (state - west(state)))
            totals[k] += narrow(face - east(face))
        slope = gate * (bed_m - west(bed_m))
        totals[1] -= gravity * centre * narrow(slope + east(slope))
        for k, state in enumerate((h_m, hu_m, hv_m)):
            fine[0, k, pl.ds(base, count), :] = narrow(state) + totals[k]

    def restrict(base, count):
        rows_of = pl.ds(pl.multiple_of(base, SUB), count)
        value = jnp.concatenate([fine[0, k, rows_of, :] for k in range(3)], axis=0)
        narrowed = dot(jnp.concatenate(split(value, 2), axis=0), pick)
        third = onehot(iota((count, 3 * count), 1) // 3 == iota((count, 3 * count), 0))
        mean = 0.0
        for part in split(narrowed[: 3 * count] + narrowed[3 * count :], 2):
            mean += dot(third, part)
        mean = mean * (1.0 / 9.0)
        cells = pl.ds(pl.multiple_of(base // 3, SUB), count // 3)
        for k in range(3):
            rest[k, cells, :] = mean[k * count // 3 : (k + 1) * count // 3]

    def arrived(t):
        big_wait(lax.rem(me + parts - t, parts))

    def halo(lowest, highest):
        for slot, edge, receives, at in ((0, 0, has_above, SUB - 1), (1, parts - 1, has_below, end)):
            here = jnp.logical_and(lowest <= edge, edge <= highest)

            @pl.when(jnp.logical_and(here, receives))
            def _(slot=slot, at=at):
                row_own(slot, 0, 0).wait()
                for k in range(3):
                    pad[k, at : at + 1, 0:tile_cols] = rowh[slot, k : k + 1, :]

    def body(s, _):
        b = band_at(s)

        @pl.when(s > 1)
        def _():
            share(s - 2)

        @pl.when(s == 0)
        def _():
            big_wait(me)
            arrived(1)

        @pl.when(s < last_three - 1)
        def _():
            arrived(s + 2)

        @pl.when(s == last_three - 1)
        def _():
            def others(t, _):
                arrived(t)
                return 0

            lax.fori_loop(last_three + 2, parts, others, 0)

        halo(b, b)
        advance(b * band, band)
        restrict(band_at(jnp.maximum(s - 1, 0)) * band, band)
        return 0

    lax.fori_loop(0, parts - 3, body, 0)
    share(parts - 5)
    share_middle(0, parts - 4)
    restrict(band_at(parts - 4) * band, band)
    arrived(last_three + 1)
    share(parts - 4)
    share_middle(parts - 4, parts - 3)
    lowest = band_at(parts - 1)
    halo(lowest, lowest + 2)
    advance(lowest * band, 3 * band)
    restrict(lowest * band, 3 * band)
    for s in range(parts - 3, parts):
        share(s)
    share_middle(parts - 3, parts)

    source = jnp.maximum(block - 1, 0) // rows
    row_own, col_own = anchor[nest, 0], anchor[nest, 1]
    row_last, col_last = anchor[source, 0], anchor[source, 1]
    cell_row = iota((cell_rows, cell_cols), 0)
    cell_col = iota((cell_rows, cell_cols), 1)
    def moved(cells, keep, by_col, from_row, by_row):
        cells = jnp.where(keep, pltpu.roll(cells, by_col, 1), 0.0)
        return jnp.where(from_row, pltpu.roll(cells, by_row, 0), 0.0)

    loads[3].wait()
    for k in range(3):
        out[k] = coarse_v[k] + moved(
            rest[k], cell_col >= col_own, col_own, cell_row >= row_own, row_own
        )

    left_three = parts - 2 if cols == 4 else last_three

    def relay(t, _):
        b = lax.rem(me + 2 * parts - 1 - turn(t, left_three), parts)
        pltpu.make_async_copy(rest_rows(left, b), rest_rows(left, b), side_recv.at[t]).wait()

        @pl.when(has_next)
        def _():
            relay_copy(b).start()

        return 0

    few = DIRECT * group

    @pl.when(jnp.logical_and(has_left, col == middle))
    def _():
        lax.fori_loop(0, parts - DIRECT, relay, 0)
        pltpu.make_async_copy(rest.at[:, :few], left.at[:, :few], side_recv.at[parts - DIRECT]).wait()

    @pl.when(jnp.logical_and(has_left, col != middle))
    def _():
        pltpu.make_async_copy(rest, left, side_recv.at[parts - DIRECT]).wait()

    @pl.when(has_left)
    def _():
        for k in range(3):
            out[k] += moved(left[k], cell_col < col_own, col_own, cell_row >= row_own, row_own)

    @pl.when(has_last)
    def _():
        settle(above, down_recv)
        for k in range(3):
            out[k] += moved(above[k], cell_col >= col_last, col_last, cell_row < row_last, row_last)

    @pl.when(jnp.logical_and(has_last, has_left))
    def _():
        settle(corner, far_recv)
        for k in range(3):
            out[k] += moved(corner[k], cell_col < col_last, col_last, cell_row < row_last, row_last)

    for k in range(3):
        out[k] = out[k] * weight[...]

    settle(pad.at[:, SUB : SUB + (parts - 1) * band, 0:tile_cols], big_send)
    settle(colh.at[0 : parts - 1], col_send)
    for slot, sends, target, _ in cell_links:
        @pl.when(sends)
        def _(slot=slot, target=target):
            cell_copy(slot, target).wait_send()
    for slot in range(2):
        @pl.when(me == owner[slot])
        def _(slot=slot):
            for row_at in range(rows):
                n = sum(j == row_at and not mine for j, _, mine in row_targets(slot))
                if n > 0:
                    sent = row_msg.at[slot, row_at, :, 0 : n * tile_cols]
                    pltpu.make_async_copy(sent, sent, row_send.at[row_at]).wait()

    @pl.when(has_right)
    def _():
        settle(rest, side_send)

    @pl.when(has_next)
    def _():
        settle(rest, down_send)

    @pl.when(jnp.logical_and(jnp.logical_and(has_next, has_right), col + 1 != middle))
    def _():
        settle(rest, far_send)

    @pl.when(jnp.logical_and(jnp.logical_and(has_next, has_right), col + 1 == middle))
    def _():
        settle(rest.at[:, :few], far_send)

    @pl.when(jnp.logical_and(jnp.logical_and(has_next, has_left), col == middle))
    def _():
        settle(rest.at[:, few:], relay_send)


def fused(nests, rows, cols, strips, anchor, wet, cls, levels, coarse):
    parts = rows * cols
    blocks, band, full_cols = strips.shape[2], strips.shape[4], strips.shape[5]
    tile_rows, tile_cols = parts * band, full_cols // cols
    cells = wet.shape[1:]
    vmem = pl.BlockSpec(memory_space=pltpu.VMEM)
    hbm = pl.BlockSpec(memory_space=pltpu.HBM)
    dma = pltpu.SemaphoreType.DMA
    f32, i32 = jnp.float32, jnp.int32
    padded = (tile_rows + 2 * SUB, tile_cols + LANES)
    results = 4 * (3 * tile_rows * tile_cols + coarse.size)
    return pl.pallas_call(
        functools.partial(fused_kernel, nests, rows, cols),
        out_shape=(
            pltpu.VMEM((1, 3, tile_rows, tile_cols), f32),
            pltpu.VMEM(coarse.shape, f32),
        ),
        in_specs=[hbm] * 6,
        out_specs=(vmem, vmem),
        scratch_shapes=[
            pltpu.SMEM(anchor.shape, i32),
            pltpu.SMEM(levels.shape, f32),
            dma((parts,)),
            pltpu.VMEM((3, blocks, band, full_cols), f32),
            pltpu.VMEM(cells, i32),
            pltpu.VMEM(cells, i32),
            pltpu.VMEM(coarse.shape, f32),
            pltpu.VMEM((3,) + padded, f32),
            pltpu.VMEM(padded, f32),
            pltpu.VMEM(padded, f32),
            pltpu.VMEM((parts, 2, LANES), f32),
            pltpu.VMEM((2, 4, tile_cols), f32),
            pltpu.VMEM((4, 2, LANES), i32),
            pltpu.VMEM((parts, 2, LANES), f32),
            pltpu.VMEM((2, blocks, 4, full_cols), f32),
            pltpu.VMEM((4, 2, LANES), i32),
            pltpu.VMEM(coarse.shape, f32),
            pltpu.VMEM(coarse.shape, f32),
            pltpu.VMEM(coarse.shape, f32),
            pltpu.VMEM(coarse.shape, f32),
            pltpu.VMEM(cells, f32),
            dma((6,)),
            dma((1,)), dma((parts,)), dma((1,)), dma((1,)),
            dma((rows,)), dma((2,)), dma((4,)), dma((4,)),
            dma((1,)), dma((parts - DIRECT + 1,)), dma((1,)), dma((1,)), dma((1,)), dma((1,)), dma((1,)),
            pltpu.SemaphoreType.REGULAR((HEAD,)),
        ],
        compiler_params=pltpu.CompilerParams(
            collective_id=2, has_side_effects=True, vmem_limit_bytes=VMEM_BYTES - results
        ),
        name="fused",
    )(anchor, levels, strips, wet, cls, coarse)


def emit_kernel(fine, coarse, fine_out, coarse_out, sems):
    copies = [
        pltpu.make_async_copy(fine, fine_out, sems.at[0]),
        pltpu.make_async_copy(coarse, coarse_out, sems.at[1]),
    ]
    for copy in copies:
        copy.start()
    for copy in copies:
        copy.wait()


def emit(fine, coarse):
    vmem = pl.BlockSpec(memory_space=pltpu.VMEM)
    hbm = pl.BlockSpec(memory_space=pl.ANY)
    return pl.pallas_call(
        emit_kernel,
        out_shape=(
            jax.ShapeDtypeStruct(fine.shape, jnp.float32),
            jax.ShapeDtypeStruct(coarse.shape, jnp.float32),
        ),
        in_specs=[vmem, vmem],
        out_specs=(hbm, hbm),
        scratch_shapes=[pltpu.SemaphoreType.DMA((2,))],
        compiler_params=pltpu.CompilerParams(vmem_limit_bytes=4 * 2**20),
        name="emit",
    )(fine, coarse)


def local(nests, rows, cols, strips, anchor, wet_mask, bathy_index, bed_levels, coarse):
    band = strips.shape[4]
    if band % (3 * SUB) == 0 and 3 * band <= LANES and rows * cols > DIRECT + 3 and cols == 4:
        return emit(*fused(
            nests, rows, cols, strips, anchor, wet_mask, bathy_index, bed_levels, coarse
        ))
    fields, colh, rowh, cellh = exchange(rows, cols, strips, wet_mask, bathy_index)
    fields = fields.reshape(3, -1, fields.shape[3])
    edge_cols = colh[:, :, :band].transpose(0, 2, 1).reshape(-1, SUB)
    updated, quads = step(
        rows, cols, anchor, bed_levels, fields, edge_cols, rowh, wet_mask[0], bathy_index[0], cellh
    )
    return updated, feedback(nests, rows, cols, anchor, quads, coarse)


def solution(mesh):
    sizes = (mesh.shape["nest"], mesh.shape["row"], mesh.shape["col"])
    return jax.shard_map(
        functools.partial(local, *sizes),
        mesh=mesh,
        in_specs=(
            P("nest", None, None, ("row", "col"), None, None),
            P(),
            P("nest", "row", "col"),
            P("nest", "row", "col"),
            P(),
            P(None, ("nest", "row"), "col"),
        ),
        out_specs=(P("nest", None, "row", "col"), P(None, ("nest", "row"), "col")),
        check_vma=False,
    )
```

```python
import functools

import jax
import jax.numpy as jnp
from jax import lax
from jax.experimental import pallas as pl
from jax.experimental.pallas import tpu as pltpu
from jax.sharding import PartitionSpec as P

gravity = 1.0
courant = 0.2
MESH = pl.DeviceIdType.MESH
LANES = 128
SUB = 8
HEAD = 3
DIRECT = 9
VMEM_BYTES = 67043328


def onehot(cond):
    return jnp.where(cond, 1.0, 0.0).astype(jnp.bfloat16)


def iota(shape, dim):
    return lax.broadcasted_iota(jnp.int32, shape, dim)


def dot(a, b):
    return jnp.dot(a, b, preferred_element_type=jnp.float32)


def dot_t(a, b):
    return lax.dot_general(
        a, b, (((1,), (1,)), ((), ())), preferred_element_type=jnp.float32
    )


def split(x, terms):
    parts = []
    for _ in range(terms):
        part = x.astype(jnp.bfloat16)
        parts.append(part)
        x = x - part.astype(jnp.float32)
    return parts


def exchange_kernel(
    rows, cols, strips, wet, cls, fields, colh, rowh, cellh,
    held, wet_v, cls_v, col_msg, row_msg, cell_msg, load_sem,
    big_send, big_recv, col_send, col_recv, row_send, row_recv, cell_send, cell_recv,
):
    parts = rows * cols
    row, col = lax.axis_index("row"), lax.axis_index("col")
    me = row * cols + col
    band = strips.shape[4]
    tile_cols = fields.shape[3]
    full_cols = strips.shape[5]

    loads = [
        pltpu.make_async_copy(strips.at[0, :, :, 0], held, load_sem.at[0]),
        pltpu.make_async_copy(wet.at[0], wet_v, load_sem.at[1]),
        pltpu.make_async_copy(cls.at[0], cls_v, load_sem.at[2]),
    ]
    for load in loads:
        load.start()

    def place(q):
        return {"row": q // cols, "col": lax.rem(q, cols)}

    barrier = pltpu.get_barrier_semaphore()

    def greet(t, _):
        q = lax.rem(me + t, parts)
        pl.semaphore_signal(barrier, inc=1, device_id=place(q), device_id_type=MESH)
        return 0

    lax.fori_loop(1, parts, greet, 0)
    pl.semaphore_wait(barrier, parts - 1)

    def columns(c):
        return pl.ds(pl.multiple_of(c * tile_cols, LANES), tile_cols)

    def big(q):
        return pltpu.make_async_remote_copy(
            src_ref=strips.at[0, :, q // cols, 0, :, columns(lax.rem(q, cols))],
            dst_ref=fields.at[:, me],
            send_sem=big_send.at[q],
            recv_sem=big_recv.at[me],
            device_id=place(q),
            device_id_type=MESH,
        )

    def big_start(t, _):
        big(lax.rem(me + t, parts)).start()
        return 0

    lax.fori_loop(1, parts, big_start, 0)
    own = pltpu.make_async_copy(
        strips.at[0, :, row, 0, :, columns(col)], fields.at[:, me], big_recv.at[me]
    )
    own.start()

    for load in loads:
        load.wait()
    lane = iota((SUB, LANES), 1)
    sub = iota((SUB, LANES), 0)
    first = onehot(lane == 0)
    last = onehot(lane == LANES - 1)
    even = iota((SUB, band), 0)
    for j in range(rows):
        for c in range(cols):
            message = jnp.zeros((SUB, band), jnp.float32)
            for k in range(3):
                if c > 0:
                    for part in split(held[k, j, :, c * tile_cols - LANES : c * tile_cols], 3):
                        message += jnp.where(even == k, dot_t(last, part), 0.0)
                if c < cols - 1:
                    for part in split(
                        held[k, j, :, (c + 1) * tile_cols : (c + 1) * tile_cols + LANES], 3
                    ):
                        message += jnp.where(even == 3 + k, dot_t(first, part), 0.0)
            col_msg[j * cols + c, :, 0:band] = message
    for j in range(rows):
        for k in range(3):
            row_msg[0, j, k : k + 1, :] = held[k, j, band - 1 : band, :]
            row_msg[1, j, k : k + 1, :] = held[k, j, 0:1, :]
    cell_rows = wet_v.shape[0]
    for at, cells in enumerate((wet_v, cls_v)):
        cell_msg[0, at : at + 1, :] = cells[cell_rows - 1 : cell_rows, :]
        cell_msg[1, at : at + 1, :] = cells[0:1, :]
        across = cells[...].astype(jnp.float32).astype(jnp.bfloat16)
        width = across.shape[1]
        pick = iota((SUB, width), 1)
        cell_msg[2, at : at + 1, :] = dot_t(onehot(pick == width - 1), across)[0:1].astype(jnp.int32)
        cell_msg[3, at : at + 1, :] = dot_t(onehot(pick == 0), across)[0:1].astype(jnp.int32)

    def col_copy(q):
        return pltpu.make_async_remote_copy(
            src_ref=col_msg.at[q],
            dst_ref=colh.at[me],
            send_sem=col_send.at[q],
            recv_sem=col_recv.at[me],
            device_id=place(q),
            device_id_type=MESH,
        )

    def col_start(t, _):
        col_copy(lax.rem(me + t, parts)).start()
        return 0

    lax.fori_loop(1, parts, col_start, 0)
    own_col = pltpu.make_async_copy(col_msg.at[me], colh.at[me], col_recv.at[me])
    own_col.start()

    cell_links = (
        (0, row < rows - 1, {"row": row + 1, "col": col}, row > 0),
        (1, row > 0, {"row": row - 1, "col": col}, row < rows - 1),
        (2, col < cols - 1, {"row": row, "col": col + 1}, col > 0),
        (3, col > 0, {"row": row, "col": col - 1}, col < cols - 1),
    )

    def cell_copy(slot, target):
        return pltpu.make_async_remote_copy(
            src_ref=cell_msg.at[slot],
            dst_ref=cellh.at[slot],
            send_sem=cell_send.at[slot],
            recv_sem=cell_recv.at[slot],
            device_id=target,
            device_id_type=MESH,
        )

    for slot, sends, target, _ in cell_links:
        @pl.when(sends)
        def _(slot=slot, target=target):
            cell_copy(slot, target).start()

    def row_copy(slot, j, c):
        target_row = j + 1 if slot == 0 else j - 1
        return pltpu.make_async_remote_copy(
            src_ref=row_msg.at[slot, j, :, c * tile_cols : (c + 1) * tile_cols],
            dst_ref=rowh.at[slot],
            send_sem=row_send.at[slot, j, c],
            recv_sem=row_recv.at[slot],
            device_id={"row": target_row, "col": c},
            device_id_type=MESH,
        )

    def row_own(slot, j, c):
        return pltpu.make_async_copy(
            row_msg.at[slot, j, :, c * tile_cols : (c + 1) * tile_cols],
            rowh.at[slot],
            row_recv.at[slot],
        )

    owner = (rows * cols - 1, 0)
    for slot in range(2):
        @pl.when(me == owner[slot])
        def _(slot=slot):
            for j in range(rows):
                target_row = j + 1 if slot == 0 else j - 1
                if target_row < 0 or target_row >= rows:
                    continue
                for c in range(cols):
                    if target_row * cols + c == owner[slot]:
                        row_own(slot, j, c).start()
                    else:
                        row_copy(slot, j, c).start()

    def arrive(t, _):
        q = lax.rem(me + t, parts)
        pltpu.make_async_copy(fields.at[:, q], fields.at[:, q], big_recv.at[q]).wait()
        pltpu.make_async_copy(colh.at[q], colh.at[q], col_recv.at[q]).wait()
        return 0

    lax.fori_loop(0, parts, arrive, 0)
    for slot, _, target, receives in cell_links:
        @pl.when(receives)
        def _(slot=slot, target=target):
            cell_copy(slot, target).wait_recv()

    for slot, receives in ((0, row > 0), (1, row < rows - 1)):
        @pl.when(receives)
        def _(slot=slot):
            row_own(slot, 0, 0).wait()

    def leave(t, _):
        q = lax.rem(me + t, parts)
        big(q).wait_send()
        col_copy(q).wait_send()
        return 0

    lax.fori_loop(1, parts, leave, 0)
    for slot, sends, target, _ in cell_links:
        @pl.when(sends)
        def _(slot=slot, target=target):
            cell_copy(slot, target).wait_send()
    for slot in range(2):
        @pl.when(me == owner[slot])
        def _(slot=slot):
            for j in range(rows):
                target_row = j + 1 if slot == 0 else j - 1
                if target_row < 0 or target_row >= rows:
                    continue
                for c in range(cols):
                    if target_row * cols + c != owner[slot]:
                        row_copy(slot, j, c).wait_send()


def exchange(rows, cols, strips, wet, cls):
    parts = rows * cols
    blocks, band, full_cols = strips.shape[2], strips.shape[4], strips.shape[5]
    tile_cols = full_cols // cols
    any_spec = pl.BlockSpec(memory_space=pl.ANY)
    dma = pltpu.SemaphoreType.DMA
    f32 = jnp.float32
    return pl.pallas_call(
        functools.partial(exchange_kernel, rows, cols),
        out_shape=(
            jax.ShapeDtypeStruct((3, parts, band, tile_cols), f32),
            jax.ShapeDtypeStruct((parts, SUB, LANES), f32),
            jax.ShapeDtypeStruct((2, SUB, tile_cols), f32),
            jax.ShapeDtypeStruct((4, SUB, LANES), jnp.int32),
        ),
        in_specs=[any_spec] * 3,
        out_specs=(any_spec,) * 4,
        scratch_shapes=[
            pltpu.VMEM((3, blocks, band, full_cols), f32),
            pltpu.VMEM(wet.shape[1:], jnp.int32),
            pltpu.VMEM(cls.shape[1:], jnp.int32),
            pltpu.VMEM((parts, SUB, LANES), f32),
            pltpu.VMEM((2, blocks, SUB, full_cols), f32),
            pltpu.VMEM((4, SUB, LANES), jnp.int32),
            dma((3,)),
            dma((parts,)), dma((parts,)), dma((parts,)), dma((parts,)),
            dma((2, rows, cols)), dma((2,)), dma((4,)), dma((4,)),
        ],
        compiler_params=pltpu.CompilerParams(collective_id=0, has_side_effects=True),
        name="exchange",
    )(strips, wet, cls)


def step_kernel(
    rows, cols, chunk, anchor, levels, fields, edge_cols, rowh, wet, cls, cellh,
    fine, quads, pad, bed_v, wet_p, bed_p,
):
    nest, row, col = lax.axis_index("nest"), lax.axis_index("row"), lax.axis_index("col")
    tile_rows, tile_cols = fields.shape[1], fields.shape[2]
    cell_rows, cell_cols = wet.shape
    wide = tile_cols + LANES
    above, below = row > 0, row < rows - 1
    left, right = col > 0, col < cols - 1
    end = SUB + tile_rows

    def look(classes):
        bed = jnp.zeros(classes.shape, jnp.float32)
        for at in range(levels.shape[0]):
            bed = jnp.where(classes == at, levels[at], bed)
        return bed

    down = onehot(iota((tile_rows, cell_rows), 0) // 3 == iota((tile_rows, cell_rows), 1))
    across = onehot(iota((cell_cols, tile_cols), 1) // 3 == iota((cell_cols, tile_cols), 0))
    lane = iota((tile_rows, LANES), 1)

    def side(low, high):
        low = jnp.where(left, low, 0.0)
        high = jnp.where(right, high, 0.0)
        return jnp.where(lane == 0, high, jnp.where(lane == LANES - 1, low, 0.0))

    edge = cellh[...]
    edge_bed = [look(edge[slot]) for slot in range(4)]
    edge_wet = [edge[slot].astype(jnp.float32) for slot in range(4)]
    bed_v[...] = look(cls[...])
    for target, inner, edges, at, terms in (
        (wet_p, wet[...].astype(jnp.float32), edge_wet, 0, 1),
        (bed_p, bed_v[...], edge_bed, 1, 3),
    ):
        full = 0.0
        for part in split(inner, terms):
            full += dot(dot(down, part).astype(jnp.bfloat16), across)
        target[SUB:end, 0:tile_cols] = full

        def row_of(slot):
            total = 0.0
            for part in split(edges[slot], terms):
                total += dot(part, across)
            return total[at : at + 1]

        def col_of(slot):
            total = 0.0
            for part in split(edges[slot], terms):
                total += dot_t(down, part)
            return total[:, at : at + 1]

        zeros = jnp.zeros((SUB, wide), jnp.float32)
        target[0:SUB, :] = zeros
        target[end : end + SUB, :] = zeros
        target[SUB - 1 : SUB, 0:tile_cols] = jnp.where(above, row_of(0), 0.0)
        target[end : end + 1, 0:tile_cols] = jnp.where(below, row_of(1), 0.0)
        target[SUB:end, tile_cols:wide] = side(col_of(2), col_of(3))

    for k in range(3):
        pad[k, SUB:end, 0:tile_cols] = fields[k]
        pad[k, 0:SUB, :] = jnp.zeros((SUB, wide), jnp.float32)
        pad[k, end : end + SUB, :] = jnp.zeros((SUB, wide), jnp.float32)
        pad[k, SUB - 1 : SUB, 0:tile_cols] = jnp.where(above, rowh[0, k : k + 1, :], 0.0)
        pad[k, end : end + 1, 0:tile_cols] = jnp.where(below, rowh[1, k : k + 1, :], 0.0)
        pad[k, SUB:end, tile_cols:wide] = side(
            edge_cols[:, k : k + 1], edge_cols[:, 3 + k : 4 + k]
        )

    window = chunk + 2 * SUB

    def west(x):
        return pltpu.roll(x, 1, 1)

    def east(x):
        return pltpu.roll(x, wide - 1, 1)

    def north(x):
        return pltpu.roll(x, 1, 0)

    def south(x):
        return pltpu.roll(x, x.shape[0] - 1, 0)

    def body(step, _):
        base = pl.multiple_of(step * chunk, SUB)
        at = pl.ds(base, window)
        h, hu, hv = pad[0, at, :], pad[1, at, :], pad[2, at, :]
        wet_w, bed_w = wet_p[at, :], bed_p[at, :]
        safe = jnp.where(wet_w > 0.5, h, 1.0)
        inverse = 1.0 / safe
        u, v = hu * inverse, hv * inverse
        speed = safe * lax.rsqrt(safe)
        pressure = 0.5 * gravity * safe * safe
        cross = hu * v

        def mid(x):
            return x[SUB : SUB + chunk]

        def narrow(x):
            return x[:, 0:tile_cols]

        h_n, hu_n, hv_n, wet_n, bed_n = [narrow(x) for x in (h, hu, hv, wet_w, bed_w)]
        gate = (0.5 * courant) * (north(wet_n) * wet_n)
        reach = narrow(jnp.abs(v) + speed)
        bound = jnp.maximum(north(reach), reach)
        totals = []
        for state, flux in (
            (h_n, hv_n), (hu_n, narrow(cross)), (hv_n, narrow(hv * v + pressure)),
        ):
            face = gate * ((north(flux) + flux) - bound * (state - north(state)))
            totals.append(mid(face) - mid(south(face)))
        slope = gate * (bed_n - north(bed_n))
        centre = mid(h_n)
        totals[2] -= gravity * centre * (mid(slope) + mid(south(slope)))

        h_m, hu_m, hv_m, wet_m, bed_m = [mid(x) for x in (h, hu, hv, wet_w, bed_w)]
        gate = (0.5 * courant) * (west(wet_m) * wet_m)
        reach = mid(jnp.abs(u) + speed)
        bound = jnp.maximum(west(reach), reach)
        for k, (state, flux) in enumerate(
            ((h_m, hu_m), (hu_m, mid(hu * u + pressure)), (hv_m, mid(cross)))
        ):
            face = gate * ((west(flux) + flux) - bound * (state - west(state)))
            totals[k] += narrow(face - east(face))
        slope = gate * (bed_m - west(bed_m))
        totals[1] -= gravity * centre * narrow(slope + east(slope))
        out = pl.ds(base, chunk)
        for k, state in enumerate((h_m, hu_m, hv_m)):
            fine[0, k, out, :] = narrow(state) + totals[k]
        return 0

    lax.fori_loop(0, tile_rows // chunk, body, 0)

    shift_r, shift_c = anchor[nest, 0], anchor[nest, 1]
    low = onehot(
        iota((2 * cell_rows, tile_rows), 1) // 3 + shift_r == iota((2 * cell_rows, tile_rows), 0)
    )
    wide_pick = onehot(
        iota((tile_cols, 2 * cell_cols), 0) // 3 + shift_c == iota((tile_cols, 2 * cell_cols), 1)
    )
    for k in range(3):
        part_rows = 0.0
        for part in split(fine[0, k], 2):
            part_rows += dot(low, part)
        placed = 0.0
        for part in split(part_rows, 2):
            placed += dot(part, wide_pick)
        placed = placed * (1.0 / 9.0)
        for a in range(2):
            for b in range(2):
                quads[2 * a + b, k] = placed[
                    a * cell_rows : (a + 1) * cell_rows, b * cell_cols : (b + 1) * cell_cols
                ]


def step(rows, cols, anchor, levels, fields, edge_cols, rowh, wet, cls, cellh):
    tile_rows, tile_cols = fields.shape[1:]
    cell_rows, cell_cols = wet.shape
    smem = pl.BlockSpec(memory_space=pltpu.SMEM)
    vmem = pl.BlockSpec(memory_space=pltpu.VMEM)
    f32 = jnp.float32
    padded = (tile_rows + 2 * SUB, tile_cols + LANES)
    return pl.pallas_call(
        functools.partial(step_kernel, rows, cols, 48),
        out_shape=(
            jax.ShapeDtypeStruct((1, 3, tile_rows, tile_cols), f32),
            jax.ShapeDtypeStruct((4, 3, cell_rows, cell_cols), f32),
        ),
        in_specs=[smem, smem] + [vmem] * 6,
        out_specs=(vmem, vmem),
        scratch_shapes=[
            pltpu.VMEM((3,) + padded, f32),
            pltpu.VMEM(wet.shape, f32),
            pltpu.VMEM(padded, f32),
            pltpu.VMEM(padded, f32),
        ],
        compiler_params=pltpu.CompilerParams(vmem_limit_bytes=40 * 1024 * 1024),
        name="step",
    )(anchor, levels, fields, edge_cols, rowh, wet, cls, cellh)


def feedback_kernel(nests, rows, cols, anchor, quads, coarse, out, held, send_sem, recv_sem):
    nest, row, col = lax.axis_index("nest"), lax.axis_index("row"), lax.axis_index("col")
    block = nest * rows + row
    blocks = nests * rows
    cell_rows, cell_cols = coarse.shape[1], coarse.shape[2]

    def place(b, c):
        return {"nest": b // rows, "row": lax.rem(b, rows), "col": c}

    links = []
    for quad in (1, 2, 3):
        db, dc = quad // 2, quad % 2
        sends = jnp.logical_and(block + db < blocks, col + dc < cols)
        takes = jnp.logical_and(block - db >= 0, col - dc >= 0)
        links.append((quad, sends, place(block + db, col + dc), takes, place(block - db, col - dc)))

    barrier = pltpu.get_barrier_semaphore()
    for _, _, _, takes, source in links:
        @pl.when(takes)
        def _(source=source):
            pl.semaphore_signal(barrier, inc=1, device_id=source, device_id_type=MESH)
    targets = sum(jnp.where(sends, 1, 0) for _, sends, _, _, _ in links)

    @pl.when(targets > 0)
    def _():
        pl.semaphore_wait(barrier, targets)

    def copy(quad, target):
        return pltpu.make_async_remote_copy(
            src_ref=quads.at[quad],
            dst_ref=held.at[quad - 1],
            send_sem=send_sem.at[quad - 1],
            recv_sem=recv_sem.at[quad - 1],
            device_id=target,
            device_id_type=MESH,
        )

    for quad, sends, target, _, _ in links:
        @pl.when(sends)
        def _(quad=quad, target=target):
            copy(quad, target).start()

    at_row = block * cell_rows + iota((cell_rows, cell_cols), 0)
    at_col = col * cell_cols + iota((cell_rows, cell_cols), 1)
    count = jnp.ones((cell_rows, cell_cols), jnp.float32)
    for n in range(nests):
        from_row = at_row - (n * rows * cell_rows + anchor[n, 0])
        from_col = at_col - anchor[n, 1]
        inside = (from_row >= 0) & (from_row < rows * cell_rows)
        inside &= (from_col >= 0) & (from_col < cols * cell_cols)
        count += jnp.where(inside, 1.0, 0.0)
    weight = 1.0 / count
    for k in range(3):
        out[k] = coarse[k] + quads[0, k]
    for quad, _, target, takes, _ in links:
        @pl.when(takes)
        def _(quad=quad, target=target):
            copy(quad, target).wait_recv()
            for k in range(3):
                out[k] += held[quad - 1, k]
    for k in range(3):
        out[k] = out[k] * weight
    for quad, sends, target, _, _ in links:
        @pl.when(sends)
        def _(quad=quad, target=target):
            copy(quad, target).wait_send()


def feedback(nests, rows, cols, anchor, quads, coarse):
    smem = pl.BlockSpec(memory_space=pltpu.SMEM)
    vmem = pl.BlockSpec(memory_space=pltpu.VMEM)
    return pl.pallas_call(
        functools.partial(feedback_kernel, nests, rows, cols),
        out_shape=jax.ShapeDtypeStruct(coarse.shape, jnp.float32),
        in_specs=[smem, vmem, vmem],
        out_specs=vmem,
        scratch_shapes=[
            pltpu.VMEM((3,) + coarse.shape, jnp.float32),
            pltpu.SemaphoreType.DMA((3,)),
            pltpu.SemaphoreType.DMA((3,)),
        ],
        compiler_params=pltpu.CompilerParams(collective_id=1, has_side_effects=True),
        name="feedback",
    )(anchor, quads, coarse)


def fused_kernel(
    nests, rows, cols, anchor_in, levels_in, strips, wet, cls, coarse, fine, out,
    anchor, levels, fine_sem, held, wet_v, cls_v, coarse_v, pad, wet_p, bed_p, colh, rowh, cellh,
    col_msg, row_msg, cell_msg, rest, left, above, corner, weight, load_sem,
    big_send, big_recv, col_send, col_recv, row_send, row_recv, cell_send, cell_recv,
    side_send, side_recv, down_send, down_recv, far_send, far_recv, relay_send, ready,
):
    parts = rows * cols
    nest, row, col = lax.axis_index("nest"), lax.axis_index("row"), lax.axis_index("col")
    me = row * cols + col
    block, blocks = nest * rows + row, nests * rows
    band = strips.shape[4]
    tile_rows, tile_cols = fine.shape[2], fine.shape[3]
    cell_rows, cell_cols = wet_v.shape
    group = band // 3
    wide = tile_cols + LANES
    end = SUB + tile_rows
    has_above, has_below = row > 0, row < rows - 1
    has_left, has_right = col > 0, col < cols - 1
    has_last, has_next = block > 0, block < blocks - 1

    loads = [
        pltpu.make_async_copy(strips.at[0, :, :, 0], held, load_sem.at[0]),
        pltpu.make_async_copy(wet.at[0], wet_v, load_sem.at[1]),
        pltpu.make_async_copy(cls.at[0], cls_v, load_sem.at[2]),
        pltpu.make_async_copy(coarse, coarse_v, load_sem.at[3]),
        pltpu.make_async_copy(anchor_in, anchor, load_sem.at[4]),
        pltpu.make_async_copy(levels_in, levels, load_sem.at[5]),
    ]
    for load in loads:
        load.start()

    def place(q):
        return {"row": q // cols, "col": lax.rem(q, cols)}

    barrier = pltpu.get_barrier_semaphore()
    to_next = jnp.logical_and(row == rows - 1, nest < nests - 1)
    to_last = jnp.logical_and(row == 0, nest > 0)
    below_id = {"nest": (block + 1) // rows, "row": lax.rem(block + 1, rows), "col": col}

    def rank(q):
        r = q // cols
        c = lax.rem(q, cols)
        return (2 * (r // 2 + lax.rem(r, 2) + c) + jnp.where(c == 2, 0, 1)) * parts + q

    mine = rank(me)

    def stride(n, col=col):
        if cols != 4:
            return n
        m = jnp.maximum(n - 2 * rows, 0)
        near = jnp.where(col == 0, 1, 3) + cols * (n - 1)
        far = jnp.where(col == 0, 2, 1) + lax.rem(m, 2) + cols * (m // 2)
        t = jnp.where(n <= rows, near, jnp.where(n < 2 * rows, cols * (n - rows), far))
        first = jnp.where(lax.rem(n, cols) == 0, n + 1 - cols, n + 1)
        first = jnp.where(n == parts - 1, parts + 1 - cols, first)
        return jnp.where(col == 1, n, jnp.where(col == 2, first, t))

    early = min(parts, HEAD)

    def turn_of(source, q):
        at = early - 1
        for n in range(early - 1, 0, -1):
            hit = lax.rem(source + stride(n, lax.rem(source, cols)), parts) == q
            at = jnp.where(hit, n - 1, at)
        return at

    def greet(t, count):
        q = lax.rem(me + t, parts)
        later = rank(q) > mine

        @pl.when(later)
        def _():
            pl.semaphore_signal(barrier, inc=1, device_id=place(q), device_id_type=MESH)

        return count + jnp.where(later, 0, 1)

    for at, takes in ((col, to_last), (col - 1, jnp.logical_and(to_last, has_left))):
        @pl.when(takes)
        def _(at=at):
            pl.semaphore_signal(
                barrier, inc=1, device_id={"nest": nest - 1, "row": rows - 1, "col": at},
                device_id_type=MESH,
            )

    earlier = lax.fori_loop(1, parts, greet, 0) + jnp.where(to_next, 1, 0)
    earlier = earlier + jnp.where(jnp.logical_and(to_next, has_right), 1, 0)

    @pl.when(earlier > 0)
    def _():
        pl.semaphore_wait(barrier, earlier)

    def answer(t, _):
        q = lax.rem(me + t, parts)

        @pl.when(rank(q) < mine)
        def _():
            pl.semaphore_signal(
                ready.at[turn_of(q, me)], inc=1, device_id=place(q), device_id_type=MESH
            )

        return 0

    lax.fori_loop(1, parts, answer, 0)

    def meet(n):
        @pl.when(rank(lax.rem(me + stride(n), parts)) > mine)
        def _():
            pl.semaphore_wait(ready.at[n - 1], 1)

    def columns(c):
        return pl.ds(pl.multiple_of(c * tile_cols, LANES), tile_cols)

    def landing(p):
        return pad.at[:, pl.ds(pl.multiple_of(SUB + p * band, SUB), band), 0:tile_cols]

    def big(q):
        return pltpu.make_async_remote_copy(
            src_ref=strips.at[0, :, q // cols, 0, :, columns(lax.rem(q, cols))],
            dst_ref=landing(me),
            send_sem=big_send.at[0],
            recv_sem=big_recv.at[me],
            device_id=place(q),
            device_id_type=MESH,
        )

    def big_start(t, _):
        big(lax.rem(me + t, parts)).start()
        return 0

    def first_start(n, _):
        meet(n)
        return big_start(stride(n), 0)

    def next_start(n, _):
        return big_start(stride(n), 0)

    lax.fori_loop(1, early, first_start, 0)
    own = pltpu.make_async_copy(
        strips.at[0, :, row, 0, :, columns(col)], landing(me), big_recv.at[me]
    )
    own.start()

    loads[1].wait()
    loads[2].wait()
    for at, cells in enumerate((wet_v, cls_v)):
        cell_msg[0, at : at + 1, :] = cells[cell_rows - 1 : cell_rows, :]
        cell_msg[1, at : at + 1, :] = cells[0:1, :]
        across = cells[...].astype(jnp.float32).astype(jnp.bfloat16)
        pick = iota((SUB, cell_cols), 1)
        cell_msg[2, at : at + 1, :] = dot_t(onehot(pick == cell_cols - 1), across)[0:1].astype(jnp.int32)
        cell_msg[3, at : at + 1, :] = dot_t(onehot(pick == 0), across)[0:1].astype(jnp.int32)
    loads[0].wait()
    for j in range(rows):
        for k in range(3):
            row_msg[0, j, k : k + 1, :] = held[k, j, band - 1 : band, :]
            row_msg[1, j, k : k + 1, :] = held[k, j, 0:1, :]
    col_msg[...] = jnp.zeros_like(col_msg)
    lane = iota((3 * band, LANES), 1)
    for j in range(rows):
        for c in range(1, cols):
            at = c * tile_cols
            low = jnp.concatenate([held[k, j, :, at - LANES : at] for k in range(3)], axis=0)
            high = jnp.concatenate([held[k, j, :, at : at + LANES] for k in range(3)], axis=0)
            both = jnp.where(lane == 0, high, low).T
            col_msg[j * cols + c, 0:1, 0 : 3 * band] = both[LANES - 1 : LANES]
            col_msg[j * cols + c - 1, 1:2, 0 : 3 * band] = both[0:1]

    def later(n, count):
        return count + jnp.where(rank(lax.rem(me + stride(n), parts)) > mine, 1, 0)

    rest_of = lax.fori_loop(early, parts, later, 0)

    @pl.when(rest_of > 0)
    def _():
        pl.semaphore_wait(ready.at[early - 1], rest_of)

    cell_links = (
        (0, has_below, {"row": row + 1, "col": col}, has_above),
        (1, has_above, {"row": row - 1, "col": col}, has_below),
        (2, has_right, {"row": row, "col": col + 1}, has_left),
        (3, has_left, {"row": row, "col": col - 1}, has_right),
    )

    def cell_copy(slot, target):
        return pltpu.make_async_remote_copy(
            src_ref=cell_msg.at[slot],
            dst_ref=cellh.at[slot],
            send_sem=cell_send.at[slot],
            recv_sem=cell_recv.at[slot],
            device_id=target,
            device_id_type=MESH,
        )

    for slot, sends, target, _ in cell_links:
        @pl.when(sends)
        def _(slot=slot, target=target):
            cell_copy(slot, target).start()

    def row_copy(slot, j, c):
        return pltpu.make_async_remote_copy(
            src_ref=row_msg.at[slot, j, :, c * tile_cols : (c + 1) * tile_cols],
            dst_ref=rowh.at[slot],
            send_sem=row_send.at[j],
            recv_sem=row_recv.at[slot],
            device_id={"row": j + 1 if slot == 0 else j - 1, "col": c},
            device_id_type=MESH,
        )

    def row_own(slot, j, c):
        return pltpu.make_async_copy(
            row_msg.at[slot, j, :, c * tile_cols : (c + 1) * tile_cols],
            rowh.at[slot],
            row_recv.at[slot],
        )

    owner = (parts - 1, 0)

    def row_targets(slot):
        for j in range(rows):
            target_row = j + 1 if slot == 0 else j - 1
            if 0 <= target_row < rows:
                for c in range(cols):
                    yield j, c, target_row * cols + c == owner[slot]

    for slot in range(2):
        @pl.when(me == owner[slot])
        def _(slot=slot):
            for j, c, mine in row_targets(slot):
                (row_own if mine else row_copy)(slot, j, c).start()

    def col_copy(q):
        return pltpu.make_async_remote_copy(
            src_ref=col_msg.at[q],
            dst_ref=colh.at[me],
            send_sem=col_send.at[0],
            recv_sem=col_recv.at[0],
            device_id=place(q),
            device_id_type=MESH,
        )

    def col_start(n, _):
        col_copy(lax.rem(me + stride(n), parts)).start()
        return 0

    lax.fori_loop(1, parts, col_start, 0)
    pltpu.make_async_copy(col_msg.at[me], colh.at[me], col_recv.at[0]).start()
    if early < parts:
        lax.fori_loop(early, parts, next_start, 0)

    loads[4].wait()
    loads[5].wait()

    def look(classes):
        bed = jnp.zeros(classes.shape, jnp.float32)
        for at in range(levels.shape[0]):
            bed = jnp.where(classes == at, levels[at], bed)
        return bed

    down = onehot(iota((tile_rows, cell_rows), 0) // 3 == iota((tile_rows, cell_rows), 1))
    across = onehot(iota((cell_cols, tile_cols), 1) // 3 == iota((cell_cols, tile_cols), 0))

    def side(low, high):
        lane = iota((low.shape[0], LANES), 1)
        low = jnp.where(has_left, low, 0.0)
        high = jnp.where(has_right, high, 0.0)
        return jnp.where(lane == 0, high, jnp.where(lane == LANES - 1, low, 0.0))

    inner = (wet_v[...].astype(jnp.float32), look(cls_v[...]))
    zeros = jnp.zeros((SUB, wide), jnp.float32)
    for target, cells, terms in ((wet_p, inner[0], 1), (bed_p, inner[1], 3)):
        full = 0.0
        for part in split(cells, terms):
            full += dot(dot(down, part).astype(jnp.bfloat16), across)
        target[SUB:end, 0:tile_cols] = full
        target[0:SUB, :] = zeros
        target[end : end + SUB, :] = zeros
    for k in range(3):
        pad[k, 0:SUB, :] = zeros
        pad[k, end : end + SUB, :] = zeros

    for slot, _, target, receives in cell_links:
        @pl.when(jnp.logical_not(receives))
        def _(slot=slot):
            cellh[slot] = jnp.zeros((2, LANES), jnp.int32)

        @pl.when(receives)
        def _(slot=slot, target=target):
            cell_copy(slot, target).wait_recv()

    for target, at, terms in ((wet_p, 0, 1), (bed_p, 1, 3)):
        def edge_of(slot, at=at):
            cells = jnp.concatenate([cellh[slot], jnp.zeros((SUB - 2, LANES), jnp.int32)], axis=0)
            return cells.astype(jnp.float32) if at == 0 else look(cells)

        def row_of(slot, at=at, terms=terms):
            total = 0.0
            for part in split(edge_of(slot), terms):
                total += dot(part, across)
            return total[at : at + 1]

        def col_of(slot, at=at, terms=terms):
            total = 0.0
            for part in split(edge_of(slot), terms):
                total += dot_t(down, part)
            return total[:, at : at + 1]

        target[SUB - 1 : SUB, 0:tile_cols] = jnp.where(has_above, row_of(0), 0.0)
        target[end : end + 1, 0:tile_cols] = jnp.where(has_below, row_of(1), 0.0)
        target[SUB:end, tile_cols:wide] = side(col_of(2), col_of(3))

    def settle(ref, sem):
        pltpu.make_async_copy(ref, ref, sem.at[0]).wait()

    settle(colh, col_recv)
    edges = jnp.concatenate([colh[b] for b in range(parts)], axis=0).T
    for k in range(3):
        edge = edges[k * band : (k + 1) * band]
        for b in range(parts):
            top = SUB + b * band
            pad[k, top : top + band, tile_cols:wide] = side(
                edge[:, 2 * b : 2 * b + 1], edge[:, 2 * b + 1 : 2 * b + 2]
            )

    at_row = block * cell_rows + iota((cell_rows, cell_cols), 0)
    at_col = col * cell_cols + iota((cell_rows, cell_cols), 1)
    count = jnp.ones((cell_rows, cell_cols), jnp.float32)
    for n in range(nests):
        from_row = at_row - (n * rows * cell_rows + anchor[n, 0])
        from_col = at_col - anchor[n, 1]
        covered = (from_row >= 0) & (from_row < rows * cell_rows)
        covered &= (from_col >= 0) & (from_col < cols * cell_cols)
        count += jnp.where(covered, 1.0, 0.0)
    weight[...] = 1.0 / count

    pick = onehot(iota((tile_cols, cell_cols), 0) // 3 == iota((tile_cols, cell_cols), 1))

    def west(x):
        return pltpu.roll(x, 1, 1)

    def east(x):
        return pltpu.roll(x, wide - 1, 1)

    def north(x):
        return pltpu.roll(x, 1, 0)

    def south(x):
        return pltpu.roll(x, x.shape[0] - 1, 0)

    def narrow(x):
        return x[:, 0:tile_cols]

    def big_wait(b):
        pltpu.make_async_copy(landing(b), landing(b), big_recv.at[b]).wait()

    def rest_rows(ref, b):
        return ref.at[:, pl.ds(pl.multiple_of(b * group, SUB), group), :]

    middle = cols // 2

    def side_copy(b, slot):
        return pltpu.make_async_remote_copy(
            src_ref=rest_rows(rest, b),
            dst_ref=rest_rows(left, b),
            send_sem=side_send.at[0],
            recv_sem=side_recv.at[slot],
            device_id={"col": col + 1},
            device_id_type=MESH,
        )

    def down_copy(b):
        return pltpu.make_async_remote_copy(
            src_ref=rest_rows(rest, b),
            dst_ref=rest_rows(above, b),
            send_sem=down_send.at[0],
            recv_sem=down_recv.at[0],
            device_id=below_id,
            device_id_type=MESH,
        )

    def far_copy(b):
        return pltpu.make_async_remote_copy(
            src_ref=rest_rows(rest, b),
            dst_ref=rest_rows(corner, b),
            send_sem=far_send.at[0],
            recv_sem=far_recv.at[0],
            device_id={**below_id, "col": col + 1},
            device_id_type=MESH,
        )

    def relay_copy(b):
        return pltpu.make_async_remote_copy(
            src_ref=rest_rows(left, b),
            dst_ref=rest_rows(corner, b),
            send_sem=relay_send.at[0],
            recv_sem=far_recv.at[0],
            device_id=below_id,
            device_id_type=MESH,
        )

    def share(s):
        b = band_at(s)

        @pl.when(jnp.logical_and(has_right, col + 1 != middle))
        def _():
            side_copy(b, parts - DIRECT).start()

        @pl.when(has_next)
        def _():
            down_copy(b).start()

        @pl.when(jnp.logical_and(jnp.logical_and(has_right, has_next), col + 1 != middle))
        def _():
            far_copy(b).start()

    def share_middle(first, last):
        def one(s, _):
            b = band_at(s)
            side_copy(b, jnp.minimum(s, parts - DIRECT)).start()

            @pl.when(jnp.logical_and(has_next, s >= parts - DIRECT))
            def _():
                far_copy(b).start()

            return 0

        @pl.when(col + 1 == middle)
        def _():
            lax.fori_loop(first, last, one, 0)

    last_three = parts - 2
    if cols == 4:
        last_three = jnp.where(col == 1, parts - 2, jnp.where(col == 2, parts - 4, parts - 3))

    def turn(s, first):
        t = jnp.where(s < first - 1, s + 1, s + 4)
        return jnp.where(s < parts - 3, t, first + s - (parts - 3))

    def band_at(s):
        return lax.rem(me + parts - turn(s, last_three), parts)

    def advance(base, count):
        def mid(x):
            return x[SUB : SUB + count]

        base = pl.multiple_of(base, SUB)
        at = pl.ds(base, count + 2 * SUB)
        h, hu, hv = pad[0, at, :], pad[1, at, :], pad[2, at, :]
        wet_w, bed_w = wet_p[at, :], bed_p[at, :]
        safe = jnp.where(wet_w > 0.5, h, 1.0)
        inverse = 1.0 / safe
        u, v = hu * inverse, hv * inverse
        speed = safe * lax.rsqrt(safe)
        pressure = 0.5 * gravity * safe * safe
        cross = hu * v

        h_n, hu_n, hv_n, wet_n, bed_n = [narrow(x) for x in (h, hu, hv, wet_w, bed_w)]
        gate = (0.5 * courant) * (north(wet_n) * wet_n)
        reach = narrow(jnp.abs(v) + speed)
        bound = jnp.maximum(north(reach), reach)
        totals = []
        for state, flux in (
            (h_n, hv_n), (hu_n, narrow(cross)), (hv_n, narrow(hv * v + pressure)),
        ):
            face = gate * ((north(flux) + flux) - bound * (state - north(state)))
            totals.append(mid(face) - mid(south(face)))
        slope = gate * (bed_n - north(bed_n))
        centre = mid(h_n)
        totals[2] -= gravity * centre * (mid(slope) + mid(south(slope)))

        h_m, hu_m, hv_m, wet_m, bed_m = [mid(x) for x in (h, hu, hv, wet_w, bed_w)]
        gate = (0.5 * courant) * (west(wet_m) * wet_m)
        reach = mid(jnp.abs(u) + speed)
        bound = jnp.maximum(west(reach), reach)
        for k, (state, flux) in enumerate(
            ((h_m, hu_m), (hu_m, mid(hu * u + pressure)), (hv_m, mid(cross)))
        ):
            face = gate * ((west(flux) + flux) - bound * (state - west(state)))
            totals[k] += narrow(face - east(face))
        slope = gate * (bed_m - west(bed_m))
        totals[1] -= gravity * centre * narrow(slope + east(slope))
        for k, state in enumerate((h_m, hu_m, hv_m)):
            fine[0, k, pl.ds(base, count), :] = narrow(state) + totals[k]

    def restrict(base, count):
        rows_of = pl.ds(pl.multiple_of(base, SUB), count)
        value = jnp.concatenate([fine[0, k, rows_of, :] for k in range(3)], axis=0)
        narrowed = dot(jnp.concatenate(split(value, 2), axis=0), pick)
        third = onehot(iota((count, 3 * count), 1) // 3 == iota((count, 3 * count), 0))
        mean = 0.0
        for part in split(narrowed[: 3 * count] + narrowed[3 * count :], 2):
            mean += dot(third, part)
        mean = mean * (1.0 / 9.0)
        cells = pl.ds(pl.multiple_of(base // 3, SUB), count // 3)
        for k in range(3):
            rest[k, cells, :] = mean[k * count // 3 : (k + 1) * count // 3]

    def arrived(t):
        big_wait(lax.rem(me + parts - t, parts))

    def halo(lowest, highest):
        for slot, edge, receives, at in ((0, 0, has_above, SUB - 1), (1, parts - 1, has_below, end)):
            here = jnp.logical_and(lowest <= edge, edge <= highest)

            @pl.when(jnp.logical_and(here, receives))
            def _(slot=slot, at=at):
                row_own(slot, 0, 0).wait()
                for k in range(3):
                    pad[k, at : at + 1, 0:tile_cols] = rowh[slot, k : k + 1, :]

    def body(s, _):
        b = band_at(s)

        @pl.when(s > 1)
        def _():
            share(s - 2)

        @pl.when(s == 0)
        def _():
            big_wait(me)
            arrived(1)

        @pl.when(s < last_three - 1)
        def _():
            arrived(s + 2)

        @pl.when(s == last_three - 1)
        def _():
            def others(t, _):
                arrived(t)
                return 0

            lax.fori_loop(last_three + 2, parts, others, 0)

        halo(b, b)
        advance(b * band, band)
        restrict(band_at(jnp.maximum(s - 1, 0)) * band, band)
        return 0

    lax.fori_loop(0, parts - 3, body, 0)
    share(parts - 5)
    share_middle(0, parts - 4)
    restrict(band_at(parts - 4) * band, band)
    lowest = band_at(parts - 1)
    halo(lowest, lowest + 2)
    advance(lowest * band, band - SUB)
    advance((lowest + 2) * band + SUB, band - SUB)
    arrived(last_three + 1)
    share(parts - 4)
    share_middle(parts - 4, parts - 3)
    advance((lowest + 1) * band - SUB, band + 2 * SUB)
    restrict(lowest * band, 3 * band)
    for s in range(parts - 3, parts):
        share(s)
    share_middle(parts - 3, parts)

    source = jnp.maximum(block - 1, 0) // rows
    row_own, col_own = anchor[nest, 0], anchor[nest, 1]
    row_last, col_last = anchor[source, 0], anchor[source, 1]
    cell_row = iota((cell_rows, cell_cols), 0)
    cell_col = iota((cell_rows, cell_cols), 1)
    def moved(cells, keep, by_col, from_row, by_row):
        cells = jnp.where(keep, pltpu.roll(cells, by_col, 1), 0.0)
        return jnp.where(from_row, pltpu.roll(cells, by_row, 0), 0.0)

    loads[3].wait()
    for k in range(3):
        out[k] = coarse_v[k] + moved(
            rest[k], cell_col >= col_own, col_own, cell_row >= row_own, row_own
        )

    left_three = parts - 2 if cols == 4 else last_three

    def relay(t, _):
        b = lax.rem(me + 2 * parts - 1 - turn(t, left_three), parts)
        pltpu.make_async_copy(rest_rows(left, b), rest_rows(left, b), side_recv.at[t]).wait()

        @pl.when(has_next)
        def _():
            relay_copy(b).start()

        return 0

    few = DIRECT * group

    @pl.when(jnp.logical_and(has_left, col == middle))
    def _():
        lax.fori_loop(0, parts - DIRECT, relay, 0)
        pltpu.make_async_copy(rest.at[:, :few], left.at[:, :few], side_recv.at[parts - DIRECT]).wait()

    @pl.when(jnp.logical_and(has_left, col != middle))
    def _():
        pltpu.make_async_copy(rest, left, side_recv.at[parts - DIRECT]).wait()

    @pl.when(has_left)
    def _():
        for k in range(3):
            out[k] += moved(left[k], cell_col < col_own, col_own, cell_row >= row_own, row_own)

    @pl.when(has_last)
    def _():
        settle(above, down_recv)
        for k in range(3):
            out[k] += moved(above[k], cell_col >= col_last, col_last, cell_row < row_last, row_last)

    @pl.when(jnp.logical_and(has_last, has_left))
    def _():
        settle(corner, far_recv)
        for k in range(3):
            out[k] += moved(corner[k], cell_col < col_last, col_last, cell_row < row_last, row_last)

    for k in range(3):
        out[k] = out[k] * weight[...]

    settle(pad.at[:, SUB : SUB + (parts - 1) * band, 0:tile_cols], big_send)
    settle(colh.at[0 : parts - 1], col_send)
    for slot, sends, target, _ in cell_links:
        @pl.when(sends)
        def _(slot=slot, target=target):
            cell_copy(slot, target).wait_send()
    for slot in range(2):
        @pl.when(me == owner[slot])
        def _(slot=slot):
            for row_at in range(rows):
                n = sum(j == row_at and not mine for j, _, mine in row_targets(slot))
                if n > 0:
                    sent = row_msg.at[slot, row_at, :, 0 : n * tile_cols]
                    pltpu.make_async_copy(sent, sent, row_send.at[row_at]).wait()

    @pl.when(has_right)
    def _():
        settle(rest, side_send)

    @pl.when(has_next)
    def _():
        settle(rest, down_send)

    @pl.when(jnp.logical_and(jnp.logical_and(has_next, has_right), col + 1 != middle))
    def _():
        settle(rest, far_send)

    @pl.when(jnp.logical_and(jnp.logical_and(has_next, has_right), col + 1 == middle))
    def _():
        settle(rest.at[:, :few], far_send)

    @pl.when(jnp.logical_and(jnp.logical_and(has_next, has_left), col == middle))
    def _():
        settle(rest.at[:, few:], relay_send)


def fused(nests, rows, cols, strips, anchor, wet, cls, levels, coarse):
    parts = rows * cols
    blocks, band, full_cols = strips.shape[2], strips.shape[4], strips.shape[5]
    tile_rows, tile_cols = parts * band, full_cols // cols
    cells = wet.shape[1:]
    vmem = pl.BlockSpec(memory_space=pltpu.VMEM)
    hbm = pl.BlockSpec(memory_space=pltpu.HBM)
    dma = pltpu.SemaphoreType.DMA
    f32, i32 = jnp.float32, jnp.int32
    padded = (tile_rows + 2 * SUB, tile_cols + LANES)
    results = 4 * (3 * tile_rows * tile_cols + coarse.size)
    return pl.pallas_call(
        functools.partial(fused_kernel, nests, rows, cols),
        out_shape=(
            pltpu.VMEM((1, 3, tile_rows, tile_cols), f32),
            pltpu.VMEM(coarse.shape, f32),
        ),
        in_specs=[hbm] * 6,
        out_specs=(vmem, vmem),
        scratch_shapes=[
            pltpu.SMEM(anchor.shape, i32),
            pltpu.SMEM(levels.shape, f32),
            dma((parts,)),
            pltpu.VMEM((3, blocks, band, full_cols), f32),
            pltpu.VMEM(cells, i32),
            pltpu.VMEM(cells, i32),
            pltpu.VMEM(coarse.shape, f32),
            pltpu.VMEM((3,) + padded, f32),
            pltpu.VMEM(padded, f32),
            pltpu.VMEM(padded, f32),
            pltpu.VMEM((parts, 2, LANES), f32),
            pltpu.VMEM((2, 4, tile_cols), f32),
            pltpu.VMEM((4, 2, LANES), i32),
            pltpu.VMEM((parts, 2, LANES), f32),
            pltpu.VMEM((2, blocks, 4, full_cols), f32),
            pltpu.VMEM((4, 2, LANES), i32),
            pltpu.VMEM(coarse.shape, f32),
            pltpu.VMEM(coarse.shape, f32),
            pltpu.VMEM(coarse.shape, f32),
            pltpu.VMEM(coarse.shape, f32),
            pltpu.VMEM(cells, f32),
            dma((6,)),
            dma((1,)), dma((parts,)), dma((1,)), dma((1,)),
            dma((rows,)), dma((2,)), dma((4,)), dma((4,)),
            dma((1,)), dma((parts - DIRECT + 1,)), dma((1,)), dma((1,)), dma((1,)), dma((1,)), dma((1,)),
            pltpu.SemaphoreType.REGULAR((HEAD,)),
        ],
        compiler_params=pltpu.CompilerParams(
            collective_id=2, has_side_effects=True, vmem_limit_bytes=VMEM_BYTES - results
        ),
        name="fused",
    )(anchor, levels, strips, wet, cls, coarse)


def emit_kernel(fine, coarse, fine_out, coarse_out, sems):
    copies = [
        pltpu.make_async_copy(fine, fine_out, sems.at[0]),
        pltpu.make_async_copy(coarse, coarse_out, sems.at[1]),
    ]
    for copy in copies:
        copy.start()
    for copy in copies:
        copy.wait()


def emit(fine, coarse):
    vmem = pl.BlockSpec(memory_space=pltpu.VMEM)
    hbm = pl.BlockSpec(memory_space=pl.ANY)
    return pl.pallas_call(
        emit_kernel,
        out_shape=(
            jax.ShapeDtypeStruct(fine.shape, jnp.float32),
            jax.ShapeDtypeStruct(coarse.shape, jnp.float32),
        ),
        in_specs=[vmem, vmem],
        out_specs=(hbm, hbm),
        scratch_shapes=[pltpu.SemaphoreType.DMA((2,))],
        compiler_params=pltpu.CompilerParams(vmem_limit_bytes=4 * 2**20),
        name="emit",
    )(fine, coarse)


def local(nests, rows, cols, strips, anchor, wet_mask, bathy_index, bed_levels, coarse):
    band = strips.shape[4]
    if band % (3 * SUB) == 0 and 3 * band <= LANES and rows * cols > DIRECT + 3 and cols == 4:
        return emit(*fused(
            nests, rows, cols, strips, anchor, wet_mask, bathy_index, bed_levels, coarse
        ))
    fields, colh, rowh, cellh = exchange(rows, cols, strips, wet_mask, bathy_index)
    fields = fields.reshape(3, -1, fields.shape[3])
    edge_cols = colh[:, :, :band].transpose(0, 2, 1).reshape(-1, SUB)
    updated, quads = step(
        rows, cols, anchor, bed_levels, fields, edge_cols, rowh, wet_mask[0], bathy_index[0], cellh
    )
    return updated, feedback(nests, rows, cols, anchor, quads, coarse)


def solution(mesh):
    sizes = (mesh.shape["nest"], mesh.shape["row"], mesh.shape["col"])
    return jax.shard_map(
        functools.partial(local, *sizes),
        mesh=mesh,
        in_specs=(
            P("nest", None, None, ("row", "col"), None, None),
            P(),
            P("nest", "row", "col"),
            P("nest", "row", "col"),
            P(),
            P(None, ("nest", "row"), "col"),
        ),
        out_specs=(P("nest", None, "row", "col"), P(None, ("nest", "row"), "col")),
        check_vma=False,
    )
```
